32 devices in a mesh: seq: 4 (over y, core), fsdp: 8 (over z, x).
Axes of the slice: x: 2, y: 2, z: 4, core: 2. Of those that a mesh axis runs over, the one named last changes fastest.
Arguments:
- tokens: bfloat16 [8, 1032, 1024], P('fsdp', 'seq'), may hold values from -6 to 6
- lengths: int32 [8], P('fsdp'), may hold values from 516 to 1025, as said below
- ln1_gain: bfloat16 [1024], P('fsdp'), may hold values from 0.5 to 1.5
- ln1_bias: bfloat16 [1024], P('fsdp'), may hold values from -3 to 3
- qkv_weight: bfloat16 [1024, 3072], P('fsdp'), may hold values from -0.34375 to 0.34375
- q_bias: bfloat16 [1024], P('fsdp'), may hold values from -3 to 3
- v_bias: bfloat16 [1024], P('fsdp'), may hold values from -3 to 3
- out_weight: bfloat16 [1024, 1024], P('fsdp'), may hold values from -3 to 3
- out_bias: bfloat16 [1024], P('fsdp'), may hold values from -3 to 3
- ln2_gain: bfloat16 [1024], P('fsdp'), may hold values from 0.5 to 1.5
- ln2_bias: bfloat16 [1024], P('fsdp'), may hold values from -3 to 3
- up_weight: bfloat16 [1024, 4096], P('fsdp'), may hold values from -0.1875 to 0.1875
- up_bias: bfloat16 [4096], P('fsdp'), may hold values from -3 to 3
- down_weight: bfloat16 [4096, 1024], P('fsdp'), may hold values from -0.09375 to 0.09375
- down_bias: bfloat16 [1024], P('fsdp'), may hold values from -3 to 3
- cotangent: bfloat16 [8, 1032, 1024], P('fsdp', 'seq'), may hold values from -6 to 6
Outputs:
- output: bfloat16 [8, 1032, 1024], P('fsdp', 'seq')
- grad_tokens: bfloat16 [8, 1032, 1024], P('fsdp', 'seq')
- grad_ln1_gain: float32 [1024], P('fsdp')
- grad_ln1_bias: float32 [1024], P('fsdp')
- grad_qkv_weight: float32 [1024, 3072], P('fsdp')
- grad_q_bias: float32 [1024], P('fsdp')
- grad_v_bias: float32 [1024], P('fsdp')
- grad_out_weight: float32 [1024, 1024], P('fsdp')
- grad_out_bias: float32 [1024], P('fsdp')
- grad_ln2_gain: float32 [1024], P('fsdp')
- grad_ln2_bias: float32 [1024], P('fsdp')
- grad_up_weight: float32 [1024, 4096], P('fsdp')
- grad_up_bias: float32 [4096], P('fsdp')
- grad_down_weight: float32 [4096, 1024], P('fsdp')
- grad_down_bias: float32 [1024], P('fsdp')
The draws below stay inside these ranges and needn't reach their ends.
Inputs may be any that keep to these rules, and one draw needn't show every extreme that they name: `lengths`: each image's valid tokens are its first ones; some image has exactly 1025 valid tokens.
All inputs are finite; a program needn't handle non-finite values.
Results may differ from the reference program's by a relative error of at most 0.012.
The reference program's roundings to bfloat16 on the way count: a program that leaves them out, or rounds other values in their place, can miss the bound.
Values may be sent and summed in bfloat16 or wider, within the bound.
A program may use at most 192 MiB of HBM per device.

```python
from functools import partial
import jax
import jax.numpy as jnp
from jax import lax

D = 1024
HEADS = 16
HEAD_DIM = 64
FF = 4096
SEQ_LEN = 1032
IMAGES = 8
VALID_MOST = 1025


def draw_lengths(key, part):
    first_key, second_key = jax.random.split(jax.random.fold_in(key, 17))
    counts = jax.random.randint(first_key, (IMAGES,), SEQ_LEN // 2, VALID_MOST + 1)
    chosen = jax.random.randint(second_key, (), 0, IMAGES)
    return jnp.where(jnp.arange(IMAGES) == chosen, VALID_MOST, counts).astype(jnp.int32)


def draw_qkv_weight(key, part):
    own_key = jax.random.fold_in(key, 29)
    order_key, factor_key, entry_key = jax.random.split(own_key, 3)
    head_order = jax.random.permutation(order_key, HEADS)
    spread_factor = jax.random.uniform(factor_key, (HEADS,), jnp.float32, 2.0, 3.0)
    strong_count = max(HEADS // 4, 1)
    head_factor = jnp.where(head_order == 0, 3.5, jnp.where(head_order < strong_count, spread_factor, 1.0))
    per_column = jnp.repeat(head_factor, HEAD_DIM, total_repeat_length=D)
    column_scale = jnp.concatenate([per_column, per_column, jnp.ones((D,), jnp.float32)])
    entries = jnp.clip(jax.random.normal(entry_key, (D, 3 * D), jnp.float32), -3.0, 3.0)
    return (entries * column_scale[None, :] * D ** (-0.5)).astype(jnp.bfloat16)


def shard_levels(stream_key, extent, pieces, smallest, largest):
    def one(dim, blocks):
        steps = jax.random.uniform(jax.random.fold_in(jax.random.fold_in(stream_key, 6), dim), (blocks,), jnp.float32, smallest / len(pieces), largest / len(pieces))
        return jnp.repeat(jnp.exp(steps), extent[dim] // blocks).reshape((-1,) + (1,) * (len(extent) - dim - 1))

    level = one(*pieces[0])
    for cut in pieces[1:]:
        level = level * one(*cut)
    return level


def gaussian(stream_key, dims, scale, most, cuts=(), held_as=jnp.bfloat16):
    gain = shard_levels(stream_key, dims, cuts, -0.22, 0.18) if cuts else 1.0
    values = jax.random.normal(stream_key, dims, jnp.float32) * scale * gain
    return jnp.minimum(jnp.maximum(values, -most), most).astype(held_as)


def setup_inputs(seed: int = 0) -> dict:
    seeds = jax.random.split(jax.random.key(seed), 17)
    return {
        "tokens": gaussian(seeds[0], (IMAGES, SEQ_LEN, D), 1.0, 6.0, ((0, 8), (1, 4))),
        "lengths": draw_lengths(jax.random.fold_in(seeds[16], 71), 0),
        "ln1_gain": jnp.clip(1.0 + 0.1 * jax.random.normal(seeds[2], (D,), jnp.float32), 0.5, 1.5).astype(jnp.bfloat16),
        "ln1_bias": gaussian(seeds[3], (D,), 0.5, 3.0, ((0, 8),)),
        "qkv_weight": draw_qkv_weight(jax.random.fold_in(seeds[16], 71), 0),
        "q_bias": gaussian(seeds[5], (D,), 0.5, 3.0, ((0, 8),)),
        "v_bias": gaussian(seeds[6], (D,), 0.5, 3.0, ((0, 8),)),
        "out_weight": gaussian(seeds[7], (D, D), (max(D // 256, 1)) ** -0.5, 3.0, ((0, 8),)),
        "out_bias": gaussian(seeds[8], (D,), 0.5, 3.0, ((0, 8),)),
        "ln2_gain": jnp.clip(1.0 + 0.1 * jax.random.normal(seeds[9], (D,), jnp.float32), 0.5, 1.5).astype(jnp.bfloat16),
        "ln2_bias": gaussian(seeds[10], (D,), 0.5, 3.0, ((0, 8),)),
        "up_weight": gaussian(seeds[11], (D, FF), D ** -0.5, 0.1875, ((0, 8),)),
        "up_bias": gaussian(seeds[12], (FF,), 0.5, 3.0, ((0, 8),)),
        "down_weight": gaussian(seeds[13], (FF, D), FF ** -0.5, 0.09375, ((0, 8),)),
        "down_bias": gaussian(seeds[14], (D,), 0.5, 3.0, ((0, 8),)),
        "cotangent": gaussian(seeds[15], (IMAGES, SEQ_LEN, D), 1.0, 6.0, ((0, 8), (1, 4))),
    }


@jax.custom_vjp
def low(v):
    return lax.optimization_barrier(v.astype(jnp.bfloat16)).astype(jnp.float32)

@jax.custom_vjp
def low_back(v):
    return v

def low_keep(v):
    return (low(v), None)

def low_pass(kept, grad):
    return (grad,)

def back_keep(v):
    return (v, None)

def back_low(kept, grad):
    return (low(grad),)
low.defvjp(low_keep, low_pass)
low_back.defvjp(back_keep, back_low)

def norm_rows(values, gain_vec, shift_vec):
    center = values - lax.optimization_barrier(jnp.mean(values, axis=-1, keepdims=True))
    spread = lax.optimization_barrier(jnp.mean(center * center, axis=-1, keepdims=True))
    return center * lax.rsqrt(spread + 1e-06) * gain_vec + shift_vec

def one_image(params, picture, length):
    ln1_gain, ln1_bias, qkv_weight, q_bias, v_bias, out_weight, out_bias, ln2_gain, ln2_bias, up_weight, up_bias, down_weight, down_bias = params
    highest = lax.Precision.HIGHEST
    normed = low(norm_rows(picture, ln1_gain, ln1_bias))
    joined_bias = jnp.concatenate([q_bias, jnp.zeros_like(q_bias), v_bias])
    project = low(low_back(jnp.dot(normed, qkv_weight, precision=highest) + joined_bias))
    queries = project[:, :D].reshape(SEQ_LEN, HEADS, HEAD_DIM)
    keys_all = project[:, D:2 * D].reshape(SEQ_LEN, HEADS, HEAD_DIM)
    values_all = project[:, 2 * D:].reshape(SEQ_LEN, HEADS, HEAD_DIM)
    raw_scores = low_back(jnp.einsum('qhd,khd->hqk', queries, keys_all, precision=highest))
    allowed = jnp.arange(SEQ_LEN) < length
    scores = jnp.where(allowed[None, None, :], raw_scores * HEAD_DIM ** (-0.5), -1e+30)
    weights = low(jax.nn.softmax(scores, axis=-1))
    context = jnp.einsum('hqk,khd->qhd', weights, values_all, precision=highest).reshape(SEQ_LEN, D)
    context = low(low_back(context))
    branch = low_back(jnp.dot(context, out_weight, precision=highest) + out_bias)
    middle = picture + branch
    normed_two = low(norm_rows(middle, ln2_gain, ln2_bias))
    before = low_back(jnp.dot(normed_two, up_weight, precision=highest) + up_bias)
    hidden = low(jax.nn.gelu(before, approximate=False))
    feed_out = low_back(jnp.dot(hidden, down_weight, precision=highest) + down_bias)
    return middle + feed_out

def reference(tokens, lengths, ln1_gain, ln1_bias, qkv_weight, q_bias, v_bias, out_weight, out_bias, ln2_gain, ln2_bias, up_weight, up_bias, down_weight, down_bias, cotangent):
    params = tuple((weight_arg.astype(jnp.float32) for weight_arg in (ln1_gain, ln1_bias, qkv_weight, q_bias, v_bias, out_weight, out_bias, ln2_gain, ln2_bias, up_weight, up_bias, down_weight, down_bias)))
    inputs = tokens.astype(jnp.float32)

    def forward(inputs, params):
        per_image = jax.checkpoint(partial(one_image, params))
        return lax.map(lambda element: per_image(element[0], element[1]), (inputs, lengths))
    output, pullback = jax.vjp(forward, inputs, params)
    grad_inputs, grads = pullback(cotangent.astype(jnp.float32))
    return (output.astype(jnp.bfloat16), grad_inputs.astype(jnp.bfloat16), grads[0], grads[1], grads[2], grads[3], grads[4], grads[5], grads[6], grads[7], grads[8], grads[9], grads[10], grads[11], grads[12])
```

```python
import functools
import math

import jax
import jax.numpy as jnp
from jax import lax
from jax.experimental import pallas as pl
from jax.experimental.pallas import tpu as pltpu
from jax.sharding import PartitionSpec as P

HEAD_DIM = 64
BF = jnp.bfloat16
F32 = jnp.float32
MESH = pl.DeviceIdType.MESH


def dot_nn(left, right):
    return lax.dot_general(left, right, (((1,), (0,)), ((), ())), preferred_element_type=F32)


def dot_nt(left, right):
    return lax.dot_general(left, right, (((1,), (1,)), ((), ())), preferred_element_type=F32)


def dot_tn(left, right):
    return lax.dot_general(left, right, (((0,), (0,)), ((), ())), preferred_element_type=F32)


def unit_rows(values):
    center = values - jnp.mean(values, axis=-1, keepdims=True)
    rate = lax.rsqrt(jnp.mean(center * center, axis=-1, keepdims=True) + 1e-6)
    return center * rate, rate


def norm_pull(grad, gain, unit, rate):
    scaled = grad * gain
    return rate * (
        scaled
        - jnp.mean(scaled, axis=-1, keepdims=True)
        - unit * jnp.mean(scaled * unit, axis=-1, keepdims=True)
    )


def layer_kernel(
    z,
    tok, cot, mask, sm_in, qkv_in, out_in, up_in, dn_in,
    o_out, o_tok, o_qkv, o_ow, o_up, o_dn, o_sm,
    xg, cg, nrm, ctx, n2, hid, gbf, pq, wqkv, wout, wup, wdn, smg, vec, gvec, lse, mid, gmid,
    gctx, dqkv, dkt, dvt, gpart, gown, grecv, opart, oown, orecv,
    dw_qkv, dw_out, dw_up, dw_dn, dw_sm, xr_qkv, xr_out, xr_up, xr_dn, xr_sm,
    zr_qkv, zr_out, zr_up, zr_dn, zr_sm,
    loc_sem, ag_zs, ag_zr, ag_xs, ag_xr, sq_s, sq_r, rs_s, rs_r, fx_s, fx_r, fz_s, fz_r,
):
    D, T, TP, R, A, w, wf, HP = z["D"], z["T"], z["TP"], z["R"], z["A"], z["w"], z["wf"], z["HP"]
    N, DH, LB, g = 2 * A, D // 4, D // 128, z["g"]
    half = D // 2
    s = lax.axis_index("seq")
    f = lax.axis_index("fsdp")
    y, c = lax.div(s, 2), lax.rem(s, 2)
    a, b = lax.div(f, 2), lax.rem(f, 2)
    s_core, s_y, s_diag = y * 2 + 1 - c, (1 - y) * 2 + c, (1 - y) * 2 + 1 - c
    f_x = a * 2 + 1 - b
    to_core, to_y, to_x = {"seq": s_core}, {"seq": s_y}, {"fsdp": f_x}

    def up_z(d):
        return lax.rem(a + d, A)

    def from_z(d):
        return lax.rem(a - d + A, A)

    started = []

    def send(src, dst, ssem, rsem, dev, keep=True, kind=None):
        copy = pltpu.make_async_remote_copy(
            src_ref=src, dst_ref=dst, send_sem=ssem, recv_sem=rsem, device_id=dev, device_id_type=MESH
        )
        copy.start()
        if keep:
            started.append((copy, kind))

    def arrive(dst, rsem, dev):
        pltpu.make_async_remote_copy(
            src_ref=dst, dst_ref=dst, send_sem=rsem, recv_sem=rsem, device_id=dev, device_id_type=MESH
        ).wait_recv()

    def rows_of(k, size):
        return pl.ds(pl.multiple_of(k * size, size), size)

    core_cols = pl.ds(pl.multiple_of(c * half, half), half)
    blocks = {
        0: lambda k: smg.at[k],
        1: lambda k: wqkv.at[rows_of(k, w)],
        2: lambda k: wout.at[rows_of(k, w), core_cols],
        3: lambda k: wup.at[rows_of(k, w)],
        4: lambda k: wdn.at[rows_of(k, wf)],
    }

    def ag_z(m):
        for d in range(1, A):
            send(blocks[m](f), blocks[m](f), ag_zs.at[m, d - 1], ag_zr.at[m, d - 1], {"fsdp": up_z(d) * 2 + b})

    def ag_x(m):
        send(blocks[m](f), blocks[m](f), ag_xs.at[m, 0], ag_xr.at[m, 0], to_x)

    def ag_relay(m):
        for d in range(1, A):
            k = from_z(d) * 2 + b
            arrive(blocks[m](k), ag_zr.at[m, d - 1], to_x)
            send(blocks[m](k), blocks[m](k), ag_xs.at[m, d], ag_xr.at[m, d], to_x)

    def ag_wait(m):
        for d in range(A):
            arrive(blocks[m](from_z(d) * 2 + 1 - b), ag_xr.at[m, d], to_x)

    def sq_send(kind, ref):
        send(ref(s), ref(s), sq_s.at[kind, 0], sq_r.at[kind, 0], to_core, kind=kind)
        send(ref(s), ref(s), sq_s.at[kind, 1], sq_r.at[kind, 1], to_y, kind=kind)

    def sq_core(kind, ref):
        arrive(ref(s_core), sq_r.at[kind, 0], to_core)

    def sq_relay(kind, ref):
        arrive(ref(s_y), sq_r.at[kind, 1], to_y)
        send(ref(s_y), ref(s_y), sq_s.at[kind, 2], sq_r.at[kind, 2], to_core, kind=kind)

    def sq_diag(kind, ref):
        arrive(ref(s_diag), sq_r.at[kind, 2], to_core)

    def x_slot(k):
        return xg.at[k]

    def c_slot(k):
        return cg.at[k]

    def ctx_slot(hp):
        return lambda k: ctx.at[k, :, hp * 128 : hp * 128 + 128]

    KX, KC, KG, KO, KCTX, KFIN = 0, 1, 2, 3, 4, 4 + HP

    def order(i):
        hb, lb = lax.div(3 - i, 2), lax.rem(3 - i, 2)
        return lax.rem(y + hb, 2) * 2 + lax.rem(c + lb, 2)

    def seq_stage(i, kind, part, own, recv, value):
        @pl.when(i < 3)
        def _():
            part[jnp.minimum(i, 2)] = value.astype(BF)

        @pl.when(i == 0)
        def _():
            send(part.at[0], recv.at[0], rs_s.at[kind, 0], rs_r.at[kind, 0], to_core, keep=False)

        @pl.when(i == 1)
        def _():
            arrive(recv.at[0], rs_r.at[kind, 0], to_core)
            part[1] = (part[1].astype(F32) + recv[0].astype(F32)).astype(BF)
            send(part.at[1], recv.at[1], rs_s.at[kind, 1], rs_r.at[kind, 1], to_y, keep=False)

        @pl.when(i == 2)
        def _():
            send(part.at[2], recv.at[2], rs_s.at[kind, 2], rs_r.at[kind, 2], to_core, keep=False)

        @pl.when(i == 3)
        def _():
            own[...] = value

    def seq_sent(kind, part):
        for j in range(3):
            pltpu.make_async_remote_copy(
                src_ref=part.at[j], dst_ref=part.at[j], send_sem=rs_s.at[kind, j], recv_sem=rs_r.at[kind, j],
                device_id=to_core, device_id_type=MESH,
            ).wait_send()

    def seq_total(kind, own, recv):
        arrive(recv.at[2], rs_r.at[kind, 2], to_core)
        arrive(recv.at[1], rs_r.at[kind, 1], to_y)
        return own[...] + recv[2].astype(F32) + recv[1].astype(F32)

    grads = {0: (dw_sm, xr_sm, zr_sm, o_sm), 1: (dw_dn, xr_dn, zr_dn, o_dn), 2: (dw_up, xr_up, zr_up, o_up), 3: (dw_out, xr_out, zr_out, o_ow)}
    for hp in range(HP):
        grads[4 + hp] = (dw_qkv.at[hp], xr_qkv.at[hp], zr_qkv.at[hp], o_qkv.at[hp])

    def rs_x(m):
        dw, xr, zr, out = grads[m]
        send(dw.at[:, 1 - b], xr, fx_s.at[m], fx_r.at[m], to_x)

    def rs_mid(m):
        dw, xr, zr, out = grads[m]
        arrive(xr, fx_r.at[m], to_x)
        dw[:, b] = (dw[:, b].astype(F32) + xr[...].astype(F32)).astype(dw.dtype)
        for d in range(1, A):
            k = up_z(d)
            send(dw.at[k, b], zr.at[d - 1], fz_s.at[m, d - 1], fz_r.at[m, d - 1], {"fsdp": k * 2 + b})

    def fin_slot(m):
        return lambda k: grads[m][3].at[k]

    def rs_fin(m):
        dw, xr, zr, out = grads[m]
        total = dw[a, b].astype(F32)
        for d in range(1, A):
            arrive(zr.at[d - 1], fz_r.at[m, d - 1], {"fsdp": from_z(d) * 2 + b})
            total = total + zr[d - 1].astype(F32)
        out[s] = total.astype(out.dtype)
        sq_send(KFIN + m, fin_slot(m))

    local = []

    def bring(src, dst):
        copy = pltpu.make_async_copy(src, dst, loc_sem.at[len(local)])
        copy.start()
        local.append(copy)

    bring(sm_in, smg.at[f])
    for hp in range(HP):
        for part in range(3):
            cols = pl.ds(pl.multiple_of(part * D + s * DH + hp * 128, 128), 128)
            lo = hp * 384 + part * 128
            bring(qkv_in.at[:, cols], wqkv.at[rows_of(f, w), lo : lo + 128])
    bring(out_in.at[:, core_cols], wout.at[rows_of(f, w), core_cols])
    if z["up_whole"]:
        for k in range(N):
            cols = pl.ds(pl.multiple_of((k * 4 + s) * wf, wf), wf)
            bring(up_in.at[:, cols], wup.at[rows_of(f, w), k * wf : (k + 1) * wf])
    else:
        bring(up_in, wup.at[rows_of(f, w)])
    bring(dn_in.at[rows_of(s, wf)], wdn.at[rows_of(f, wf)])

    def padded(ref):
        return jnp.concatenate([ref[...].astype(F32), jnp.zeros((TP - T, D), F32)], axis=0)

    xg[s] = padded(tok).astype(BF)
    cg[s] = padded(cot).astype(BF)
    gvec[...] = jnp.zeros_like(gvec)

    barrier = pltpu.get_barrier_semaphore()
    peers = [to_core, to_y, {"seq": s_diag}, to_x] + [{"fsdp": up_z(d) * 2 + b} for d in range(1, A)]
    for dev in peers:
        pl.semaphore_signal(barrier, inc=1, device_id=dev, device_id_type=MESH)
    for copy in local:
        copy.wait()
    pl.semaphore_wait(barrier, len(peers))

    ag_z(0)
    ag_x(0)
    sq_send(KX, x_slot)
    ag_z(1)
    ag_x(1)
    ag_z(2)
    ag_z(3)
    ag_z(4)
    ag_relay(0)
    ag_wait(0)
    for j in range(LB):
        piece = smg[j * g].astype(F32)
        for i in range(1, g):
            piece = piece + smg[j * g + i].astype(F32)
        vec[:, j * 128 : (j + 1) * 128] = piece

    def row(k):
        return vec[k : k + 1, :]

    def first_norm(k):
        unit, _ = unit_rows(xg[k].astype(F32))
        nrm[k] = (unit * row(0) + row(1)).astype(BF)

    first_norm(s)
    sq_core(KX, x_slot)
    first_norm(s_core)
    sq_relay(KX, x_slot)
    sq_send(KC, c_slot)
    first_norm(s_y)
    ag_relay(1)
    ag_x(2)
    sq_diag(KX, x_slot)
    first_norm(s_diag)
    ag_wait(1)

    pieces = []
    for hp in range(HP):
        cols = pl.ds(pl.multiple_of(s * DH + hp * 128, 128), 128)
        pieces += [vec[2:3, cols], jnp.zeros((1, 128), F32), vec[3:4, cols]]
    proj_bias = jnp.concatenate(pieces, axis=1)
    lanes = lax.broadcasted_iota(jnp.int32, (1, HP * 384), 1)
    proj_scale = jnp.where(lax.rem(lanes, 384) < 128, HEAD_DIM ** (-0.5), 1.0).astype(F32)

    @pl.loop(0, 4)
    def _(k):
        value = dot_nn(nrm[k], wqkv[...]) + proj_bias
        pq[k] = (value * proj_scale).astype(BF)

    flat = pq.reshape(R, HP * 384)
    lane = lax.broadcasted_iota(jnp.int32, (1, 128), 1)
    first = (lane < HEAD_DIM).astype(F32)
    picks = (first.astype(BF), (1.0 - first).astype(BF))

    def tiles(fn):
        full = R // 256

        @pl.loop(0, full)
        def _(i):
            fn(pl.ds(pl.multiple_of(i * 256, 256), 256), 256)

        if R % 256:
            fn(pl.ds(full * 256, R % 256), R % 256)

    ctx_rows = ctx.reshape(4 * R, DH)

    def forward_tile(hp, rows, count, start):
        lo = hp * 384
        query = flat[rows, lo : lo + 128]
        keys = flat[:, lo + 128 : lo + 256]
        vals = flat[:, lo + 256 : lo + 384]
        both = []
        for h in range(2):
            scores = dot_nt(query * picks[h], keys) + mask[...]
            top = jnp.max(scores, axis=-1, keepdims=True)
            grown = jnp.exp(scores - top)
            total = jnp.sum(grown, axis=-1, keepdims=True)
            lse[hp * 2 + h, rows, :] = top + jnp.log(total)
            both.append(dot_nn((grown * (1.0 / total)).astype(BF), vals))
        here = jnp.where(lane < HEAD_DIM, both[0], both[1]).astype(BF)
        ctx_rows[pl.ds(pl.multiple_of(s * R + start, 16), count), hp * 128 : hp * 128 + 128] = here

    def attend_forward(hp):
        full = R // 256

        @pl.loop(0, full)
        def _(i):
            forward_tile(hp, pl.ds(pl.multiple_of(i * 256, 256), 256), 256, i * 256)

        if R % 256:
            forward_tile(hp, pl.ds(full * 256, R % 256), R % 256, full * 256)

    for hp in range(HP):
        attend_forward(hp)
        sq_send(KCTX + hp, ctx_slot(hp))
        if hp == 0:
            ag_relay(2)
            sq_relay(KC, c_slot)
    ag_x(3)
    ag_wait(2)
    send(wout.at[:, core_cols], wout.at[:, core_cols], sq_s.at[KO, 0], sq_r.at[KO, 0], to_core)
    for hp in range(HP):
        sq_core(KCTX + hp, ctx_slot(hp))
        sq_relay(KCTX + hp, ctx_slot(hp))
    ag_relay(3)
    ag_x(4)
    other_cols = pl.ds(pl.multiple_of((1 - c) * half, half), half)
    arrive(wout.at[:, other_cols], sq_r.at[KO, 0], to_core)
    for hp in range(HP):
        sq_diag(KCTX + hp, ctx_slot(hp))

    @pl.loop(0, 4)
    def _(i):
        k = order(i)
        rows = pl.ds(pl.multiple_of(k * TP, 16), TP)
        joined = jnp.concatenate([ctx[j, rows, :] for j in range(4)], axis=1)
        value = xg[k].astype(F32) + dot_nn(joined, wout[...]) + row(4)
        unit, _ = unit_rows(value)
        n2[k] = (unit * row(5) + row(6)).astype(BF)

        @pl.when(i == 3)
        def _():
            mid[...] = value

    for copy in [copy for copy, kind in started if kind == KX]:
        copy.wait_send()
    ag_relay(4)
    sq_core(KC, c_slot)
    sq_diag(KC, c_slot)
    ag_wait(3)
    ag_wait(4)

    @pl.loop(0, 4)
    def _(i):
        k = order(i)
        before = dot_nn(n2[k], wup[...]) + row(8)
        cdf = 0.5 + 0.5 * lax.erf(before * (0.5**0.5))
        slope = cdf + before * (jnp.exp(before * before * -0.5) * (1.0 / math.sqrt(2.0 * math.pi)))
        hid[k] = (before * cdf).astype(BF)
        grad = (dot_nt(cg[k], wdn[...]) * slope).astype(BF)
        gbf[k] = grad
        gvec[8:9, :] += jnp.sum(grad.astype(F32), axis=0, keepdims=True)
        seq_stage(i, 0, gpart, gown, grecv, dot_nt(grad, wup[...]))
        seq_stage(i, 1, opart, oown, orecv, dot_nn(hid[k], wdn[...]))

    gn = seq_total(0, gown, grecv)
    seq_sent(0, gpart)
    unit, rate = unit_rows(mid[...])
    gvec[5:6, :] = jnp.sum(gn * unit, axis=0, keepdims=True)
    gvec[6:7, :] = jnp.sum(gn, axis=0, keepdims=True)
    c_own = cg[s].astype(F32)
    gvec[7:8, :] = jnp.sum(c_own, axis=0, keepdims=True)
    gm = c_own + norm_pull(gn, row(5), unit, rate)
    gmid[...] = gm
    branch = gm.astype(BF)
    gvec[4:5, :] = jnp.sum(branch.astype(F32), axis=0, keepdims=True)
    xg[s] = branch
    sq_send(KG, x_slot)

    def weight_grad(left, right, dw, size, cols=None):
        per = max(256 // size, 1)

        @pl.loop(0, dw.shape[0] * 2 // per)
        def _(i):
            lo = pl.ds(pl.multiple_of(i * per * size, per * size), per * size)
            value = dot_tn(left[:, lo], right).astype(BF)
            for j in range(per):
                k = i * per + j
                dw[lax.div(k, 2), lax.rem(k, 2)] = value[j * size : (j + 1) * size]

    weight_grad(hid.reshape(R, D), cg.reshape(R, D)[...], dw_dn, wf)
    rs_x(1)
    weight_grad(n2.reshape(R, D), gbf.reshape(R, D)[...], dw_up, w)
    rs_x(2)
    out_total = seq_total(1, oown, orecv)
    o_out[...] = (mid[...] + out_total + row(7))[:T].astype(BF)
    sq_core(KG, x_slot)
    sq_relay(KG, x_slot)
    rs_mid(1)
    sq_diag(KG, x_slot)

    @pl.loop(0, 4)
    def _(k):
        mine = wout[pl.ds(pl.multiple_of(s * DH, DH), DH), :]
        gctx[k] = dot_nt(xg[k], mine).astype(BF)

    own_cols = pl.ds(pl.multiple_of(s * DH, DH), DH)
    right = xg.reshape(R, D)[:, own_cols]
    for j in range(4):
        value = dot_tn(ctx[j], right).astype(BF)
        for i in range(DH // w):
            k = j * (DH // w) + i
            dw_out[k // 2, k % 2] = value[i * w : (i + 1) * w]
    rs_x(3)
    rs_mid(2)

    flat_g = gctx.reshape(R, DH)
    flat_d = dqkv.reshape(R, HP * 384)

    def backward_tile(hp, rows, count):
        lo = hp * 384
        query = flat[rows, lo : lo + 128]
        keys = flat[:, lo + 128 : lo + 256]
        vals = flat[:, lo + 256 : lo + 384]
        grad = flat_g[rows, hp * 128 : hp * 128 + 128]
        both = []
        for h in range(2):
            qh, gh = query * picks[h], grad * picks[h]
            probs = jnp.exp(dot_nt(qh, keys) + mask[...] - lse[hp * 2 + h, rows, :])
            dp = dot_nt(gh, vals)
            inner = jnp.sum(probs * dp, axis=-1, keepdims=True)
            ds = (probs * (dp - inner)).astype(BF)
            both.append(dot_nn(ds, keys))
            dkt[...] += dot_tn(qh, ds)
            dvt[...] += dot_tn(gh, probs.astype(BF))
        dq = jnp.where(lane < HEAD_DIM, both[0], both[1]) * HEAD_DIM ** (-0.5)
        flat_d[rows, lo : lo + 128] = dq.astype(BF)

    for hp in range(HP):
        lo = hp * 384
        dkt[...] = jnp.zeros_like(dkt)
        dvt[...] = jnp.zeros_like(dvt)
        tiles(functools.partial(backward_tile, hp))
        flat_d[:, lo + 128 : lo + 256] = dkt[...].T.astype(BF)
        flat_d[:, lo + 256 : lo + 384] = dvt[...].T.astype(BF)
        weight_grad(nrm.reshape(R, D), flat_d[:, lo : lo + 384], dw_qkv.at[hp], w)
        rs_x(4 + hp)
        if hp == 0:
            rs_fin(1)
            rs_fin(2)
            rs_mid(3)
        off = pl.ds(pl.multiple_of(s * DH + hp * 128, 128), 128)
        gvec[2:3, off] = jnp.sum(flat_d[:, lo : lo + 128].astype(F32), axis=0, keepdims=True)
        gvec[3:4, off] = jnp.sum(flat_d[:, lo + 256 : lo + 384].astype(F32), axis=0, keepdims=True)

    @pl.loop(0, 4)
    def _(i):
        seq_stage(i, 2, gpart, gown, grecv, dot_nt(dqkv[order(i)], wqkv[...]))

    for hp in range(HP):
        rs_mid(4 + hp)
    rs_fin(3)
    for m in (1, 2, 3):
        sq_relay(KFIN + m, fin_slot(m))
    gn = seq_total(2, gown, grecv)
    unit, rate = unit_rows(padded(tok))
    gvec[0:1, :] = jnp.sum(gn * unit, axis=0, keepdims=True)
    gvec[1:2, :] = jnp.sum(gn, axis=0, keepdims=True)
    for k in range(N):
        j = k // g
        dw_sm[k // 2, k % 2] = gvec[:, j * 128 : (j + 1) * 128]
    rs_x(0)
    o_tok[...] = (gmid[...] + norm_pull(gn, row(0), unit, rate))[:T].astype(BF)
    rs_mid(0)
    for hp in range(HP):
        rs_fin(4 + hp)
    rs_fin(0)
    rest = [4 + hp for hp in range(HP)] + [0]
    for m in rest:
        sq_relay(KFIN + m, fin_slot(m))
    for m in [1, 2, 3] + rest:
        sq_core(KFIN + m, fin_slot(m))
        sq_diag(KFIN + m, fin_slot(m))
    for copy, kind in started:
        if kind != KX:
            copy.wait_send()
    for kind in (1, 2):
        seq_sent(kind, opart if kind == 1 else gpart)


def make_body(mesh):
    N = mesh.shape["fsdp"]
    A = N // 2

    def body(
        tokens, lengths, ln1_gain, ln1_bias, qkv_weight, q_bias, v_bias, out_weight, out_bias,
        ln2_gain, ln2_bias, up_weight, up_bias, down_weight, down_bias, cotangent,
    ):
        _, T, D = tokens.shape
        w, FF = D // N, up_weight.shape[1]
        wf = FF // (4 * N)
        TP = -(-T // 16) * 16
        R = 4 * TP
        DH = D // 4
        HP = DH // 128
        FQ = FF // 4
        assert FQ == D and wf == w
        g = max(128 // w, 1)
        s = lax.axis_index("seq")
        f = lax.axis_index("fsdp")
        up_whole = wf % 128 == 0
        ub = lax.dynamic_slice(up_bias, (s * wf,), (wf,))
        packed = jnp.stack([ln1_gain, ln1_bias, q_bias, v_bias, out_bias, ln2_gain, ln2_bias, down_bias, ub])
        if g == 1:
            small = jnp.pad(packed, ((0, 7), (0, 0)))
        else:
            small = lax.dynamic_update_slice(jnp.zeros((16, 128), BF), packed, (0, lax.rem(f, g) * w))
        if not up_whole:
            up_weight = lax.dynamic_index_in_dim(up_weight.reshape(w, N, 4, wf), s, 2, False).reshape(w, FQ)
        place = jnp.arange(R)
        slot, inside = place // TP, place % TP
        valid = (inside < T) & (slot * T + inside < lengths[0])
        mask = jnp.where(valid, 0.0, -1e30).astype(F32)[None, :]

        z = dict(D=D, T=T, TP=TP, R=R, A=A, w=w, wf=wf, HP=HP, g=g, up_whole=up_whole)
        vm = pltpu.VMEM
        A1 = max(A - 1, 1)
        M = 4 + HP
        C = 384
        scratch = [
            vm((4, TP, D), BF),
            vm((4, TP, D), BF),
            vm((4, TP, D), BF),
            vm((4, R, DH), BF),
            vm((4, TP, D), BF),
            vm((4, TP, D), BF),
            vm((4, TP, D), BF),
            vm((4, TP, HP * C), BF),
            vm((D, HP * C), BF),
            vm((D, D), BF),
            vm((D, FQ), BF),
            vm((FQ, D), BF),
            vm((N, 16, 128), BF),
            vm((16, D), F32),
            vm((16, D), F32),
            vm((HP * 2, R, 1), F32),
            vm((TP, D), F32),
            vm((TP, D), F32),
            vm((4, TP, DH), BF),
            vm((4, TP, HP * C), BF),
            vm((128, R), F32),
            vm((128, R), F32),
            vm((3, TP, D), BF), vm((TP, D), F32), vm((3, TP, D), BF),
            vm((3, TP, D), BF), vm((TP, D), F32), vm((3, TP, D), BF),
            vm((HP, A, 2, w, C), BF), vm((A, 2, w, DH), BF), vm((A, 2, w, FQ), BF), vm((A, 2, wf, D), BF), vm((A, 2, 16, 128), F32),
            vm((HP, A, w, C), BF), vm((A, w, DH), BF), vm((A, w, FQ), BF), vm((A, wf, D), BF), vm((A, 16, 128), F32),
            vm((HP, A1, w, C), BF), vm((A1, w, DH), BF), vm((A1, w, FQ), BF), vm((A1, wf, D), BF), vm((A1, 16, 128), F32),
        ]
        dma = pltpu.SemaphoreType.DMA
        scratch += [
            dma((3 + 3 * HP + (N if up_whole else 1),)),
            dma((5, A1)), dma((5, A1)), dma((5, A)), dma((5, A)),
            dma((4 + HP + M, 3)), dma((4 + HP + M, 3)),
            dma((3, 3)), dma((3, 3)),
            dma((M,)), dma((M,)), dma((M, A1)), dma((M, A1)),
        ]
        here = pl.BlockSpec(memory_space=pltpu.VMEM)
        there = pl.BlockSpec(memory_space=pl.ANY)
        out_shapes = [
            jax.ShapeDtypeStruct((T, D), BF),
            jax.ShapeDtypeStruct((T, D), BF),
            jax.ShapeDtypeStruct((HP, 4, w, C), BF),
            jax.ShapeDtypeStruct((4, w, DH), BF),
            jax.ShapeDtypeStruct((4, w, FQ), BF),
            jax.ShapeDtypeStruct((4, wf, D), BF),
            jax.ShapeDtypeStruct((4, 16, 128), F32),
        ]
        out, gtok, gq, go, gu, gd, gs = pl.pallas_call(
            functools.partial(layer_kernel, z),
            out_shape=out_shapes,
            in_specs=[here, here, here, there, there, there, there, there],
            out_specs=[here] * 7,
            scratch_shapes=scratch,
            compiler_params=pltpu.CompilerParams(
                collective_id=0, has_side_effects=True, vmem_limit_bytes=67_000_000
            ),
            name="layer",
        )(tokens[0], cotangent[0], mask, small, qkv_weight, out_weight, up_weight, down_weight)

        g_qkv = gq.reshape(HP, 4, w, 3, 128).transpose(2, 3, 1, 0, 4).reshape(w, 3 * D).astype(F32)
        g_out = go.transpose(1, 0, 2).reshape(w, D).astype(F32)
        g_up = gu.reshape(4, w, N, wf).transpose(1, 2, 0, 3).reshape(w, FF).astype(F32)
        g_down = gd.reshape(4 * wf, D).astype(F32)
        if g > 1:
            gs = lax.dynamic_slice(gs, (0, 0, lax.rem(f, g) * w), (4, 16, w))
        sums = jnp.sum(gs[:, :8], axis=0)
        return (
            out[None], gtok[None], sums[0], sums[1], g_qkv, sums[2], sums[3], g_out, sums[4],
            sums[5], sums[6], g_up, gs[:, 8].reshape(4 * wf), g_down, sums[7],
        )

    return body


def solution(mesh):
    row, mat, act = P("fsdp"), P("fsdp", None), P("fsdp", "seq", None)
    return jax.shard_map(
        make_body(mesh),
        mesh=mesh,
        in_specs=(act, row, row, row, mat, row, row, mat, row, row, row, mat, row, mat, row, act),
        out_specs=(act, act, row, row, mat, row, row, mat, row, row, row, mat, row, mat, row),
        check_vma=False,
    )
```

```python
import functools
import math

import jax
import jax.numpy as jnp
from jax import lax
from jax.experimental import pallas as pl
from jax.experimental.pallas import tpu as pltpu
from jax.sharding import PartitionSpec as P

HEAD_DIM = 64
BF = jnp.bfloat16
F32 = jnp.float32
MESH = pl.DeviceIdType.MESH


def dot_nn(left, right):
    return lax.dot_general(left, right, (((1,), (0,)), ((), ())), preferred_element_type=F32)


def dot_nt(left, right):
    return lax.dot_general(left, right, (((1,), (1,)), ((), ())), preferred_element_type=F32)


def dot_tn(left, right):
    return lax.dot_general(left, right, (((0,), (0,)), ((), ())), preferred_element_type=F32)


def unit_rows(values):
    center = values - jnp.mean(values, axis=-1, keepdims=True)
    rate = lax.rsqrt(jnp.mean(center * center, axis=-1, keepdims=True) + 1e-6)
    return center * rate, rate


def norm_pull(grad, gain, unit, rate):
    scaled = grad * gain
    return rate * (
        scaled
        - jnp.mean(scaled, axis=-1, keepdims=True)
        - unit * jnp.mean(scaled * unit, axis=-1, keepdims=True)
    )


def layer_kernel(
    z,
    tok, cot, mask, sm_in, qkv_in, out_in, up_in, dn_in,
    o_out, o_tok, o_qkv, o_ow, o_up, o_dn, o_sm,
    xg, cg, nrm, ctx, n2, hid, gbf, pq, wqkv, wout, wup, wdn, smg, vec, gvec, lse, mid, gmid,
    gctx, dqkv, dkt, dvt, gpart, gown, grecv, opart, oown, orecv,
    dw_qkv, dw_out, dw_up, dw_dn, dw_sm, rr_qkv, rr_out, rr_up, rr_dn, rr_sm,
    loc_sem, ag_s, ag_r, rg_s, rg_r, sq_s, sq_r, rs_s, rs_r, sa_s, sa_r, sg_s, sg_r,
):
    D, T, TP, R, A, w, wf, HP = z["D"], z["T"], z["TP"], z["R"], z["A"], z["w"], z["wf"], z["HP"]
    N, H, DH, LB, g = 2 * A, A, D // 4, D // 128, z["g"]
    s = lax.axis_index("seq")
    f = lax.axis_index("fsdp")
    y, c = lax.div(s, 2), lax.rem(s, 2)
    s_core, s_y, s_diag = y * 2 + 1 - c, (1 - y) * 2 + c, (1 - y) * 2 + 1 - c
    to_core, to_y = {"seq": s_core}, {"seq": s_y}

    odd = lax.rem(f, 2)
    place = (1 - odd) * lax.div(f, 2) + odd * (N - 1 - lax.div(f, 2))

    def at_place(q):
        late = lax.div(q, A)
        return (1 - late) * 2 * q + late * (2 * (N - 1 - q) + 1)

    def ahead(d):
        return at_place(lax.rem(place + d + N, N))

    to_ring = ({"fsdp": ahead(1)}, {"fsdp": ahead(-1)})

    def send(src, dst, ssem, rsem, dev):
        pltpu.make_async_remote_copy(
            src_ref=src, dst_ref=dst, send_sem=ssem, recv_sem=rsem, device_id=dev, device_id_type=MESH
        ).start()

    def arrive(dst, rsem, dev):
        pltpu.make_async_remote_copy(
            src_ref=dst, dst_ref=dst, send_sem=rsem, recv_sem=rsem, device_id=dev, device_id_type=MESH
        ).wait_recv()

    def sent(src, ssem, dev):
        pltpu.make_async_remote_copy(
            src_ref=src, dst_ref=src, send_sem=ssem, recv_sem=ssem, device_id=dev, device_id_type=MESH
        ).wait_send()

    def thirds(first, last):
        count = max(last - first, 0)
        cut = [first + (count * k) // 3 for k in range(4)]
        return [range(cut[k], cut[k + 1]) for k in range(3)]

    quarter = pl.ds(pl.multiple_of(s * DH, DH), DH)

    def rows_of(k, size, half=None):
        if half is None:
            return pl.ds(pl.multiple_of(k * size, size), size)
        return pl.ds(pl.multiple_of(k * size + half * (size // 2), size // 2), size // 2)

    blocks = {
        0: lambda k, half=None: wqkv.at[rows_of(k, w, half)],
        1: lambda k, half=None: wout.at[rows_of(k, w, half), quarter],
        2: lambda k, half=None: wup.at[rows_of(k, w, half)],
        3: lambda k, half=None: wdn.at[rows_of(k, wf, half)],
    }

    def ag_block(m, way, d, back):
        k = ahead(-back if way == 0 else back)
        return blocks[m](k, way if d == H else None)

    def ag_own(m):
        for way in range(2):
            ref = ag_block(m, way, 1, 0)
            send(ref, ref, ag_s.at[m, way, 0], ag_r.at[m, way, 0], to_ring[way])

    def ag_take(m, d):
        for way in range(2):
            arrive(ag_block(m, way, d, d), ag_r.at[m, way, d - 1], to_ring[way])
            if d < H:
                ref = ag_block(m, way, d + 1, d)
                send(ref, ref, ag_s.at[m, way, d], ag_r.at[m, way, d], to_ring[way])

    def ag_fwd(m, third):
        for d in thirds(1, H)[third]:
            ag_take(m, d)

    def ag_last(m):
        ag_take(m, H)

    def ag_sent(m):
        for way in range(2):
            for d in range(1, H + 1):
                sent(ag_block(m, way, d, d - 1), ag_s.at[m, way, d - 1], to_ring[way])

    def sq_send(kind, ref):
        send(ref(s), ref(s), sq_s.at[kind, 0], sq_r.at[kind, 0], to_core)
        send(ref(s), ref(s), sq_s.at[kind, 1], sq_r.at[kind, 1], to_y)

    def sq_core(kind, ref):
        arrive(ref(s_core), sq_r.at[kind, 0], to_core)

    def sq_relay(kind, ref):
        arrive(ref(s_y), sq_r.at[kind, 1], to_y)
        send(ref(s_y), ref(s_y), sq_s.at[kind, 2], sq_r.at[kind, 2], to_core)

    def sq_diag(kind, ref):
        arrive(ref(s_diag), sq_r.at[kind, 2], to_core)

    def sq_sent(kind, ref):
        sent(ref(s), sq_s.at[kind, 0], to_core)
        sent(ref(s), sq_s.at[kind, 1], to_y)
        sent(ref(s_y), sq_s.at[kind, 2], to_core)

    def x_slot(k):
        return xg.at[k]

    def c_slot(k):
        return cg.at[k]

    def out_slot(k):
        return wout.at[:, pl.ds(pl.multiple_of(k * DH, DH), DH)]

    def ctx_slot(hp):
        return lambda k: ctx.at[k, :, hp * 128 : hp * 128 + 128]

    KX, KC, KG, KO, KCTX, KFIN = 0, 1, 2, 3, 4, 4 + HP

    def order(i):
        hb, lb = lax.div(3 - i, 2), lax.rem(3 - i, 2)
        return lax.rem(y + hb, 2) * 2 + lax.rem(c + lb, 2)

    def seq_stage(i, kind, part, own, recv, value):
        @pl.when(i < 3)
        def _():
            part[jnp.minimum(i, 2)] = value.astype(BF)

        @pl.when(i == 0)
        def _():
            send(part.at[0], recv.at[0], rs_s.at[kind, 0], rs_r.at[kind, 0], to_core)

        @pl.when(i == 1)
        def _():
            arrive(recv.at[0], rs_r.at[kind, 0], to_core)
            part[1] = (part[1].astype(F32) + recv[0].astype(F32)).astype(BF)
            send(part.at[1], recv.at[1], rs_s.at[kind, 1], rs_r.at[kind, 1], to_y)

        @pl.when(i == 2)
        def _():
            send(part.at[2], recv.at[2], rs_s.at[kind, 2], rs_r.at[kind, 2], to_core)

        @pl.when(i == 3)
        def _():
            own[...] = value

    def seq_sent(kind, part):
        for j in range(3):
            sent(part.at[j], rs_s.at[kind, j], to_core)

    def seq_total(kind, own, recv):
        arrive(recv.at[2], rs_r.at[kind, 2], to_core)
        arrive(recv.at[1], rs_r.at[kind, 1], to_y)
        return own[...] + recv[2].astype(F32) + recv[1].astype(F32)

    grads = {0: (dw_dn, rr_dn, o_dn), 1: (dw_up, rr_up, o_up), 2: (dw_out, rr_out, o_ow)}
    for hp in range(HP):
        grads[3 + hp] = (dw_qkv.at[hp], rr_qkv.at[hp], o_qkv.at[hp])
    MG = 3 + HP

    def rg_rows(m, way, j):
        size = grads[m][0].shape[1]
        return slice(way * (size // 2), (way + 1) * (size // 2)) if j == 0 else slice(0, size)

    def rg_owner(way, j):
        return ahead(H - j if way == 0 else j - H)

    def rg_src(m, way, j):
        return grads[m][0].at[rg_owner(way, j), rg_rows(m, way, j)]

    def rg_send(m, way, j):
        dst = grads[m][1].at[way, j, rg_rows(m, way, j)]
        send(rg_src(m, way, j), dst, rg_s.at[m, way, j], rg_r.at[m, way, j], to_ring[way])

    def rg_arrive(m, way, j):
        arrive(grads[m][1].at[way, j, rg_rows(m, way, j)], rg_r.at[m, way, j], to_ring[way])

    def rg_own(m):
        for way in range(2):
            rg_send(m, way, 0)

    def rg_fwd(m, third):
        dw, rr, _ = grads[m]
        for j in thirds(1, H)[third]:
            for way in range(2):
                rows = rg_rows(m, way, j - 1)
                owner = rg_owner(way, j)
                rg_arrive(m, way, j - 1)
                dw[owner, rows] = (dw[owner, rows].astype(F32) + rr[way, j - 1, rows].astype(F32)).astype(dw.dtype)
                rg_send(m, way, j)

    def fin_slot(m):
        return lambda k: grads[m][2].at[k]

    def rg_fin(m):
        dw, rr, out = grads[m]
        total = dw[f].astype(F32)
        for way in range(2):
            rg_arrive(m, way, H - 1)
            total = total + rr[way, H - 1].astype(F32)
        out[s] = total.astype(out.dtype)
        sq_send(KFIN + m, fin_slot(m))

    def rg_sent(m):
        for way in range(2):
            for j in range(H):
                sent(rg_src(m, way, j), rg_s.at[m, way, j], to_ring[way])

    def other(d):
        return lax.rem(f + d, N)

    local = []

    def bring(src, dst):
        copy = pltpu.make_async_copy(src, dst, loc_sem.at[len(local)])
        copy.start()
        local.append(copy)

    bring(sm_in, smg.at[f])
    for hp in range(HP):
        for part in range(3):
            cols = pl.ds(pl.multiple_of(part * D + s * DH + hp * 128, 128), 128)
            lo = hp * 384 + part * 128
            bring(qkv_in.at[:, cols], wqkv.at[rows_of(f, w), lo : lo + 128])
    bring(out_in.at[:, quarter], wout.at[rows_of(f, w), quarter])
    if z["up_whole"]:
        for k in range(N):
            cols = pl.ds(pl.multiple_of((k * 4 + s) * wf, wf), wf)
            bring(up_in.at[:, cols], wup.at[rows_of(f, w), k * wf : (k + 1) * wf])
    else:
        bring(up_in, wup.at[rows_of(f, w)])
    bring(dn_in.at[rows_of(s, wf)], wdn.at[rows_of(f, wf)])

    def padded(ref):
        return jnp.concatenate([ref[...].astype(F32), jnp.zeros((TP - T, D), F32)], axis=0)

    barrier = pltpu.get_barrier_semaphore()
    peers = [to_core, to_y] + [{"fsdp": other(d)} for d in range(1, N)]
    for dev in peers:
        pl.semaphore_signal(barrier, inc=1, device_id=dev, device_id_type=MESH)
    xg[s] = padded(tok).astype(BF)
    cg[s] = padded(cot).astype(BF)
    gvec[...] = jnp.zeros_like(gvec)
    for copy in local:
        copy.wait()
    pl.semaphore_wait(barrier, len(peers))

    for d in range(1, N):
        send(smg.at[f], smg.at[f], sa_s.at[d - 1], sa_r.at[d - 1], {"fsdp": other(d)})
    sq_send(KX, x_slot)
    ag_own(0)
    ag_own(1)
    sq_send(KC, c_slot)
    for d in range(1, N):
        arrive(smg.at[other(N - d)], sa_r.at[d - 1], to_ring[0])
    for j in range(LB):
        piece = smg[j * g].astype(F32)
        for i in range(1, g):
            piece = piece + smg[j * g + i].astype(F32)
        vec[:, j * 128 : (j + 1) * 128] = piece

    def row(k):
        return vec[k : k + 1, :]

    def first_norm(k):
        unit, _ = unit_rows(xg[k].astype(F32))
        nrm[k] = (unit * row(0) + row(1)).astype(BF)

    first_norm(s)
    ag_fwd(0, 0)
    sq_core(KX, x_slot)
    first_norm(s_core)
    ag_fwd(1, 0)
    ag_own(2)
    sq_relay(KX, x_slot)
    ag_fwd(0, 1)
    first_norm(s_y)
    ag_fwd(1, 1)
    sq_diag(KX, x_slot)
    first_norm(s_diag)
    ag_fwd(0, 2)
    ag_own(3)
    ag_fwd(1, 2)
    ag_last(0)

    pieces = []
    for hp in range(HP):
        cols = pl.ds(pl.multiple_of(s * DH + hp * 128, 128), 128)
        pieces += [vec[2:3, cols], jnp.zeros((1, 128), F32), vec[3:4, cols]]
    proj_bias = jnp.concatenate(pieces, axis=1)
    lanes = lax.broadcasted_iota(jnp.int32, (1, HP * 384), 1)
    proj_scale = jnp.where(lax.rem(lanes, 384) < 128, HEAD_DIM ** (-0.5), 1.0).astype(F32)

    @pl.loop(0, 4)
    def _(k):
        value = dot_nn(nrm[k], wqkv[...]) + proj_bias
        pq[k] = (value * proj_scale).astype(BF)

    ag_last(1)
    sq_send(KO, out_slot)

    flat = pq.reshape(R, HP * 384)
    lane = lax.broadcasted_iota(jnp.int32, (1, 128), 1)
    first = (lane < HEAD_DIM).astype(F32)
    picks = (first.astype(BF), (1.0 - first).astype(BF))

    def forward_tile(hp, k):
        lo = hp * 384
        query = pq[k, :, lo : lo + 128]
        keys = flat[:, lo + 128 : lo + 256]
        vals = flat[:, lo + 256 : lo + 384]
        both, logs = [], []
        for h in range(2):
            scores = dot_nt(query * picks[h], keys) + mask[...]
            top = jnp.max(scores, axis=-1, keepdims=True)
            grown = jnp.exp(scores - top)
            total = jnp.sum(grown, axis=-1, keepdims=True)
            logs.append(top + jnp.log(total))
            both.append(dot_nn((grown * (1.0 / total)).astype(BF), vals))
        here = jnp.where(lane < HEAD_DIM, both[0], both[1]).astype(BF)
        rows = pl.ds(pl.multiple_of(k * TP, 16), TP)
        ctx[s, rows, hp * 128 : hp * 128 + 128] = here
        lse[hp, rows, :] = jnp.where(lane < HEAD_DIM, logs[0], logs[1])

    for hp in range(HP):
        @pl.loop(0, 4)
        def _(i):
            forward_tile(hp, i)

            if hp < 2:
                @pl.when(i == 1)
                def _():
                    ag_fwd(2, hp)

                @pl.when(i == 3)
                def _():
                    ag_fwd(3, hp)

        sq_send(KCTX + hp, ctx_slot(hp))
        if hp == 0:
            sq_relay(KC, c_slot)
        if hp == 1:
            sq_relay(KO, out_slot)
            sq_relay(KCTX, ctx_slot(0))
    for hp in range(HP, 2):
        ag_fwd(2, hp)
        ag_fwd(3, hp)
    if HP == 1:
        sq_relay(KO, out_slot)
        sq_relay(KCTX, ctx_slot(0))
    ag_fwd(2, 2)
    sq_core(KO, out_slot)
    sq_diag(KO, out_slot)
    for hp in range(1, HP):
        sq_relay(KCTX + hp, ctx_slot(hp))
    for hp in range(HP):
        sq_core(KCTX + hp, ctx_slot(hp))
        sq_diag(KCTX + hp, ctx_slot(hp))

    @pl.loop(0, 4)
    def _(i):
        k = order(i)
        rows = pl.ds(pl.multiple_of(k * TP, 16), TP)
        joined = jnp.concatenate([ctx[j, rows, :] for j in range(4)], axis=1)
        value = xg[k].astype(F32) + dot_nn(joined, wout[...]) + row(4)
        unit, _ = unit_rows(value)
        n2[k] = (unit * row(5) + row(6)).astype(BF)

        @pl.when(i == 3)
        def _():
            mid[...] = value

    sq_sent(KX, x_slot)
    ag_fwd(3, 2)
    ag_last(2)

    @pl.loop(0, 4)
    def _(k):
        before = dot_nn(n2[k], wup[...]) + row(8)
        cdf = 0.5 + 0.5 * lax.erf(before * (0.5**0.5))
        slope = cdf + before * (jnp.exp(before * before * -0.5) * (1.0 / math.sqrt(2.0 * math.pi)))
        hid[k] = (before * cdf).astype(BF)
        gbf[k] = slope.astype(BF)

    def weight_grad(left, right, dw, size):
        per = max(256 // size, 1)

        @pl.loop(0, dw.shape[0] // per)
        def _(i):
            lo = pl.ds(pl.multiple_of(i * per * size, per * size), per * size)
            value = dot_tn(left[:, lo], right).astype(BF)
            for j in range(per):
                dw[i * per + j] = value[j * size : (j + 1) * size]

    sq_core(KC, c_slot)
    sq_diag(KC, c_slot)
    weight_grad(hid.reshape(R, D), cg.reshape(R, D)[...], dw_dn, wf)
    rg_own(0)
    ag_last(3)

    @pl.loop(0, 4)
    def _(i):
        k = order(i)
        grad = (dot_nt(cg[k], wdn[...]) * gbf[k].astype(F32)).astype(BF)
        gbf[k] = grad
        gvec[8:9, :] += jnp.sum(grad.astype(F32), axis=0, keepdims=True)
        seq_stage(i, 0, gpart, gown, grecv, dot_nt(grad, wup[...]))
        seq_stage(i, 1, opart, oown, orecv, dot_nn(hid[k], wdn[...]))

    rg_fwd(0, 0)
    weight_grad(n2.reshape(R, D), gbf.reshape(R, D)[...], dw_up, w)
    rg_own(1)

    gn = seq_total(0, gown, grecv)
    seq_sent(0, gpart)
    unit, rate = unit_rows(mid[...])
    gvec[5:6, :] = jnp.sum(gn * unit, axis=0, keepdims=True)
    gvec[6:7, :] = jnp.sum(gn, axis=0, keepdims=True)
    c_own = cg[s].astype(F32)
    gvec[7:8, :] = jnp.sum(c_own, axis=0, keepdims=True)
    gm = c_own + norm_pull(gn, row(5), unit, rate)
    gmid[...] = gm
    branch = gm.astype(BF)
    gvec[4:5, :] = jnp.sum(branch.astype(F32), axis=0, keepdims=True)
    xg[s] = branch
    sq_send(KG, x_slot)
    rg_fwd(0, 1)
    rg_fwd(1, 0)
    sq_core(KG, x_slot)
    out_total = seq_total(1, oown, orecv)
    o_out[...] = (mid[...] + out_total + row(7))[:T].astype(BF)
    sq_relay(KG, x_slot)
    rg_fwd(0, 2)
    sq_diag(KG, x_slot)

    @pl.loop(0, 4)
    def _(k):
        gctx[k] = dot_nt(xg[k], wout[pl.ds(pl.multiple_of(s * DH, DH), DH), :]).astype(BF)

    right = xg.reshape(R, D)[:, quarter]
    for j in range(4):
        value = dot_tn(ctx[j], right).astype(BF)
        for i in range(DH // w):
            dw_out[j * (DH // w) + i] = value[i * w : (i + 1) * w]
    rg_own(2)

    flat_g = gctx.reshape(R, DH)
    flat_d = dqkv.reshape(R, HP * 384)

    def backward_tile(hp, rows):
        lo = hp * 384
        query = flat[rows, lo : lo + 128]
        keys = flat[:, lo + 128 : lo + 256]
        vals = flat[:, lo + 256 : lo + 384]
        grad = flat_g[rows, hp * 128 : hp * 128 + 128]
        logs = lse[hp, rows, :]
        both = []
        for h in range(2):
            qh, gh = query * picks[h], grad * picks[h]
            probs = jnp.exp(dot_nt(qh, keys) + mask[...] - logs[:, h * HEAD_DIM : h * HEAD_DIM + 1])
            dp = dot_nt(gh, vals)
            inner = jnp.sum(probs * dp, axis=-1, keepdims=True)
            ds = (probs * (dp - inner)).astype(BF)
            both.append(dot_nn(ds, keys))
            dkt[...] += dot_tn(qh, ds)
            dvt[...] += dot_tn(gh, probs.astype(BF))
        dq = jnp.where(lane < HEAD_DIM, both[0], both[1]) * HEAD_DIM ** (-0.5)
        flat_d[rows, lo : lo + 128] = dq.astype(BF)

    polls = {
        (0, 0): lambda: rg_fwd(1, 1),
        (0, 1): lambda: rg_fin(0),
        (0, 2): lambda: rg_fwd(2, 0),
        (0, 3): lambda: rg_fwd(1, 2),
        (1, 0): lambda: rg_fwd(2, 1),
        (1, 1): lambda: rg_fwd(3, 0),
        (1, 2): lambda: rg_fin(1),
        (1, 3): lambda: [rg_fwd(2, 2), rg_fwd(3, 1)],
    }

    def poll_at(poll):
        poll()

    full = R // 256
    for hp in range(HP):
        lo = hp * 384
        dkt[...] = jnp.zeros_like(dkt)
        dvt[...] = jnp.zeros_like(dvt)

        @pl.loop(0, full)
        def _(i):
            backward_tile(hp, pl.ds(pl.multiple_of(i * 256, 256), 256))
            for (which, when), poll in polls.items():
                if which == hp and when < full:
                    pl.when(i == when)(functools.partial(poll_at, poll))

        if R % 256:
            backward_tile(hp, pl.ds(full * 256, R % 256))
        flat_d[:, lo + 128 : lo + 256] = dkt[...].T.astype(BF)
        flat_d[:, lo + 256 : lo + 384] = dvt[...].T.astype(BF)
        weight_grad(nrm.reshape(R, D), flat_d[:, lo : lo + 384], dw_qkv.at[hp], w)
        rg_own(3 + hp)
        off = pl.ds(pl.multiple_of(s * DH + hp * 128, 128), 128)
        gvec[2:3, off] = jnp.sum(flat_d[:, lo : lo + 128].astype(F32), axis=0, keepdims=True)
        gvec[3:4, off] = jnp.sum(flat_d[:, lo + 256 : lo + 384].astype(F32), axis=0, keepdims=True)
    for (which, when), poll in polls.items():
        if which >= HP or when >= full:
            poll()

    @pl.loop(0, 4)
    def _(i):
        seq_stage(i, 2, gpart, gown, grecv, dot_nt(dqkv[order(i)], wqkv[...]))

    last = 2 + HP
    if HP > 1:
        rg_fwd(3, 2)
        rg_fwd(last, 0)
    sq_relay(KFIN + 0, fin_slot(0))
    rg_fin(2)
    if HP > 1:
        rg_fin(3)
        rg_fwd(last, 1)
        sq_relay(KFIN + 1, fin_slot(1))
        sq_relay(KFIN + 2, fin_slot(2))
        rg_fwd(last, 2)
    else:
        rg_fwd(3, 2)
        sq_relay(KFIN + 1, fin_slot(1))
        sq_relay(KFIN + 2, fin_slot(2))
    gn = seq_total(2, gown, grecv)
    unit, rate = unit_rows(padded(tok))
    gvec[0:1, :] = jnp.sum(gn * unit, axis=0, keepdims=True)
    gvec[1:2, :] = jnp.sum(gn, axis=0, keepdims=True)
    for k in range(N):
        j = k // g
        dw_sm[k] = gvec[:, j * 128 : (j + 1) * 128]
    for d in range(1, N):
        send(dw_sm.at[other(d)], rr_sm.at[d - 1], sg_s.at[d - 1], sg_r.at[d - 1], {"fsdp": other(d)})
    o_tok[...] = (gmid[...] + norm_pull(gn, row(0), unit, rate))[:T].astype(BF)
    rg_fin(last)
    total = dw_sm[f]
    for d in range(1, N):
        arrive(rr_sm.at[d - 1], sg_r.at[d - 1], to_ring[0])
        total = total + rr_sm[d - 1]
    o_sm[s] = total

    def sm_slot(k):
        return o_sm.at[k]

    sq_send(KFIN + MG, sm_slot)
    finals = [(KFIN + m, fin_slot(m)) for m in range(MG)] + [(KFIN + MG, sm_slot)]
    for kind, ref in finals[3:]:
        sq_relay(kind, ref)
    for kind, ref in finals:
        sq_core(kind, ref)
        sq_diag(kind, ref)

    for m in range(4):
        ag_sent(m)
    for m in range(MG):
        rg_sent(m)
    for kind, ref in [(KC, c_slot), (KG, x_slot), (KO, out_slot)] + finals:
        sq_sent(kind, ref)
    for hp in range(HP):
        sq_sent(KCTX + hp, ctx_slot(hp))
    seq_sent(1, opart)
    seq_sent(2, gpart)
    for d in range(1, N):
        sent(smg.at[f], sa_s.at[d - 1], to_ring[0])
        sent(dw_sm.at[other(d)], sg_s.at[d - 1], to_ring[0])


def make_body(mesh):
    N = mesh.shape["fsdp"]
    A = N // 2

    def body(
        tokens, lengths, ln1_gain, ln1_bias, qkv_weight, q_bias, v_bias, out_weight, out_bias,
        ln2_gain, ln2_bias, up_weight, up_bias, down_weight, down_bias, cotangent,
    ):
        _, T, D = tokens.shape
        w, FF = D // N, up_weight.shape[1]
        wf = FF // (4 * N)
        TP = -(-T // 16) * 16
        R = 4 * TP
        DH = D // 4
        HP = DH // 128
        FQ = FF // 4
        assert FQ == D and wf == w
        g = max(128 // w, 1)
        s = lax.axis_index("seq")
        f = lax.axis_index("fsdp")
        up_whole = wf % 128 == 0
        ub = lax.dynamic_slice(up_bias, (s * wf,), (wf,))
        packed = jnp.stack([ln1_gain, ln1_bias, q_bias, v_bias, out_bias, ln2_gain, ln2_bias, down_bias, ub])
        if g == 1:
            small = jnp.pad(packed, ((0, 7), (0, 0)))
        else:
            small = lax.dynamic_update_slice(jnp.zeros((16, 128), BF), packed, (0, lax.rem(f, g) * w))
        if not up_whole:
            up_weight = lax.dynamic_index_in_dim(up_weight.reshape(w, N, 4, wf), s, 2, False).reshape(w, FQ)
        place = jnp.arange(R)
        slot, inside = place // TP, place % TP
        valid = (inside < T) & (slot * T + inside < lengths[0])
        mask = jnp.where(valid, 0.0, -1e30).astype(F32)[None, :]

        z = dict(D=D, T=T, TP=TP, R=R, A=A, w=w, wf=wf, HP=HP, g=g, up_whole=up_whole)
        vm = pltpu.VMEM
        C = 384
        scratch = [
            vm((4, TP, D), BF),
            vm((4, TP, D), BF),
            vm((4, TP, D), BF),
            vm((4, R, DH), BF),
            vm((4, TP, D), BF),
            vm((4, TP, D), BF),
            vm((4, TP, D), BF),
            vm((4, TP, HP * C), BF),
            vm((D, HP * C), BF),
            vm((D, D), BF),
            vm((D, FQ), BF),
            vm((FQ, D), BF),
            vm((N, 16, 128), BF),
            vm((16, D), F32),
            vm((16, D), F32),
            vm((HP, R, 128), F32),
            vm((TP, D), F32),
            vm((TP, D), F32),
            vm((4, TP, DH), BF),
            vm((4, TP, HP * C), BF),
            vm((128, R), F32),
            vm((128, R), F32),
            vm((3, TP, D), BF), vm((TP, D), F32), vm((3, TP, D), BF),
            vm((3, TP, D), BF), vm((TP, D), F32), vm((3, TP, D), BF),
            vm((HP, N, w, C), BF), vm((N, w, DH), BF), vm((N, w, FQ), BF), vm((N, wf, D), BF), vm((N, 16, 128), F32),
            vm((HP, 2, A, w, C), BF), vm((2, A, w, DH), BF), vm((2, A, w, FQ), BF), vm((2, A, wf, D), BF), vm((N - 1, 16, 128), F32),
        ]
        dma = pltpu.SemaphoreType.DMA
        scratch += [
            dma((3 + 3 * HP + (N if up_whole else 1),)),
            dma((4, 2, A)), dma((4, 2, A)), dma((3 + HP, 2, A)), dma((3 + HP, 2, A)),
            dma((8 + 2 * HP, 3)), dma((8 + 2 * HP, 3)),
            dma((3, 3)), dma((3, 3)),
            dma((N - 1,)), dma((N - 1,)), dma((N - 1,)), dma((N - 1,)),
        ]
        here = pl.BlockSpec(memory_space=pltpu.VMEM)
        there = pl.BlockSpec(memory_space=pl.ANY)
        out_shapes = [
            jax.ShapeDtypeStruct((T, D), BF),
            jax.ShapeDtypeStruct((T, D), BF),
            jax.ShapeDtypeStruct((HP, 4, w, C), BF),
            jax.ShapeDtypeStruct((4, w, DH), BF),
            jax.ShapeDtypeStruct((4, w, FQ), BF),
            jax.ShapeDtypeStruct((4, wf, D), BF),
            jax.ShapeDtypeStruct((4, 16, 128), F32),
        ]
        out, gtok, gq, go, gu, gd, gs = pl.pallas_call(
            functools.partial(layer_kernel, z),
            out_shape=out_shapes,
            in_specs=[here, here, here, there, there, there, there, there],
            out_specs=[here] * 7,
            scratch_shapes=scratch,
            compiler_params=pltpu.CompilerParams(
                collective_id=0, has_side_effects=True, vmem_limit_bytes=67_000_000
            ),
            name="layer",
        )(tokens[0], cotangent[0], mask, small, qkv_weight, out_weight, up_weight, down_weight)

        g_qkv = gq.reshape(HP, 4, w, 3, 128).transpose(2, 3, 1, 0, 4).reshape(w, 3 * D).astype(F32)
        g_out = go.transpose(1, 0, 2).reshape(w, D).astype(F32)
        g_up = gu.reshape(4, w, N, wf).transpose(1, 2, 0, 3).reshape(w, FF).astype(F32)
        g_down = gd.reshape(4 * wf, D).astype(F32)
        if g > 1:
            gs = lax.dynamic_slice(gs, (0, 0, lax.rem(f, g) * w), (4, 16, w))
        sums = jnp.sum(gs[:, :8], axis=0)
        return (
            out[None], gtok[None], sums[0], sums[1], g_qkv, sums[2], sums[3], g_out, sums[4],
            sums[5], sums[6], g_up, gs[:, 8].reshape(4 * wf), g_down, sums[7],
        )

    return body


def solution(mesh):
    row, mat, act = P("fsdp"), P("fsdp", None), P("fsdp", "seq", None)
    return jax.shard_map(
        make_body(mesh),
        mesh=mesh,
        in_specs=(act, row, row, row, mat, row, row, mat, row, row, row, mat, row, mat, row, act),
        out_specs=(act, act, row, row, mat, row, row, mat, row, row, row, mat, row, mat, row),
        check_vma=False,
    )
```

```python
import functools
import math

import jax
import jax.numpy as jnp
from jax import lax
from jax.experimental import pallas as pl
from jax.experimental.pallas import tpu as pltpu
from jax.sharding import PartitionSpec as P

HEAD_DIM = 64
BF = jnp.bfloat16
F32 = jnp.float32
MESH = pl.DeviceIdType.MESH


def dot_nn(left, right):
    return lax.dot_general(left, right, (((1,), (0,)), ((), ())), preferred_element_type=F32)


def dot_nt(left, right):
    return lax.dot_general(left, right, (((1,), (1,)), ((), ())), preferred_element_type=F32)


def dot_tn(left, right):
    return lax.dot_general(left, right, (((0,), (0,)), ((), ())), preferred_element_type=F32)


def unit_rows(values):
    center = values - jnp.mean(values, axis=-1, keepdims=True)
    rate = lax.rsqrt(jnp.mean(center * center, axis=-1, keepdims=True) + 1e-6)
    return center * rate, rate


def norm_pull(grad, gain, unit, rate):
    scaled = grad * gain
    return rate * (
        scaled
        - jnp.mean(scaled, axis=-1, keepdims=True)
        - unit * jnp.mean(scaled * unit, axis=-1, keepdims=True)
    )


def layer_kernel(
    z,
    tok, cot, len_in, sm_in, qkv_in, out_in, up_in, dn_in,
    o_out, o_tok, o_qkv, o_ow, o_up, o_dn, o_sm,
    xg, cg, nrm, ctx, n2, hid, gbf, pq, wqkv, wout, wup, wdn, smg, vec, gvec, lse, mid, gmid,
    gctx, dkt, dvt, gpart, gown, grecv, opart, orecv, mask,
    dw_qkv, dw_out, dw_up, dw_dn, dw_sm, rr_qkv, rr_out, rr_up, rr_dn, rr_sm,
    loc_sem, ag_s, ag_r, rg_s, rg_r, sq_s, sq_r, rs_s, rs_r, sa_s, sa_r, sg_s, sg_r, sm_s, sm_r,
):
    D, T, TP, R, A, w, wf, HP = z["D"], z["T"], z["TP"], z["R"], z["A"], z["w"], z["wf"], z["HP"]
    N, H, DH, LB, g = 2 * A, A, D // 4, D // 128, z["g"]
    s = lax.axis_index("seq")
    f = lax.axis_index("fsdp")
    y, c = lax.div(s, 2), lax.rem(s, 2)
    s_core, s_y, s_diag = y * 2 + 1 - c, (1 - y) * 2 + c, (1 - y) * 2 + 1 - c
    to_core, to_y = {"seq": s_core}, {"seq": s_y}

    odd = lax.rem(f, 2)
    place = (1 - odd) * lax.div(f, 2) + odd * (N - 1 - lax.div(f, 2))

    def at_place(q):
        late = lax.div(q, A)
        return (1 - late) * 2 * q + late * (2 * (N - 1 - q) + 1)

    def ahead(d):
        return at_place(lax.rem(place + d + N, N))

    to_ring = ({"fsdp": ahead(1)}, {"fsdp": ahead(-1)})

    def send(src, dst, ssem, rsem, dev):
        pltpu.make_async_remote_copy(
            src_ref=src, dst_ref=dst, send_sem=ssem, recv_sem=rsem, device_id=dev, device_id_type=MESH
        ).start()

    def arrive(dst, rsem, dev):
        pltpu.make_async_remote_copy(
            src_ref=dst, dst_ref=dst, send_sem=rsem, recv_sem=rsem, device_id=dev, device_id_type=MESH
        ).wait_recv()

    def sent(src, ssem, dev):
        pltpu.make_async_remote_copy(
            src_ref=src, dst_ref=src, send_sem=ssem, recv_sem=ssem, device_id=dev, device_id_type=MESH
        ).wait_send()

    def thirds(first, last):
        count = max(last - first, 0)
        cut = [first + (count * k) // 3 for k in range(4)]
        return [range(cut[k], cut[k + 1]) for k in range(3)]

    quarter = pl.ds(pl.multiple_of(s * DH, DH), DH)

    def rows_of(k, size, half=None):
        if half is None:
            return pl.ds(pl.multiple_of(k * size, size), size)
        return pl.ds(pl.multiple_of(k * size + half * (size // 2), size // 2), size // 2)

    OUT, UP, DN = HP, HP + 1, HP + 2
    blocks = {
        OUT: lambda k, half=None: wout.at[rows_of(k, w, half), quarter],
        UP: lambda k, half=None: wup.at[rows_of(k, w, half)],
        DN: lambda k, half=None: wdn.at[rows_of(k, wf, half)],
    }
    for hp in range(HP):
        blocks[hp] = lambda k, half=None, hp=hp: wqkv.at[rows_of(k, w, half), hp * 384 : hp * 384 + 384]

    def ag_block(m, way, d, back):
        k = ahead(-back if way == 0 else back)
        return blocks[m](k, way if d == H else None)

    def ag_own(m):
        for way in range(2):
            ref = ag_block(m, way, 1, 0)
            send(ref, ref, ag_s.at[m, way, 0], ag_r.at[m, way, 0], to_ring[way])

    def ag_take(m, d):
        for way in range(2):
            arrive(ag_block(m, way, d, d), ag_r.at[m, way, d - 1], to_ring[way])
            if d < H:
                ref = ag_block(m, way, d + 1, d)
                send(ref, ref, ag_s.at[m, way, d], ag_r.at[m, way, d], to_ring[way])

    def ag_fwd(m, third):
        for d in thirds(1, H)[third]:
            ag_take(m, d)

    def ag_last(m):
        ag_take(m, H)

    def ag_sent(m):
        for way in range(2):
            for d in range(1, H + 1):
                sent(ag_block(m, way, d, d - 1), ag_s.at[m, way, d - 1], to_ring[way])

    def sq_send(kind, ref):
        send(ref(s), ref(s), sq_s.at[kind, 0], sq_r.at[kind, 0], to_core)
        send(ref(s), ref(s), sq_s.at[kind, 1], sq_r.at[kind, 1], to_y)

    def sq_core(kind, ref):
        arrive(ref(s_core), sq_r.at[kind, 0], to_core)

    def sq_relay(kind, ref):
        arrive(ref(s_y), sq_r.at[kind, 1], to_y)
        send(ref(s_y), ref(s_y), sq_s.at[kind, 2], sq_r.at[kind, 2], to_core)

    def sq_diag(kind, ref):
        arrive(ref(s_diag), sq_r.at[kind, 2], to_core)

    def sq_sent(kind, ref):
        sent(ref(s), sq_s.at[kind, 0], to_core)
        sent(ref(s), sq_s.at[kind, 1], to_y)
        sent(ref(s_y), sq_s.at[kind, 2], to_core)

    def x_slot(k):
        return xg.at[k]

    def c_slot(k):
        return cg.at[k]

    def g_slot(k):
        return nrm.at[k]

    def out_slot(k):
        return wout.at[:, pl.ds(pl.multiple_of(k * DH, DH), DH)]

    def ctx_slot(hp):
        return lambda k: ctx.at[k, :, hp * 128 : hp * 128 + 128]

    KX, KC, KG, KO, KCTX, KFIN = 0, 1, 2, 3, 4, 4 + HP

    def order(i):
        hb, lb = lax.div(3 - i, 2), lax.rem(3 - i, 2)
        return lax.rem(y + hb, 2) * 2 + lax.rem(c + lb, 2)

    def seq_stage(i, kind, part, own, recv, value):
        @pl.when(i < 3)
        def _():
            part[jnp.minimum(i, 2)] = value.astype(BF)

        @pl.when(i == 0)
        def _():
            send(part.at[0], recv.at[0], rs_s.at[kind, 0], rs_r.at[kind, 0], to_core)

        @pl.when(i == 1)
        def _():
            arrive(recv.at[0], rs_r.at[kind, 0], to_core)
            part[1] = (part[1].astype(F32) + recv[0].astype(F32)).astype(BF)
            send(part.at[1], recv.at[1], rs_s.at[kind, 1], rs_r.at[kind, 1], to_y)

        @pl.when(i == 2)
        def _():
            send(part.at[2], recv.at[2], rs_s.at[kind, 2], rs_r.at[kind, 2], to_core)

        @pl.when(i == 3)
        def _():
            own[...] = value

    def seq_sent(kind, part):
        for j in range(3):
            sent(part.at[j], rs_s.at[kind, j], to_core)

    def seq_total(kind, own, recv):
        arrive(recv.at[2], rs_r.at[kind, 2], to_core)
        arrive(recv.at[1], rs_r.at[kind, 1], to_y)
        return own[...] + recv[2].astype(F32) + recv[1].astype(F32)

    grads = {0: (dw_dn, rr_dn, o_dn), 1: (dw_up, rr_up, o_up), 2: (dw_out, rr_out, o_ow)}
    for hp in range(HP):
        grads[3 + hp] = (dw_qkv.at[hp], rr_qkv.at[hp], o_qkv.at[hp])
    MG = 3 + HP

    def rg_rows(m, way, j):
        size = grads[m][0].shape[1]
        return slice(way * (size // 2), (way + 1) * (size // 2)) if j == 0 else slice(0, size)

    def rg_owner(way, j):
        return ahead(H - j if way == 0 else j - H)

    def rg_src(m, way, j):
        return grads[m][0].at[rg_owner(way, j), rg_rows(m, way, j)]

    def rg_send(m, way, j):
        dst = grads[m][1].at[way, j, rg_rows(m, way, j)]
        send(rg_src(m, way, j), dst, rg_s.at[m, way, j], rg_r.at[m, way, j], to_ring[way])

    def rg_arrive(m, way, j):
        arrive(grads[m][1].at[way, j, rg_rows(m, way, j)], rg_r.at[m, way, j], to_ring[way])

    def rg_own(m):
        for way in range(2):
            rg_send(m, way, 0)

    def rg_fwd(m, third):
        dw, rr, _ = grads[m]
        for j in thirds(1, H)[third]:
            for way in range(2):
                rows = rg_rows(m, way, j - 1)
                owner = rg_owner(way, j)
                rg_arrive(m, way, j - 1)
                dw[owner, rows] = (dw[owner, rows].astype(F32) + rr[way, j - 1, rows].astype(F32)).astype(dw.dtype)
                rg_send(m, way, j)

    def fin_slot(m):
        return lambda k: grads[m][2].at[k]

    def rg_fin(m):
        dw, rr, out = grads[m]
        total = dw[f].astype(F32)
        for way in range(2):
            rg_arrive(m, way, H - 1)
            total = total + rr[way, H - 1].astype(F32)
        out[s] = total.astype(out.dtype)
        sq_send(KFIN + m, fin_slot(m))

    def rg_sent(m):
        for way in range(2):
            for j in range(H):
                sent(rg_src(m, way, j), rg_s.at[m, way, j], to_ring[way])

    def other(d):
        return lax.rem(f + d, N)

    local = []

    def bring(src, dst):
        copy = pltpu.make_async_copy(src, dst, loc_sem.at[len(local)])
        copy.start()
        local.append(copy)

    bring(sm_in, smg.at[f])
    for hp in range(HP):
        for part in range(3):
            cols = pl.ds(pl.multiple_of(part * D + s * DH + hp * 128, 128), 128)
            lo = hp * 384 + part * 128
            bring(qkv_in.at[:, cols], wqkv.at[rows_of(f, w), lo : lo + 128])
    bring(out_in.at[:, quarter], wout.at[rows_of(f, w), quarter])
    if z["up_whole"]:
        for k in range(N):
            cols = pl.ds(pl.multiple_of((k * 4 + s) * wf, wf), wf)
            bring(up_in.at[:, cols], wup.at[rows_of(f, w), k * wf : (k + 1) * wf])
    else:
        bring(up_in, wup.at[rows_of(f, w)])
    bring(dn_in.at[rows_of(s, wf)], wdn.at[rows_of(f, wf)])

    def padded(ref):
        return jnp.concatenate([ref[...].astype(F32), jnp.zeros((TP - T, D), F32)], axis=0)

    barrier = pltpu.get_barrier_semaphore()
    peers = [to_core, to_y, {"seq": s_diag}] + [{"fsdp": other(d)} for d in range(1, N)]
    for dev in peers:
        pl.semaphore_signal(barrier, inc=1, device_id=dev, device_id_type=MESH)
    xg[s] = padded(tok).astype(BF)
    cg[s] = padded(cot).astype(BF)
    gvec[...] = jnp.zeros_like(gvec)
    column = lax.broadcasted_iota(jnp.int32, (1, R), 1)
    slot = sum((column >= TP * k).astype(jnp.int32) for k in range(1, 4))
    inside = column - slot * TP
    valid = (inside < T) & (slot * T + inside < len_in[0])
    mask[...] = jnp.where(valid, 0.0, -1e30).astype(F32)
    for copy in local:
        copy.wait()
    pl.semaphore_wait(barrier, len(peers))

    for d in range(1, N):
        send(smg.at[f], smg.at[f], sa_s.at[d - 1], sa_r.at[d - 1], {"fsdp": other(d)})
    sq_send(KX, x_slot)
    for m in (0, 1, OUT):
        ag_own(m)
    sq_send(KC, c_slot)
    for d in range(1, N):
        arrive(smg.at[other(N - d)], sa_r.at[d - 1], to_ring[0])
    for j in range(LB):
        piece = smg[j * g].astype(F32)
        for i in range(1, g):
            piece = piece + smg[j * g + i].astype(F32)
        vec[:, j * 128 : (j + 1) * 128] = piece

    def row(k):
        return vec[k : k + 1, :]

    def first_norm(k, into=nrm):
        unit, _ = unit_rows(xg[k].astype(F32))
        into[k] = (unit * row(0) + row(1)).astype(BF)

    def project(hp):
        cols = pl.ds(pl.multiple_of(s * DH + hp * 128, 128), 128)
        bias = jnp.concatenate([vec[2:3, cols], jnp.zeros((1, 128), F32), vec[3:4, cols]], axis=1)
        lanes = lax.broadcasted_iota(jnp.int32, (1, 384), 1)
        scale = jnp.where(lanes < 128, HEAD_DIM ** (-0.5), 1.0).astype(F32)
        here = slice(hp * 384, hp * 384 + 384)

        @pl.loop(0, 4)
        def _(k):
            pq[k, :, here] = ((dot_nn(nrm[k], wqkv[:, here]) + bias) * scale).astype(BF)

    first_norm(s)
    ag_fwd(0, 0)
    sq_core(KX, x_slot)
    first_norm(s_core)
    ag_fwd(1, 0)
    ag_fwd(OUT, 0)
    ag_fwd(0, 1)
    ag_fwd(1, 1)
    ag_fwd(OUT, 1)
    sq_relay(KX, x_slot)
    first_norm(s_y)
    ag_fwd(0, 2)
    ag_fwd(1, 2)
    ag_fwd(OUT, 2)
    ag_own(UP)
    ag_own(DN)
    sq_diag(KX, x_slot)
    first_norm(s_diag)
    ag_last(0)
    project(0)

    flat = pq.reshape(R, HP * 384)
    lane = lax.broadcasted_iota(jnp.int32, (1, 128), 1)
    first = (lane < HEAD_DIM).astype(F32)
    picks = (first.astype(BF), (1.0 - first).astype(BF))

    def lanes_at(off):
        return pl.ds(pl.multiple_of(off, 128), 128)

    def slot_rows(k):
        return pl.ds(pl.multiple_of(k * TP, 16), TP)

    @pl.loop(0, 8)
    def _(t):
        hp, k = lax.div(t, 4), lax.rem(t, 4)
        query = pq[k, :, lanes_at(hp * 384)]
        keys = flat[:, lanes_at(hp * 384 + 128)]
        vals = flat[:, lanes_at(hp * 384 + 256)]
        both, logs = [], []
        for h in range(2):
            scores = dot_nt(query * picks[h], keys) + mask[...]
            top = jnp.max(scores, axis=-1, keepdims=True)
            grown = jnp.exp(scores - top)
            total = jnp.sum(grown, axis=-1, keepdims=True)
            logs.append(top + jnp.log(total))
            both.append(dot_nn((grown * (1.0 / total)).astype(BF), vals))
        rows = slot_rows(k)
        ctx[s, rows, lanes_at(hp * 128)] = jnp.where(lane < HEAD_DIM, both[0], both[1]).astype(BF)
        lse[hp, rows, :] = jnp.where(lane < HEAD_DIM, logs[0], logs[1])

        @pl.when(t == 0)
        def _():
            ag_last(OUT)
            sq_send(KO, out_slot)
            ag_last(1)
            project(1)

        @pl.when(t == 2)
        def _():
            ag_fwd(UP, 0)
            sq_relay(KC, c_slot)

        @pl.when(t == 3)
        def _():
            sq_send(KCTX, ctx_slot(0))

        @pl.when(t == 5)
        def _():
            ag_fwd(DN, 0)

        @pl.when(t == 7)
        def _():
            sq_send(KCTX + 1, ctx_slot(1))

    sq_relay(KO, out_slot)
    ag_fwd(UP, 1)
    sq_relay(KCTX, ctx_slot(0))
    sq_core(KO, out_slot)
    sq_diag(KO, out_slot)
    sq_core(KCTX, ctx_slot(0))
    sq_core(KCTX + 1, ctx_slot(1))
    ag_fwd(DN, 1)
    sq_relay(KCTX + 1, ctx_slot(1))
    sq_diag(KCTX, ctx_slot(0))
    sq_diag(KCTX + 1, ctx_slot(1))
    ag_fwd(UP, 2)

    @pl.loop(0, 4)
    def _(i):
        k = order(i)
        joined = jnp.concatenate([ctx[j, slot_rows(k), :] for j in range(4)], axis=1)
        value = xg[k].astype(F32) + dot_nn(joined, wout[...]) + row(4)
        unit, _ = unit_rows(value)
        n2[k] = (unit * row(5) + row(6)).astype(BF)

        @pl.when(i == 3)
        def _():
            mid[...] = value

    ag_fwd(DN, 2)
    sq_core(KC, c_slot)
    sq_diag(KC, c_slot)
    ag_last(UP)
    ag_last(DN)

    @pl.loop(0, 4)
    def _(i):
        k = order(i)
        before = dot_nn(n2[k], wup[...]) + row(8)
        cdf = 0.5 + 0.5 * lax.erf(before * (0.5**0.5))
        slope = cdf + before * (jnp.exp(before * before * -0.5) * (1.0 / math.sqrt(2.0 * math.pi)))
        hid[k] = (before * cdf).astype(BF)
        grad = (dot_nt(cg[k], wdn[...]) * slope).astype(BF)
        gbf[k] = grad
        gvec[8:9, :] += jnp.sum(grad.astype(F32), axis=0, keepdims=True)
        seq_stage(i, 0, gpart, gown, grecv, dot_nt(grad, wup[...]))

    def weight_grad(left, right, dw, size):
        per = max(256 // size, 1)

        @pl.loop(0, dw.shape[0] // per)
        def _(i):
            lo = pl.ds(pl.multiple_of(i * per * size, per * size), per * size)
            value = dot_tn(left[:, lo], right).astype(BF)
            for j in range(per):
                dw[i * per + j] = value[j * size : (j + 1) * size]

    weight_grad(hid.reshape(R, D), cg.reshape(R, D)[...], dw_dn, wf)
    rg_own(0)
    weight_grad(n2.reshape(R, D), gbf.reshape(R, D)[...], dw_up, w)
    rg_own(1)
    rg_fwd(0, 0)

    @pl.loop(0, 4)
    def _(k):
        first_norm(k, n2)


    gn = seq_total(0, gown, grecv)
    seq_sent(0, gpart)
    unit, rate = unit_rows(mid[...])
    gvec[5:6, :] = jnp.sum(gn * unit, axis=0, keepdims=True)
    gvec[6:7, :] = jnp.sum(gn, axis=0, keepdims=True)
    c_own = cg[s].astype(F32)
    gvec[7:8, :] = jnp.sum(c_own, axis=0, keepdims=True)
    gm = c_own + norm_pull(gn, row(5), unit, rate)
    gmid[...] = gm
    branch = gm.astype(BF)
    gvec[4:5, :] = jnp.sum(branch.astype(F32), axis=0, keepdims=True)
    nrm[s] = branch
    sq_send(KG, g_slot)

    @pl.loop(0, 4)
    def _(i):
        seq_stage(i, 1, opart, gown, orecv, dot_nn(hid[order(i)], wdn[...]))

    rg_fwd(1, 0)

    flat_g = gctx.reshape(R, DH)
    dkt[...] = jnp.zeros_like(dkt)
    dvt[...] = jnp.zeros_like(dvt)

    def branch_back(k):
        gctx[k] = dot_nt(nrm[k], wout[pl.ds(pl.multiple_of(s * DH, DH), DH), :]).astype(BF)

    def close_pair(hp):
        lo = hp * 384
        flat[:, lo + 128 : lo + 256] = dkt[hp].T.astype(BF)
        flat[:, lo + 256 : lo + 384] = dvt[hp].T.astype(BF)
        weight_grad(n2.reshape(R, D), flat[:, lo : lo + 384], dw_qkv.at[hp], w)
        rg_own(3 + hp)
        off = lanes_at(s * DH + hp * 128)
        gvec[2:3, off] = jnp.sum(flat[:, lo : lo + 128].astype(F32), axis=0, keepdims=True)
        gvec[3:4, off] = jnp.sum(flat[:, lo + 256 : lo + 384].astype(F32), axis=0, keepdims=True)

    branch_back(s)
    sq_core(KG, g_slot)
    branch_back(s_core)

    @pl.loop(0, 8)
    def _(t):
        late, u = lax.div(t, 4), lax.rem(t, 4)
        hp = (1 - late) * lax.rem(u, 2) + late * lax.div(u, 2)
        flip = (1 - late) * lax.div(u, 2) + late * lax.rem(u, 2)
        k = lax.rem(y + late, 2) * 2 + lax.rem(c + flip, 2)
        query = pq[k, :, lanes_at(hp * 384)]
        keys = flat[:, lanes_at(hp * 384 + 128)]
        vals = flat[:, lanes_at(hp * 384 + 256)]
        grad = gctx[k, :, lanes_at(hp * 128)]
        logs = lse[hp, slot_rows(k), :]
        both = []
        for h in range(2):
            qh, gh = query * picks[h], grad * picks[h]
            probs = jnp.exp(dot_nt(qh, keys) + mask[...] - logs[:, h * HEAD_DIM : h * HEAD_DIM + 1])
            dp = dot_nt(gh, vals)
            inner = jnp.sum(probs * dp, axis=-1, keepdims=True)
            ds = (probs * (dp - inner)).astype(BF)
            both.append(dot_nn(ds, keys))
            dkt[hp] += dot_tn(qh, ds)
            dvt[hp] += dot_tn(gh, probs.astype(BF))
        dq = jnp.where(lane < HEAD_DIM, both[0], both[1]) * HEAD_DIM ** (-0.5)
        pq[k, :, lanes_at(hp * 384)] = dq.astype(BF)

        @pl.when(t == 1)
        def _():
            rg_fwd(0, 1)

        @pl.when(t == 3)
        def _():
            rg_fwd(1, 1)
            sq_relay(KG, g_slot)
            branch_back(s_y)
            sq_diag(KG, g_slot)
            branch_back(s_diag)
            right = nrm.reshape(R, D)[:, quarter]
            for j in range(4):
                value = dot_tn(ctx[j], right).astype(BF)
                for i in range(DH // w):
                    dw_out[j * (DH // w) + i] = value[i * w : (i + 1) * w]
            rg_own(2)

        @pl.when(t == 4)
        def _():
            rg_fwd(0, 2)

        @pl.when(t == 5)
        def _():
            close_pair(0)
            rg_fwd(2, 0)

        @pl.when(t == 6)
        def _():
            rg_fwd(1, 2)

        @pl.when(t == 7)
        def _():
            rg_fwd(2, 1)

    close_pair(1)
    rg_fin(0)
    out_total = seq_total(1, gown, orecv)
    o_out[...] = (mid[...] + out_total + row(7))[:T].astype(BF)

    @pl.loop(0, 4)
    def _(i):
        seq_stage(i, 2, gpart, gown, grecv, dot_nt(pq[order(i)], wqkv[...]))

    rg_fwd(3, 0)
    rg_fwd(2, 2)
    arrive(grecv.at[2], rs_r.at[2, 2], to_core)
    here = gown[...] + grecv[2].astype(F32)
    away = gpart[1].astype(F32)
    unit, rate = unit_rows(xg[s].astype(F32))
    unit_y, _ = unit_rows(xg[s_y].astype(F32))
    gvec[0:1, :] = jnp.sum(here * unit + away * unit_y, axis=0, keepdims=True)
    gvec[1:2, :] = jnp.sum(here + away, axis=0, keepdims=True)
    for k in range(N):
        j = k // g
        dw_sm[k] = gvec[:, j * 128 : (j + 1) * 128]
    for d in range(1, N):
        send(dw_sm.at[other(d)], rr_sm.at[d - 1], sg_s.at[d - 1], sg_r.at[d - 1], {"fsdp": other(d)})
    rg_fwd(4, 0)
    rg_fin(1)
    rg_fwd(3, 1)
    total = dw_sm[f]
    for d in range(1, N):
        arrive(rr_sm.at[d - 1], sg_r.at[d - 1], to_ring[0])
        total = total + rr_sm[d - 1]
    o_sm[s] = total

    def sm_slot(k):
        return o_sm.at[k]

    three = ((to_core, s_core), (to_y, s_y), ({"seq": s_diag}, s_diag))
    for d, (dev, _) in enumerate(three):
        send(o_sm.at[s], o_sm.at[s], sm_s.at[d], sm_r.at[d], dev)
    rg_fwd(4, 1)
    rg_fin(2)
    rg_fwd(3, 2)
    sq_relay(KFIN + 0, fin_slot(0))
    rg_fwd(4, 2)
    arrive(grecv.at[1], rs_r.at[2, 1], to_y)
    gn = here + grecv[1].astype(F32)
    o_tok[...] = (gmid[...] + norm_pull(gn, row(0), unit, rate))[:T].astype(BF)
    rg_fin(3)
    sq_relay(KFIN + 1, fin_slot(1))
    rg_fin(4)
    sq_relay(KFIN + 2, fin_slot(2))
    finals = [(KFIN + m, fin_slot(m)) for m in range(MG)]
    for kind, ref in (finals[3], finals[4]):
        sq_relay(kind, ref)
    for kind, ref in finals:
        sq_core(kind, ref)
        sq_diag(kind, ref)
    for d, (dev, k) in enumerate(three):
        arrive(o_sm.at[k], sm_r.at[d], dev)
        sent(o_sm.at[s], sm_s.at[d], dev)

    for m in range(3 + HP):
        ag_sent(m)
    for m in range(MG):
        rg_sent(m)
    for kind, ref in [(KX, x_slot), (KC, c_slot), (KG, g_slot), (KO, out_slot)] + finals:
        sq_sent(kind, ref)
    for hp in range(HP):
        sq_sent(KCTX + hp, ctx_slot(hp))
    seq_sent(1, opart)
    seq_sent(2, gpart)
    for d in range(1, N):
        sent(smg.at[f], sa_s.at[d - 1], to_ring[0])
        sent(dw_sm.at[other(d)], sg_s.at[d - 1], to_ring[0])


def finish_kernel(z, out, tok, gq, go, gu, gd, gs, *outs):
    o_out, o_tok, o_qkv, o_ow, o_up, o_dn = outs[:6]
    D, wf, HP, N = z["D"], z["wf"], z["HP"], 2 * z["A"]
    DH = D // 4
    for s in range(4):
        for hp in range(HP):
            for part in range(3):
                lo = part * D + s * DH + hp * 128
                o_qkv[:, lo : lo + 128] = gq[hp, s, :, part * 128 : part * 128 + 128].astype(F32)
        o_ow[:, s * DH : (s + 1) * DH] = go[s].astype(F32)
        if z["up_whole"]:
            for k in range(N):
                o_up[:, (k * 4 + s) * wf : (k * 4 + s + 1) * wf] = gu[s, :, k * wf : (k + 1) * wf].astype(F32)
    if not z["up_whole"]:
        o_up[...] = gu[...].astype(F32)
    o_dn[...] = gd[0].astype(F32)

    @pl.when(pl.program_id(0) == 0)
    def _():
        o_out[...] = out[...]
        o_tok[...] = tok[...]
        total = gs[0] + gs[1] + gs[2] + gs[3]
        for k in range(8):
            outs[6 + k][...] = total[k : k + 1]
        outs[14][...] = jnp.concatenate([gs[s, 8:9] for s in range(4)], axis=1)


def make_body(mesh):
    N = mesh.shape["fsdp"]
    A = N // 2

    def body(
        tokens, lengths, ln1_gain, ln1_bias, qkv_weight, q_bias, v_bias, out_weight, out_bias,
        ln2_gain, ln2_bias, up_weight, up_bias, down_weight, down_bias, cotangent,
    ):
        _, T, D = tokens.shape
        w, FF = D // N, up_weight.shape[1]
        wf = FF // (4 * N)
        TP = -(-T // 16) * 16
        R = 4 * TP
        DH = D // 4
        HP = DH // 128
        FQ = FF // 4
        assert FQ == D and wf == w and HP == 2
        g = max(128 // w, 1)
        s = lax.axis_index("seq")
        f = lax.axis_index("fsdp")
        up_whole = wf % 128 == 0
        ub = lax.dynamic_slice(up_bias, (s * wf,), (wf,))
        packed = jnp.stack(
            [ln1_gain, ln1_bias, q_bias, v_bias, out_bias, ln2_gain, ln2_bias, down_bias, ub]
            + [jnp.zeros_like(ub)] * 7
        )
        if g == 1:
            small = packed
        else:
            small = lax.dynamic_update_slice(jnp.zeros((16, 128), BF), packed, (0, lax.rem(f, g) * w))
        if not up_whole:
            up_weight = lax.dynamic_index_in_dim(up_weight.reshape(w, N, 4, wf), s, 2, False).reshape(w, FQ)
        z = dict(D=D, T=T, TP=TP, R=R, A=A, w=w, wf=wf, HP=HP, g=g, up_whole=up_whole)
        vm = pltpu.VMEM
        C = 384
        scratch = [
            vm((4, TP, D), BF),
            vm((4, TP, D), BF),
            vm((4, TP, D), BF),
            vm((4, R, DH), BF),
            vm((4, TP, D), BF),
            vm((4, TP, D), BF),
            vm((4, TP, D), BF),
            vm((4, TP, HP * C), BF),
            vm((D, HP * C), BF),
            vm((D, D), BF),
            vm((D, FQ), BF),
            vm((FQ, D), BF),
            vm((N, 16, 128), BF),
            vm((16, D), F32),
            vm((16, D), F32),
            vm((HP, R, 128), F32),
            vm((TP, D), F32),
            vm((TP, D), F32),
            vm((4, TP, DH), BF),
            vm((HP, 128, R), F32),
            vm((HP, 128, R), F32),
            vm((3, TP, D), BF), vm((TP, D), F32), vm((3, TP, D), BF),
            vm((3, TP, D), BF), vm((3, TP, D), BF),
            vm((1, R), F32),
            vm((HP, N, w, C), BF), vm((N, w, DH), BF), vm((N, w, FQ), BF), vm((N, wf, D), BF), vm((N, 16, 128), F32),
            vm((HP, 2, A, w, C), BF), vm((2, A, w, DH), BF), vm((2, A, w, FQ), BF), vm((2, A, wf, D), BF), vm((N - 1, 16, 128), F32),
        ]
        dma = pltpu.SemaphoreType.DMA
        scratch += [
            dma((3 + 3 * HP + (N if up_whole else 1),)),
            dma((3 + HP, 2, A)), dma((3 + HP, 2, A)), dma((3 + HP, 2, A)), dma((3 + HP, 2, A)),
            dma((7 + 2 * HP, 3)), dma((7 + 2 * HP, 3)),
            dma((3, 3)), dma((3, 3)),
            dma((N - 1,)), dma((N - 1,)), dma((N - 1,)), dma((N - 1,)), dma((3,)), dma((3,)),
        ]
        here = pl.BlockSpec(memory_space=pltpu.VMEM)
        there = pl.BlockSpec(memory_space=pl.ANY)
        out_shapes = [
            jax.ShapeDtypeStruct((T, D), BF),
            jax.ShapeDtypeStruct((T, D), BF),
            jax.ShapeDtypeStruct((HP, 4, w, C), BF),
            jax.ShapeDtypeStruct((4, w, DH), BF),
            jax.ShapeDtypeStruct((4, w, FQ), BF),
            jax.ShapeDtypeStruct((4, wf, D), BF),
            jax.ShapeDtypeStruct((4, 16, 128), F32),
        ]
        out, gtok, gq, go, gu, gd, gs = pl.pallas_call(
            functools.partial(layer_kernel, z),
            out_shape=out_shapes,
            in_specs=[here, here, pl.BlockSpec(memory_space=pltpu.SMEM), there, there, there, there, there],
            out_specs=[here] * 7,
            scratch_shapes=scratch,
            compiler_params=pltpu.CompilerParams(
                collective_id=0, has_side_effects=True, vmem_limit_bytes=67_000_000
            ),
            name="layer",
        )(tokens[0], cotangent[0], lengths, small, qkv_weight, out_weight, up_weight, down_weight)

        if not up_whole:
            gu = gu.reshape(4, w, N, wf).transpose(1, 2, 0, 3).reshape(w, FF)
        if g > 1:
            gs = lax.dynamic_slice(gs, (0, 0, lax.rem(f, g) * w), (4, 16, w))
        parts = 4
        rb = w // parts
        whole = lambda shape: pl.BlockSpec(shape, lambda i: (0,) * len(shape))
        vectors = [jax.ShapeDtypeStruct((1, w), F32)] * 8 + [jax.ShapeDtypeStruct((1, 4 * wf), F32)]
        up_spec = pl.BlockSpec((4, rb, FQ), lambda i: (0, i, 0)) if up_whole else pl.BlockSpec((rb, FF), lambda i: (i, 0))
        done = pl.pallas_call(
            functools.partial(finish_kernel, z),
            grid=(parts,),
            out_shape=[
                jax.ShapeDtypeStruct((T, D), BF), jax.ShapeDtypeStruct((T, D), BF),
                jax.ShapeDtypeStruct((w, 3 * D), F32), jax.ShapeDtypeStruct((w, D), F32),
                jax.ShapeDtypeStruct((w, FF), F32), jax.ShapeDtypeStruct((4 * wf, D), F32),
            ] + vectors,
            in_specs=[
                whole((T, D)), whole((T, D)),
                pl.BlockSpec((HP, 4, rb, C), lambda i: (0, 0, i, 0)),
                pl.BlockSpec((4, rb, DH), lambda i: (0, i, 0)),
                up_spec,
                pl.BlockSpec((1, wf, D), lambda i: (i, 0, 0)),
                whole((4, 16, w)),
            ],
            out_specs=[
                whole((T, D)), whole((T, D)),
                pl.BlockSpec((rb, 3 * D), lambda i: (i, 0)),
                pl.BlockSpec((rb, D), lambda i: (i, 0)),
                pl.BlockSpec((rb, FF), lambda i: (i, 0)),
                pl.BlockSpec((wf, D), lambda i: (i, 0)),
            ] + [whole((1, w))] * 8 + [whole((1, 4 * wf))],
            name="finish",
        )(out, gtok, gq, go, gu, gd, gs)
        out, gtok, g_qkv, g_out, g_up, g_down = done[:6]
        sums = [v.reshape(-1) for v in done[6:]]
        return (
            out[None], gtok[None], sums[0], sums[1], g_qkv, sums[2], sums[3], g_out, sums[4],
            sums[5], sums[6], g_up, sums[8], g_down, sums[7],
        )

    return body


def solution(mesh):
    row, mat, act = P("fsdp"), P("fsdp", None), P("fsdp", "seq", None)
    return jax.shard_map(
        make_body(mesh),
        mesh=mesh,
        in_specs=(act, row, row, row, mat, row, row, mat, row, row, row, mat, row, mat, row, act),
        out_specs=(act, act, row, row, mat, row, row, mat, row, row, row, mat, row, mat, row),
        check_vma=False,
    )
```

```python
import functools
import math

import jax
import jax.numpy as jnp
from jax import lax
from jax.experimental import pallas as pl
from jax.experimental.pallas import tpu as pltpu
from jax.sharding import PartitionSpec as P

HEAD_DIM = 64
BF = jnp.bfloat16
F32 = jnp.float32
MESH = pl.DeviceIdType.MESH


def dot_nn(left, right):
    return lax.dot_general(left, right, (((1,), (0,)), ((), ())), preferred_element_type=F32)


def dot_nt(left, right):
    return lax.dot_general(left, right, (((1,), (1,)), ((), ())), preferred_element_type=F32)


def dot_tn(left, right):
    return lax.dot_general(left, right, (((0,), (0,)), ((), ())), preferred_element_type=F32)


def unit_rows(values):
    center = values - jnp.mean(values, axis=-1, keepdims=True)
    rate = lax.rsqrt(jnp.mean(center * center, axis=-1, keepdims=True) + 1e-6)
    return center * rate, rate


def norm_pull(grad, gain, unit, rate):
    scaled = grad * gain
    return rate * (
        scaled
        - jnp.mean(scaled, axis=-1, keepdims=True)
        - unit * jnp.mean(scaled * unit, axis=-1, keepdims=True)
    )


def layer_entry(z, *refs):
    layer_kernel(z, *refs[:3], refs[3:11], *refs[11:])


def layer_kernel(
    z,
    tok_in, cot_in, len_in, vecs_in, ub_in, qkv_in, out_in, up_in, dn_in,
    h_out, h_tok, h_qkv, h_ow, h_up, h_dn, h_sm,
    tok, cot, lens, vecs, ub4, o_qkv, o_ow, o_up, o_dn, o_sm,
    xg, cg, nrm, ctx, n2, hid, gbf, pq, wqkv, wout, wup, wdn, smg, vec, gvec, lse, mid, gmid,
    gctx, dkt, dvt, gpart, gown, grecv, opart, oown, orecv, mask,
    dw_qkv, dw_out, dw_up, dw_dn, dw_sm, rr_qkv, rr_out, rr_up, rr_dn, rr_sm,
    loc_sem, put_sem, ag_s, ag_r, rg_s, rg_r, sq_s, sq_r, rs_s, rs_r, sa_s, sa_r, sg_s, sg_r, sm_s, sm_r,
):
    D, T, TP, R, A, w, wf, HP = z["D"], z["T"], z["TP"], z["R"], z["A"], z["w"], z["wf"], z["HP"]
    N, H, DH, LB, g = 2 * A, A, D // 4, D // 128, z["g"]
    s = lax.axis_index("seq")
    f = lax.axis_index("fsdp")
    y, c = lax.div(s, 2), lax.rem(s, 2)
    s_core, s_y, s_diag = y * 2 + 1 - c, (1 - y) * 2 + c, (1 - y) * 2 + 1 - c
    to_core, to_y = {"seq": s_core}, {"seq": s_y}

    odd = lax.rem(f, 2)
    place = (1 - odd) * lax.div(f, 2) + odd * (N - 1 - lax.div(f, 2))

    def at_place(q):
        late = lax.div(q, A)
        return (1 - late) * 2 * q + late * (2 * (N - 1 - q) + 1)

    def ahead(d):
        return at_place(lax.rem(place + d + N, N))

    to_ring = ({"fsdp": ahead(1)}, {"fsdp": ahead(-1)})

    def send(src, dst, ssem, rsem, dev):
        pltpu.make_async_remote_copy(
            src_ref=src, dst_ref=dst, send_sem=ssem, recv_sem=rsem, device_id=dev, device_id_type=MESH
        ).start()

    def arrive(dst, rsem, dev):
        pltpu.make_async_remote_copy(
            src_ref=dst, dst_ref=dst, send_sem=rsem, recv_sem=rsem, device_id=dev, device_id_type=MESH
        ).wait_recv()

    def sent(src, ssem, dev):
        pltpu.make_async_remote_copy(
            src_ref=src, dst_ref=src, send_sem=ssem, recv_sem=ssem, device_id=dev, device_id_type=MESH
        ).wait_send()

    def thirds(first, last):
        count = max(last - first, 0)
        cut = [first + (count * k) // 3 for k in range(4)]
        return [range(cut[k], cut[k + 1]) for k in range(3)]

    quarter = pl.ds(pl.multiple_of(s * DH, DH), DH)

    def rows_of(k, size, half=None):
        if half is None:
            return pl.ds(pl.multiple_of(k * size, size), size)
        return pl.ds(pl.multiple_of(k * size + half * (size // 2), size // 2), size // 2)

    OUT, UP, DN = HP, HP + 1, HP + 2
    blocks = {
        OUT: lambda k, half=None: wout.at[rows_of(k, w, half), quarter],
        UP: lambda k, half=None: wup.at[rows_of(k, w, half)],
        DN: lambda k, half=None: wdn.at[rows_of(k, wf, half)],
    }
    for hp in range(HP):
        blocks[hp] = lambda k, half=None, hp=hp: wqkv.at[rows_of(k, w, half), hp * 384 : hp * 384 + 384]

    def ag_block(m, way, d, back):
        k = ahead(-back if way == 0 else back)
        return blocks[m](k, way if d == H else None)

    def ag_own(m):
        for way in range(2):
            ref = ag_block(m, way, 1, 0)
            send(ref, ref, ag_s.at[m], ag_r.at[m, way, 0], to_ring[way])

    def ag_take(m, d):
        for way in range(2):
            arrive(ag_block(m, way, d, d), ag_r.at[m, way, d - 1], to_ring[way])
            if d < H:
                ref = ag_block(m, way, d + 1, d)
                send(ref, ref, ag_s.at[m], ag_r.at[m, way, d], to_ring[way])

    def ag_fwd(m, third):
        for d in thirds(1, H)[third]:
            ag_take(m, d)

    def ag_last(m):
        ag_take(m, H)

    def ag_sent(m):
        size = (N - 1) * (wf if m == DN else w)
        every = {OUT: wout.at[:size, quarter], UP: wup.at[:size], DN: wdn.at[:size]}
        sent(every[m] if m in every else wqkv.at[:size, m * 384 : m * 384 + 384], ag_s.at[m], to_ring[0])

    def sq_send(kind, ref):
        send(ref(s), ref(s), sq_s.at[kind], sq_r.at[kind, 0], to_core)
        send(ref(s), ref(s), sq_s.at[kind], sq_r.at[kind, 1], to_y)

    def sq_core(kind, ref):
        arrive(ref(s_core), sq_r.at[kind, 0], to_core)

    def sq_relay(kind, ref):
        arrive(ref(s_y), sq_r.at[kind, 1], to_y)
        send(ref(s_y), ref(s_y), sq_s.at[kind], sq_r.at[kind, 2], to_core)

    def sq_diag(kind, ref):
        arrive(ref(s_diag), sq_r.at[kind, 2], to_core)

    def sq_sent(kind, three):
        sent(three, sq_s.at[kind], to_core)

    def x_slot(k):
        return xg.at[k]

    def c_slot(k):
        return cg.at[k]

    def g_slot(k):
        return nrm.at[k]

    def out_slot(k):
        return wout.at[:, pl.ds(pl.multiple_of(k * DH, DH), DH)]

    def ctx_slot(hp):
        return lambda k: ctx.at[k, :, hp * 128 : hp * 128 + 128]

    KX, KC, KG, KO, KCTX, KFIN = 0, 1, 2, 3, 4, 4 + HP

    def order(i):
        hb, lb = lax.div(3 - i, 2), lax.rem(3 - i, 2)
        return lax.rem(y + hb, 2) * 2 + lax.rem(c + lb, 2)

    def seq_across(kind, part, recv):
        send(part.at[1], recv.at[1], rs_s.at[kind], rs_r.at[kind, 1], to_y)

    def seq_stage(i, kind, part, own, recv, value, defer=False):
        @pl.when(i < 3)
        def _():
            part[jnp.minimum(i, 2)] = value.astype(BF)

        @pl.when(i == 0)
        def _():
            send(part.at[0], recv.at[0], rs_s.at[kind], rs_r.at[kind, 0], to_core)

        @pl.when(i == 1)
        def _():
            arrive(recv.at[0], rs_r.at[kind, 0], to_core)
            part[1] = (part[1].astype(F32) + recv[0].astype(F32)).astype(BF)
            if not defer:
                seq_across(kind, part, recv)

        @pl.when(i == 2)
        def _():
            send(part.at[2], recv.at[2], rs_s.at[kind], rs_r.at[kind, 2], to_core)

        @pl.when(i == 3)
        def _():
            own[...] = value

    def seq_sent(kind, part):
        sent(part, rs_s.at[kind], to_core)

    def seq_total(kind, own, recv):
        arrive(recv.at[2], rs_r.at[kind, 2], to_core)
        arrive(recv.at[1], rs_r.at[kind, 1], to_y)
        return own[...] + recv[2].astype(F32) + recv[1].astype(F32)

    grads = {0: (dw_dn, rr_dn, o_dn), 1: (dw_up, rr_up, o_up), 2: (dw_out, rr_out, o_ow)}
    for hp in range(HP):
        grads[3 + hp] = (dw_qkv.at[hp], rr_qkv.at[hp], o_qkv.at[hp])
    MG = 3 + HP

    def rg_rows(m, way, j):
        size = grads[m][0].shape[1]
        return slice(way * (size // 2), (way + 1) * (size // 2)) if j == 0 else slice(0, size)

    def rg_owner(way, j):
        return ahead(H - j if way == 0 else j - H)

    def rg_src(m, way, j):
        return grads[m][0].at[rg_owner(way, j), rg_rows(m, way, j)]

    def rg_send(m, way, j):
        dst = grads[m][1].at[way, j, rg_rows(m, way, j)]
        send(rg_src(m, way, j), dst, rg_s.at[m], rg_r.at[m, way, j], to_ring[way])

    def rg_arrive(m, way, j):
        arrive(grads[m][1].at[way, j, rg_rows(m, way, j)], rg_r.at[m, way, j], to_ring[way])

    def rg_own(m):
        for way in range(2):
            rg_send(m, way, 0)

    def rg_fwd(m, third):
        dw, rr, _ = grads[m]
        for j in thirds(1, H)[third]:
            for way in range(2):
                rows = rg_rows(m, way, j - 1)
                owner = rg_owner(way, j)
                rg_arrive(m, way, j - 1)
                dw[owner, rows] = (dw[owner, rows].astype(F32) + rr[way, j - 1, rows].astype(F32)).astype(dw.dtype)
                rg_send(m, way, j)

    def fin_slot(m):
        return lambda k: grads[m][2].at[k]

    def rg_fin(m):
        dw, rr, out = grads[m]
        total = dw[f].astype(F32)
        for way in range(2):
            rg_arrive(m, way, H - 1)
            total = total + rr[way, H - 1].astype(F32)
        out[s] = total.astype(out.dtype)
        sq_send(KFIN + m, fin_slot(m))

    def rg_sent(m):
        sent(grads[m][0].at[: N - 1], rg_s.at[m], to_ring[0])

    def other(d):
        return lax.rem(f + d, N)

    barrier = pltpu.get_barrier_semaphore()
    peers = [to_core, to_y, {"seq": s_diag}] + [{"fsdp": other(d)} for d in range(1, N)]
    for dev in peers:
        pl.semaphore_signal(barrier, inc=1, device_id=dev, device_id_type=MESH)

    def bring(k, src, dst):
        pltpu.make_async_copy(src, dst, loc_sem.at[k]).start()

    bring(0, tok_in, tok)
    for k in range(8):
        bring(1, vecs_in[k], vecs.at[k])
    bring(2, ub_in, ub4)
    for hp in range(HP):
        for part in range(3):
            cols = pl.ds(pl.multiple_of(part * D + s * DH + hp * 128, 128), 128)
            lo = hp * 384 + part * 128
            bring(3, qkv_in.at[:, cols], wqkv.at[rows_of(f, w), lo : lo + 128])
    bring(4, out_in.at[:, quarter], wout.at[rows_of(f, w), quarter])
    bring(5, cot_in, cot)
    bring(6, len_in, lens)
    if z["up_whole"]:
        for k in range(N):
            cols = pl.ds(pl.multiple_of((k * 4 + s) * wf, wf), wf)
            bring(7, up_in.at[:, cols], wup.at[rows_of(f, w), k * wf : (k + 1) * wf])
    else:
        bring(7, up_in, wup.at[rows_of(f, w)])
    bring(8, dn_in.at[rows_of(s, wf)], wdn.at[rows_of(f, wf)])

    def put(src, dst, k):
        pltpu.make_async_copy(src, dst, put_sem.at[k]).start()

    def padded(ref):
        return jnp.concatenate([ref[...].astype(F32), jnp.zeros((TP - T, D), F32)], axis=0)

    gvec[...] = jnp.zeros_like(gvec)
    own_rows = [tok, vecs, ub4, wqkv.at[rows_of(f, w)], wout.at[rows_of(f, w), quarter], cot, lens, wup.at[rows_of(f, w)], wdn.at[rows_of(f, wf)]]
    for k, dst in enumerate(own_rows):
        pltpu.make_async_copy(dst, dst, loc_sem.at[k]).wait()
    quarters = ub4[...].astype(F32)
    ub = sum(quarters[k : k + 1] * (s == k).astype(F32) for k in range(4))
    vector_rows = [vecs[k].astype(F32) for k in range(8)] + [ub, jnp.zeros((7, 128), F32)]
    smg[f] = jnp.concatenate(vector_rows, axis=0).astype(BF)
    xg[s] = padded(tok).astype(BF)
    cg[s] = padded(cot).astype(BF)
    column = lax.broadcasted_iota(jnp.int32, (1, R), 1)
    slot = sum((column >= TP * k).astype(jnp.int32) for k in range(1, 4))
    inside = column - slot * TP
    valid = (inside < T) & (slot * T + inside < lens[0])
    mask[...] = jnp.where(valid, 0.0, -1e30).astype(F32)
    pl.semaphore_wait(barrier, len(peers))

    for d in range(1, N):
        send(smg.at[f], smg.at[f], sa_s.at[0], sa_r.at[0], {"fsdp": other(d)})
    sq_send(KX, x_slot)
    for m in (0, 1, OUT):
        ag_own(m)
    sq_send(KC, c_slot)
    arrive(smg.at[: N - 1], sa_r.at[0], to_ring[0])
    for j in range(LB):
        piece = smg[j * g].astype(F32)
        for i in range(1, g):
            piece = piece + smg[j * g + i].astype(F32)
        vec[:, j * 128 : (j + 1) * 128] = piece

    def row(k):
        return vec[k : k + 1, :]

    def first_norm(k, into=nrm):
        unit, _ = unit_rows(xg[k].astype(F32))
        into[k] = (unit * row(0) + row(1)).astype(BF)

    def project(hp):
        cols = pl.ds(pl.multiple_of(s * DH + hp * 128, 128), 128)
        bias = jnp.concatenate([vec[2:3, cols], jnp.zeros((1, 128), F32), vec[3:4, cols]], axis=1)
        lanes = lax.broadcasted_iota(jnp.int32, (1, 384), 1)
        scale = jnp.where(lanes < 128, HEAD_DIM ** (-0.5), 1.0).astype(F32)
        here = slice(hp * 384, hp * 384 + 384)

        @pl.loop(0, 4)
        def _(k):
            pq[k, :, here] = ((dot_nn(nrm[k], wqkv[:, here]) + bias) * scale).astype(BF)

    first_norm(s)
    ag_fwd(0, 0)
    sq_core(KX, x_slot)
    first_norm(s_core)
    ag_fwd(1, 0)
    ag_fwd(OUT, 0)
    ag_fwd(0, 1)
    ag_fwd(1, 1)
    ag_fwd(OUT, 1)
    sq_relay(KX, x_slot)
    first_norm(s_y)
    ag_fwd(0, 2)
    ag_fwd(1, 2)
    ag_fwd(OUT, 2)
    ag_own(UP)
    ag_own(DN)
    sq_diag(KX, x_slot)
    first_norm(s_diag)
    ag_last(0)
    project(0)

    flat = pq.reshape(R, HP * 384)
    lane = lax.broadcasted_iota(jnp.int32, (1, 128), 1)
    first = (lane < HEAD_DIM).astype(F32)
    picks = (first.astype(BF), (1.0 - first).astype(BF))

    def lanes_at(off):
        return pl.ds(pl.multiple_of(off, 128), 128)

    def slot_rows(k):
        return pl.ds(pl.multiple_of(k * TP, 16), TP)

    @pl.loop(0, 8)
    def _(t):
        hp, k = lax.div(t, 4), lax.rem(t, 4)
        query = pq[k, :, lanes_at(hp * 384)]
        keys = flat[:, lanes_at(hp * 384 + 128)]
        vals = flat[:, lanes_at(hp * 384 + 256)]
        both, logs = [], []
        for h in range(2):
            scores = dot_nt(query * picks[h], keys) + mask[...]
            top = jnp.max(scores, axis=-1, keepdims=True)
            grown = jnp.exp(scores - top)
            total = jnp.sum(grown, axis=-1, keepdims=True)
            logs.append(top + jnp.log(total))
            both.append(dot_nn((grown * (1.0 / total)).astype(BF), vals))
        rows = slot_rows(k)
        ctx[s, rows, lanes_at(hp * 128)] = jnp.where(lane < HEAD_DIM, both[0], both[1]).astype(BF)
        lse[hp, rows, :] = jnp.where(lane < HEAD_DIM, logs[0], logs[1])

        @pl.when(t == 0)
        def _():
            ag_last(OUT)
            sq_send(KO, out_slot)
            ag_last(1)
            project(1)

        @pl.when(t == 2)
        def _():
            ag_fwd(UP, 0)
            sq_relay(KC, c_slot)

        @pl.when(t == 3)
        def _():
            sq_send(KCTX, ctx_slot(0))

        @pl.when(t == 6)
        def _():
            ag_fwd(UP, 1)
            ag_fwd(DN, 0)

        @pl.when(t == 7)
        def _():
            sq_send(KCTX + 1, ctx_slot(1))

    sq_relay(KO, out_slot)
    sq_relay(KCTX, ctx_slot(0))
    sq_core(KO, out_slot)
    sq_diag(KO, out_slot)
    sq_core(KCTX, ctx_slot(0))
    sq_core(KCTX + 1, ctx_slot(1))
    ag_fwd(UP, 2)
    sq_relay(KCTX + 1, ctx_slot(1))
    sq_diag(KCTX, ctx_slot(0))
    sq_diag(KCTX + 1, ctx_slot(1))

    @pl.loop(0, 4)
    def _(i):
        k = order(i)
        joined = jnp.concatenate([ctx[j, slot_rows(k), :] for j in range(4)], axis=1)
        value = xg[k].astype(F32) + dot_nn(joined, wout[...]) + row(4)
        unit, _ = unit_rows(value)
        n2[k] = (unit * row(5) + row(6)).astype(BF)

        @pl.when(i == 3)
        def _():
            mid[...] = value

        @pl.when(i == 0)
        def _():
            ag_fwd(DN, 1)

    sq_core(KC, c_slot)
    sq_diag(KC, c_slot)
    ag_last(UP)

    @pl.loop(0, 4)
    def _(k):
        before = dot_nn(n2[k], wup[...]) + row(8)
        cdf = 0.5 + 0.5 * lax.erf(before * (0.5**0.5))
        slope = cdf + before * (jnp.exp(before * before * -0.5) * (1.0 / math.sqrt(2.0 * math.pi)))
        hid[k] = (before * cdf).astype(BF)
        gbf[k] = slope.astype(BF)

    ag_fwd(DN, 2)

    def weight_grad(left, right, dw, size):
        per = max(256 // size, 1)

        @pl.loop(0, dw.shape[0] // per)
        def _(i):
            lo = pl.ds(pl.multiple_of(i * per * size, per * size), per * size)
            value = dot_tn(left[:, lo], right).astype(BF)
            for j in range(per):
                dw[i * per + j] = value[j * size : (j + 1) * size]

    weight_grad(hid.reshape(R, D), cg.reshape(R, D)[...], dw_dn, wf)
    rg_own(0)
    ag_last(DN)

    @pl.loop(0, 4)
    def _(i):
        k = order(i)
        grad = (dot_nt(cg[k], wdn[...]) * gbf[k].astype(F32)).astype(BF)
        gbf[k] = grad
        gvec[8:9, :] += jnp.sum(grad.astype(F32), axis=0, keepdims=True)
        seq_stage(i, 0, gpart, gown, grecv, dot_nt(grad, wup[...]))

        @pl.when(i == 2)
        def _():
            rg_fwd(0, 0)

    weight_grad(n2.reshape(R, D), gbf.reshape(R, D)[...], dw_up, w)
    rg_own(1)

    @pl.loop(0, 4)
    def _(k):
        first_norm(k, n2)

    rg_fwd(0, 1)

    @pl.loop(0, 4)
    def _(i):
        seq_stage(i, 1, opart, oown, orecv, dot_nn(hid[order(i)], wdn[...]), defer=True)

    rg_fwd(1, 0)

    gn = seq_total(0, gown, grecv)
    seq_sent(0, gpart)
    unit, rate = unit_rows(mid[...])
    gvec[5:6, :] = jnp.sum(gn * unit, axis=0, keepdims=True)
    gvec[6:7, :] = jnp.sum(gn, axis=0, keepdims=True)
    c_own = cg[s].astype(F32)
    gvec[7:8, :] = jnp.sum(c_own, axis=0, keepdims=True)
    gm = c_own + norm_pull(gn, row(5), unit, rate)
    gmid[...] = gm
    branch = gm.astype(BF)
    gvec[4:5, :] = jnp.sum(branch.astype(F32), axis=0, keepdims=True)
    nrm[s] = branch
    sq_send(KG, g_slot)

    seq_across(1, opart, orecv)

    flat_g = gctx.reshape(R, DH)
    dkt[...] = jnp.zeros_like(dkt)
    dvt[...] = jnp.zeros_like(dvt)

    def branch_back(k):
        gctx[k] = dot_nt(nrm[k], wout[pl.ds(pl.multiple_of(s * DH, DH), DH), :]).astype(BF)

    def close_pair(hp):
        lo = hp * 384
        flat[:, lo + 128 : lo + 256] = dkt[hp].T.astype(BF)
        flat[:, lo + 256 : lo + 384] = dvt[hp].T.astype(BF)
        weight_grad(n2.reshape(R, D), flat[:, lo : lo + 384], dw_qkv.at[hp], w)
        rg_own(3 + hp)
        off = lanes_at(s * DH + hp * 128)
        gvec[2:3, off] = jnp.sum(flat[:, lo : lo + 128].astype(F32), axis=0, keepdims=True)
        gvec[3:4, off] = jnp.sum(flat[:, lo + 256 : lo + 384].astype(F32), axis=0, keepdims=True)

    branch_back(s)
    sq_core(KG, g_slot)
    branch_back(s_core)

    @pl.loop(0, 8)
    def _(t):
        late, u = lax.div(t, 4), lax.rem(t, 4)
        hp = (1 - late) * lax.rem(u, 2) + late * lax.div(u, 2)
        flip = (1 - late) * lax.div(u, 2) + late * lax.rem(u, 2)
        k = lax.rem(y + late, 2) * 2 + lax.rem(c + flip, 2)
        query = pq[k, :, lanes_at(hp * 384)]
        keys = flat[:, lanes_at(hp * 384 + 128)]
        vals = flat[:, lanes_at(hp * 384 + 256)]
        grad = gctx[k, :, lanes_at(hp * 128)]
        logs = lse[hp, slot_rows(k), :]
        both = []
        for h in range(2):
            qh, gh = query * picks[h], grad * picks[h]
            probs = jnp.exp(dot_nt(qh, keys) + mask[...] - logs[:, h * HEAD_DIM : h * HEAD_DIM + 1])
            dp = dot_nt(gh, vals)
            inner = jnp.sum(probs * dp, axis=-1, keepdims=True)
            ds = (probs * (dp - inner)).astype(BF)
            both.append(dot_nn(ds, keys))
            dkt[hp] += dot_tn(qh, ds)
            dvt[hp] += dot_tn(gh, probs.astype(BF))
        dq = jnp.where(lane < HEAD_DIM, both[0], both[1]) * HEAD_DIM ** (-0.5)
        pq[k, :, lanes_at(hp * 384)] = dq.astype(BF)

        @pl.when(t == 0)
        def _():
            rg_fwd(0, 2)

        @pl.when(t == 1)
        def _():
            rg_fwd(1, 1)

        @pl.when(t == 3)
        def _():
            sq_relay(KG, g_slot)
            branch_back(s_y)
            sq_diag(KG, g_slot)
            branch_back(s_diag)
            right = nrm.reshape(R, D)[:, quarter]
            for j in range(4):
                value = dot_tn(ctx[j], right).astype(BF)
                for i in range(DH // w):
                    dw_out[j * (DH // w) + i] = value[i * w : (i + 1) * w]
            rg_own(2)
            rg_fin(0)

        @pl.when(t == 4)
        def _():
            rg_fwd(2, 0)
            rg_fwd(1, 2)

        @pl.when(t == 5)
        def _():
            close_pair(0)
            rg_fwd(2, 1)

        @pl.when(t == 6)
        def _():
            rg_fin(1)

        @pl.when(t == 7)
        def _():
            rg_fwd(3, 0)
            rg_fwd(2, 2)

    close_pair(1)
    rg_fwd(3, 1)

    @pl.loop(0, 4)
    def _(i):
        seq_stage(i, 2, gpart, gown, grecv, dot_nt(pq[order(i)], wqkv[...]))

        @pl.when(i == 2)
        def _():
            rg_fwd(4, 0)
            rg_fwd(3, 2)

    arrive(orecv.at[2], rs_r.at[1, 2], to_core)
    arrive(orecv.at[1], rs_r.at[1, 1], to_y)
    tok[...] = (mid[...] + (oown[...] + orecv[2].astype(F32) + orecv[1].astype(F32)) + row(7))[:T].astype(BF)
    put(tok, h_out, 6)
    rg_fin(2)
    arrive(grecv.at[2], rs_r.at[2, 2], to_core)
    here = gown[...] + grecv[2].astype(F32)
    away = gpart[1].astype(F32)
    unit, rate = unit_rows(xg[s].astype(F32))
    unit_y, _ = unit_rows(xg[s_y].astype(F32))
    gvec[0:1, :] = jnp.sum(here * unit + away * unit_y, axis=0, keepdims=True)
    gvec[1:2, :] = jnp.sum(here + away, axis=0, keepdims=True)
    for k in range(N):
        j = k // g
        dw_sm[k] = gvec[:, j * 128 : (j + 1) * 128]
    for d in range(1, N):
        send(dw_sm.at[other(d)], rr_sm.at[d - 1], sg_s.at[0], sg_r.at[0], {"fsdp": other(d)})
    rg_fwd(4, 1)
    rg_fin(3)
    total = dw_sm[f]
    arrive(rr_sm, sg_r.at[0], to_ring[0])
    for d in range(1, N):
        total = total + rr_sm[d - 1]
    o_sm[s] = total
    for dev in (to_core, to_y, {"seq": s_diag}):
        send(o_sm.at[s], o_sm.at[s], sm_s.at[0], sm_r.at[0], dev)
    rg_fwd(4, 2)

    hbm = [h_dn, h_up, h_ow] + [h_qkv.at[hp] for hp in range(HP)]
    finals = [(KFIN + m, fin_slot(m)) for m in range(MG)]

    def put_slot(m, k):
        put(grads[m][2].at[k], hbm[m].at[k], m)

    def relay_out(m):
        sq_relay(*finals[m])
        put_slot(m, s_y)

    put_slot(0, s)
    put_slot(1, s)
    put_slot(2, s)
    put_slot(3, s)
    relay_out(0)
    arrive(grecv.at[1], rs_r.at[2, 1], to_y)
    gn = here + grecv[1].astype(F32)
    cot[...] = (gmid[...] + norm_pull(gn, row(0), unit, rate))[:T].astype(BF)
    put(cot, h_tok, 7)
    rg_fin(4)
    put_slot(4, s)
    for m in range(MG):
        sq_core(*finals[m])
        put_slot(m, s_core)
    for m in range(1, MG):
        relay_out(m)
    arrive(o_sm.at[:3], sm_r.at[0], to_core)
    put(o_sm, h_sm, 5)
    for m in range(MG):
        sq_diag(*finals[m])
        put_slot(m, s_diag)

    for m in range(3 + HP):
        ag_sent(m)
    for m in range(MG):
        rg_sent(m)
    for kind, ref in ((KX, xg), (KC, cg), (KG, nrm)):
        sq_sent(kind, ref.at[:3])
    sq_sent(KO, wout.at[:, : 3 * DH])
    for hp in range(HP):
        sq_sent(KCTX + hp, ctx.at[:3, :, hp * 128 : hp * 128 + 128])
    for m in range(MG):
        sq_sent(KFIN + m, grads[m][2].at[:3])
    seq_sent(1, opart)
    seq_sent(2, gpart)
    sent(smg.at[: N - 1], sa_s.at[0], to_ring[0])
    sent(dw_sm.at[: N - 1], sg_s.at[0], to_ring[0])
    sent(o_sm.at[:3], sm_s.at[0], to_core)
    for src, dst, k in [(grads[m][2], hbm[m], m) for m in range(MG)] + [(o_sm, h_sm, 5), (tok, h_out, 6), (cot, h_tok, 7)]:
        pltpu.make_async_copy(src, dst, put_sem.at[k]).wait()


def finish_kernel(z, *refs):
    srcs, dsts = refs[:7], refs[7:22]
    (out, tok, gq, go, gu, gd, gs), bufs = refs[22:29], refs[29:42]
    s_in, s_out = refs[42:]
    D, w, wf, HP, N = z["D"], z["w"], z["wf"], z["HP"], 2 * z["A"]
    DH = D // 4
    loads = [pltpu.make_async_copy(src, dst, s_in.at[k]) for k, (src, dst) in enumerate(zip(srcs, (out, tok, gq, go, gu, gd, gs)))]
    saves = []

    def save(src, k):
        copy = pltpu.make_async_copy(src, dsts[k], s_out.at[k])
        copy.start()
        saves.append(copy)

    for k in (5, 4, 2, 3, 6, 0, 1):
        loads[k].start()
    f_qkv, f_ow, f_up, f_dn = bufs[:4]
    loads[5].wait()
    for s in range(4):
        f_dn[s * wf : (s + 1) * wf] = gd[s].astype(F32)
    save(f_dn, 5)
    loads[4].wait()
    if z["up_whole"]:
        for s in range(4):
            for k in range(N):
                f_up[:, (k * 4 + s) * wf : (k * 4 + s + 1) * wf] = gu[s, :, k * wf : (k + 1) * wf].astype(F32)
    else:
        f_up[...] = gu[...].astype(F32)
    save(f_up, 4)
    loads[2].wait()
    for s in range(4):
        for hp in range(HP):
            for part in range(3):
                lo = part * D + s * DH + hp * 128
                f_qkv[:, lo : lo + 128] = gq[hp, s, :, part * 128 : part * 128 + 128].astype(F32)
    save(f_qkv, 2)
    loads[3].wait()
    for s in range(4):
        f_ow[:, s * DH : (s + 1) * DH] = go[s].astype(F32)
    save(f_ow, 3)
    loads[6].wait()
    total = gs[0] + gs[1] + gs[2] + gs[3]
    for k in range(8):
        bufs[4 + k][...] = total[k : k + 1]
        save(bufs[4 + k], 6 + k)
    bufs[12][...] = jnp.concatenate([gs[s, 8:9] for s in range(4)], axis=1)
    save(bufs[12], 14)
    for k, buf in ((0, out), (1, tok)):
        loads[k].wait()
        save(buf, k)
    for copy in saves:
        copy.wait()


def make_body(mesh):
    N = mesh.shape["fsdp"]
    A = N // 2

    def body(
        tokens, lengths, ln1_gain, ln1_bias, qkv_weight, q_bias, v_bias, out_weight, out_bias,
        ln2_gain, ln2_bias, up_weight, up_bias, down_weight, down_bias, cotangent,
    ):
        _, T, D = tokens.shape
        w, FF = D // N, up_weight.shape[1]
        wf = FF // (4 * N)
        TP = -(-T // 16) * 16
        R = 4 * TP
        DH = D // 4
        HP = DH // 128
        FQ = FF // 4
        assert FQ == D and wf == w and HP == 2
        g = max(128 // w, 1)
        s = lax.axis_index("seq")
        f = lax.axis_index("fsdp")
        up_whole = wf % 128 == 0
        plain = (ln1_gain, ln1_bias, q_bias, v_bias, out_bias, ln2_gain, ln2_bias, down_bias)
        if g == 1:
            vectors_in = [v.reshape(1, w) for v in plain]
            ub_in = up_bias.reshape(4, wf)
        else:
            spot = lax.rem(f, g) * w
            blank = jnp.zeros((1, 128), BF)
            vectors_in = [lax.dynamic_update_slice(blank, v[None], (0, spot)) for v in plain]
            mine = lax.dynamic_slice(up_bias, (s * wf,), (wf,))
            ub_in = lax.dynamic_update_slice(jnp.zeros((4, 128), BF), mine[None], (s, spot))
        if not up_whole:
            up_weight = lax.dynamic_index_in_dim(up_weight.reshape(w, N, 4, wf), s, 2, False).reshape(w, FQ)
        z = dict(D=D, T=T, TP=TP, R=R, A=A, w=w, wf=wf, HP=HP, g=g, up_whole=up_whole)
        vm = pltpu.VMEM
        C = 384
        scratch = [
            vm((T, D), BF), vm((T, D), BF), pltpu.SMEM((1,), jnp.int32), vm((8, 1, 128), BF), vm((4, 128), BF),
            vm((HP, 4, w, C), BF), vm((4, w, DH), BF), vm((4, w, FQ), BF), vm((4, wf, D), BF), vm((4, 16, 128), F32),
            vm((4, TP, D), BF),
            vm((4, TP, D), BF),
            vm((4, TP, D), BF),
            vm((4, R, DH), BF),
            vm((4, TP, D), BF),
            vm((4, TP, D), BF),
            vm((4, TP, D), BF),
            vm((4, TP, HP * C), BF),
            vm((D, HP * C), BF),
            vm((D, D), BF),
            vm((D, FQ), BF),
            vm((FQ, D), BF),
            vm((N, 16, 128), BF),
            vm((16, D), F32),
            vm((16, D), F32),
            vm((HP, R, 128), F32),
            vm((TP, D), F32),
            vm((TP, D), F32),
            vm((4, TP, DH), BF),
            vm((HP, 128, R), F32),
            vm((HP, 128, R), F32),
            vm((3, TP, D), BF), vm((TP, D), F32), vm((3, TP, D), BF),
            vm((3, TP, D), BF), vm((TP, D), F32), vm((3, TP, D), BF),
            vm((1, R), F32),
            vm((HP, N, w, C), BF), vm((N, w, DH), BF), vm((N, w, FQ), BF), vm((N, wf, D), BF), vm((N, 16, 128), F32),
            vm((HP, 2, A, w, C), BF), vm((2, A, w, DH), BF), vm((2, A, w, FQ), BF), vm((2, A, wf, D), BF), vm((N - 1, 16, 128), F32),
        ]
        dma = pltpu.SemaphoreType.DMA
        scratch += [
            dma((9,)), dma((8,)),
            dma((3 + HP,)), dma((3 + HP, 2, A)), dma((3 + HP,)), dma((3 + HP, 2, A)),
            dma((7 + 2 * HP,)), dma((7 + 2 * HP, 3)),
            dma((3,)), dma((3, 3)),
            dma((1,)), dma((1,)), dma((1,)), dma((1,)), dma((1,)), dma((1,)),
        ]
        there = pl.BlockSpec(memory_space=pl.ANY)
        out_shapes = [
            jax.ShapeDtypeStruct((T, D), BF),
            jax.ShapeDtypeStruct((T, D), BF),
            jax.ShapeDtypeStruct((HP, 4, w, C), BF),
            jax.ShapeDtypeStruct((4, w, DH), BF),
            jax.ShapeDtypeStruct((4, w, FQ), BF),
            jax.ShapeDtypeStruct((4, wf, D), BF),
            jax.ShapeDtypeStruct((4, 16, 128), F32),
        ]
        out, gtok, gq, go, gu, gd, gs = pl.pallas_call(
            functools.partial(layer_entry, z),
            out_shape=out_shapes,
            in_specs=[there] * 16,
            out_specs=[there] * 7,
            scratch_shapes=scratch,
            compiler_params=pltpu.CompilerParams(
                collective_id=0, has_side_effects=True, vmem_limit_bytes=67_000_000
            ),
            name="layer",
        )(tokens[0], cotangent[0], lengths, *vectors_in, ub_in, qkv_weight, out_weight, up_weight, down_weight)

        if not up_whole:
            gu = gu.reshape(4, w, N, wf).transpose(1, 2, 0, 3).reshape(w, FF)
        if g > 1:
            gs = lax.dynamic_slice(gs, (0, 0, lax.rem(f, g) * w), (4, 16, w))
        shapes = [((w, 3 * D), F32), ((w, D), F32), ((w, FF), F32), ((4 * wf, D), F32)]
        shapes += [((1, w), F32)] * 8 + [((1, 4 * wf), F32)]
        sources = (out, gtok, gq, go, gu, gd, gs)
        done = pl.pallas_call(
            functools.partial(finish_kernel, z),
            out_shape=[jax.ShapeDtypeStruct(*v) for v in [((T, D), BF)] * 2 + shapes],
            in_specs=[there] * 7,
            out_specs=[there] * 15,
            scratch_shapes=[vm(v.shape, v.dtype) for v in sources] + [vm(*v) for v in shapes] + [dma((7,)), dma((15,))],
            name="finish",
        )(*sources)
        out, gtok, g_qkv, g_out, g_up, g_down = done[:6]
        sums = [v.reshape(-1) for v in done[6:]]
        return (
            out[None], gtok[None], sums[0], sums[1], g_qkv, sums[2], sums[3], g_out, sums[4],
            sums[5], sums[6], g_up, sums[8], g_down, sums[7],
        )

    return body


def solution(mesh):
    row, mat, act = P("fsdp"), P("fsdp", None), P("fsdp", "seq", None)
    return jax.shard_map(
        make_body(mesh),
        mesh=mesh,
        in_specs=(act, row, row, row, mat, row, row, mat, row, row, row, mat, row, mat, row, act),
        out_specs=(act, act, row, row, mat, row, row, mat, row, row, row, mat, row, mat, row),
        check_vma=False,
    )
```

```python
import functools
import math

import jax
import jax.numpy as jnp
from jax import lax
from jax.experimental import pallas as pl
from jax.experimental.pallas import tpu as pltpu
from jax.sharding import PartitionSpec as P

HEAD_DIM = 64
BF = jnp.bfloat16
F32 = jnp.float32
MESH = pl.DeviceIdType.MESH


def dot_nn(left, right):
    return lax.dot_general(left, right, (((1,), (0,)), ((), ())), preferred_element_type=F32)


def dot_nt(left, right):
    return lax.dot_general(left, right, (((1,), (1,)), ((), ())), preferred_element_type=F32)


def dot_tn(left, right):
    return lax.dot_general(left, right, (((0,), (0,)), ((), ())), preferred_element_type=F32)


def unit_rows(values):
    center = values - jnp.mean(values, axis=-1, keepdims=True)
    rate = lax.rsqrt(jnp.mean(center * center, axis=-1, keepdims=True) + 1e-6)
    return center * rate, rate


def norm_pull(grad, gain, unit, rate):
    scaled = grad * gain
    return rate * (
        scaled
        - jnp.mean(scaled, axis=-1, keepdims=True)
        - unit * jnp.mean(scaled * unit, axis=-1, keepdims=True)
    )


def layer_entry(z, *refs):
    layer_kernel(z, *refs[:3], refs[3:11], *refs[11:])


def layer_kernel(
    z,
    tok_in, cot_in, len_in, vecs_in, ub_in, qkv_in, out_in, up_in, dn_in,
    h_out, h_tok, h_qkv, h_ow, h_up, h_dn, h_sm,
    tok, cot, lens, vecs, ub4, o_qkv, o_ow, o_up, o_dn, o_sm,
    xg, cg, nrm, ctx, n2, hid, gbf, pq, wqkv, wout, wup, wdn, smg, vec, gvec, lse, mid, gmid,
    gctx, dkt, dvt, gpart, gown, grecv, opart, oown, orecv, mask,
    dw_qkv, dw_out, dw_up, dw_dn, dw_sm, rr_qkv, rr_out, rr_up, rr_dn, rr_sm,
    loc_sem, put_sem, ag_s, ag_r, rg_s, rg_r, sq_s, sq_r, rs_s, rs_r, sa_s, sa_r, sg_s, sg_r, sm_s, sm_r,
):
    D, T, TP, R, A, w, wf, HP = z["D"], z["T"], z["TP"], z["R"], z["A"], z["w"], z["wf"], z["HP"]
    N, H, DH, LB, g = 2 * A, A, D // 4, D // 128, z["g"]
    s = lax.axis_index("seq")
    f = lax.axis_index("fsdp")
    y, c = lax.div(s, 2), lax.rem(s, 2)
    s_core, s_y, s_diag = y * 2 + 1 - c, (1 - y) * 2 + c, (1 - y) * 2 + 1 - c
    to_core, to_y = {"seq": s_core}, {"seq": s_y}

    odd = lax.rem(f, 2)
    place = (1 - odd) * lax.div(f, 2) + odd * (N - 1 - lax.div(f, 2))

    def at_place(q):
        late = lax.div(q, A)
        return (1 - late) * 2 * q + late * (2 * (N - 1 - q) + 1)

    def ahead(d):
        return at_place(lax.rem(place + d + N, N))

    to_ring = ({"fsdp": ahead(1)}, {"fsdp": ahead(-1)})

    def send(src, dst, ssem, rsem, dev):
        pltpu.make_async_remote_copy(
            src_ref=src, dst_ref=dst, send_sem=ssem, recv_sem=rsem, device_id=dev, device_id_type=MESH
        ).start()

    def arrive(dst, rsem, dev):
        pltpu.make_async_remote_copy(
            src_ref=dst, dst_ref=dst, send_sem=rsem, recv_sem=rsem, device_id=dev, device_id_type=MESH
        ).wait_recv()

    def sent(src, ssem, dev):
        pltpu.make_async_remote_copy(
            src_ref=src, dst_ref=src, send_sem=ssem, recv_sem=ssem, device_id=dev, device_id_type=MESH
        ).wait_send()

    def thirds(first, last):
        count = max(last - first, 0)
        cut = [first + (count * k) // 3 for k in range(4)]
        return [range(cut[k], cut[k + 1]) for k in range(3)]

    quarter = pl.ds(pl.multiple_of(s * DH, DH), DH)

    def rows_of(k, size, half=None):
        if half is None:
            return pl.ds(pl.multiple_of(k * size, size), size)
        return pl.ds(pl.multiple_of(k * size + half * (size // 2), size // 2), size // 2)

    OUT, UP, DN = HP, HP + 1, HP + 2
    blocks = {
        OUT: lambda k, half=None: wout.at[rows_of(k, w, half), quarter],
        UP: lambda k, half=None: wup.at[rows_of(k, w, half)],
        DN: lambda k, half=None: wdn.at[rows_of(k, wf, half)],
    }
    for hp in range(HP):
        blocks[hp] = lambda k, half=None, hp=hp: wqkv.at[rows_of(k, w, half), hp * 384 : hp * 384 + 384]

    def ag_block(m, way, d, back):
        k = ahead(-back if way == 0 else back)
        return blocks[m](k, way if d == H else None)

    def ag_own(m):
        for way in range(2):
            ref = ag_block(m, way, 1, 0)
            send(ref, ref, ag_s.at[m], ag_r.at[m, 0], to_ring[way])

    def ag_take(m, d):
        arrive(ag_rows(m, 1 if d == H else 2), ag_r.at[m, d - 1], to_ring[0])
        for way in range(2):
            if d < H:
                ref = ag_block(m, way, d + 1, d)
                send(ref, ref, ag_s.at[m], ag_r.at[m, d], to_ring[way])

    def ag_fwd(m, third):
        for d in thirds(1, H)[third]:
            ag_take(m, d)

    def ag_last(m):
        ag_take(m, H)

    def ag_rows(m, shards):
        size = shards * (wf if m == DN else w)
        every = {OUT: wout.at[:size, quarter], UP: wup.at[:size], DN: wdn.at[:size]}
        return every[m] if m in every else wqkv.at[:size, m * 384 : m * 384 + 384]

    def ag_sent(m):
        sent(ag_rows(m, N - 1), ag_s.at[m], to_ring[0])

    def sq_send(kind, ref):
        send(ref(s), ref(s), sq_s.at[kind], sq_r.at[kind, 0], to_core)
        send(ref(s), ref(s), sq_s.at[kind], sq_r.at[kind, 1], to_y)

    def sq_core(kind, ref):
        arrive(ref(s_core), sq_r.at[kind, 0], to_core)

    def sq_relay(kind, ref):
        arrive(ref(s_y), sq_r.at[kind, 1], to_y)
        send(ref(s_y), ref(s_y), sq_s.at[kind], sq_r.at[kind, 2], to_core)

    def sq_diag(kind, ref):
        arrive(ref(s_diag), sq_r.at[kind, 2], to_core)

    def sq_sent(kind, three):
        sent(three, sq_s.at[kind], to_core)

    def x_slot(k):
        return xg.at[k]

    def c_slot(k):
        return cg.at[k]

    def g_slot(h):
        return lambda k: nrm.at[k, halves[h]]

    def out_slot(k):
        return wout.at[:, pl.ds(pl.multiple_of(k * DH, DH), DH)]

    def ctx_slot(hp):
        return lambda k: ctx.at[k, :, hp * 128 : hp * 128 + 128]

    KX, KC, KG, KO, KCTX, KFIN = 0, 1, 2, 4, 5, 5 + HP

    def order(i):
        hb, lb = lax.div(3 - i, 2), lax.rem(3 - i, 2)
        return lax.rem(y + hb, 2) * 2 + lax.rem(c + lb, 2)

    cut = -(-TP // 32) * 16
    halves = (slice(0, cut), slice(cut, TP))

    def seq_across(kind, part, recv, h):
        send(part.at[1, halves[h]], recv.at[1, halves[h]], rs_s.at[kind], rs_r.at[kind, 1, h], to_y)

    def seq_pass(kind, part, own, recv, compute, defer=False, poll=None):
        def chip_sum(h):
            rows = halves[h]
            arrive(recv.at[0, rows], rs_r.at[kind, 0, h], to_core)
            part[1, rows] = (part[1, rows].astype(F32) + recv[0, rows].astype(F32)).astype(BF)
            if not defer:
                seq_across(kind, part, recv, h)

        @pl.loop(0, 2)
        def _(p):
            chip = lax.rem(y + 1 - p, 2) * 2
            theirs, ours = chip + 1 - c, chip + c
            for h, rows in enumerate(halves):
                count = rows.stop - rows.start
                value = compute(theirs, ours, rows)

                @pl.when(p == 0)
                def _():
                    part[0, rows] = value[:count].astype(BF)
                    part[1, rows] = value[count:].astype(BF)
                    send(part.at[0, rows], recv.at[0, rows], rs_s.at[kind], rs_r.at[kind, 0, h], to_core)
                    if h == 1:
                        chip_sum(0)

                @pl.when(p == 1)
                def _():
                    part[2, rows] = value[:count].astype(BF)
                    own[rows] = value[count:]
                    send(part.at[2, rows], recv.at[2, rows], rs_s.at[kind], rs_r.at[kind, 2, h], to_core)
                    if h == 0:
                        chip_sum(1)
                        if poll:
                            poll()

    def both_rows(ref, theirs, ours, rows):
        return jnp.concatenate([ref[theirs, rows], ref[ours, rows]], axis=0)

    def seq_sent(kind, part):
        sent(part, rs_s.at[kind], to_core)

    def from_core(kind, recv, h):
        arrive(recv.at[2, halves[h]], rs_r.at[kind, 2, h], to_core)

    def from_y(kind, recv, h):
        arrive(recv.at[1, halves[h]], rs_r.at[kind, 1, h], to_y)

    grads = {0: (dw_dn, rr_dn, o_dn), 1: (dw_up, rr_up, o_up), 2: (dw_out, rr_out, o_ow)}
    for hp in range(HP):
        grads[3 + hp] = (dw_qkv.at[hp], rr_qkv.at[hp], o_qkv.at[hp])
    MG = 3 + HP

    def rg_rows(m, way, j):
        size = grads[m][0].shape[1]
        return slice(way * (size // 2), (way + 1) * (size // 2)) if j == 0 else slice(0, size)

    def rg_owner(way, j):
        return ahead(H - j if way == 0 else j - H)

    def rg_src(m, way, j):
        return grads[m][0].at[rg_owner(way, j), rg_rows(m, way, j)]

    def rg_send(m, way, j):
        dst = grads[m][1].at[way, j, rg_rows(m, way, j)]
        send(rg_src(m, way, j), dst, rg_s.at[m], rg_r.at[m, j], to_ring[way])

    def rg_arrive(m, j):
        arrive(grads[m][0].at[: 1 if j == 0 else 2], rg_r.at[m, j], to_ring[0])

    def rg_own(m):
        for way in range(2):
            rg_send(m, way, 0)

    def rg_fwd(m, third):
        dw, rr, _ = grads[m]
        for j in thirds(1, H)[third]:
            rg_arrive(m, j - 1)
            for way in range(2):
                rows = rg_rows(m, way, j - 1)
                owner = rg_owner(way, j)
                dw[owner, rows] = (dw[owner, rows].astype(F32) + rr[way, j - 1, rows].astype(F32)).astype(dw.dtype)
                rg_send(m, way, j)

    def fin_slot(m):
        return lambda k: grads[m][2].at[k]

    def rg_fin(m):
        dw, rr, out = grads[m]
        total = dw[f].astype(F32)
        rg_arrive(m, H - 1)
        for way in range(2):
            total = total + rr[way, H - 1].astype(F32)
        out[s] = total.astype(out.dtype)
        sq_send(KFIN + m, fin_slot(m))

    def rg_sent(m):
        sent(grads[m][0].at[: N - 1], rg_s.at[m], to_ring[0])

    def other(d):
        return lax.rem(f + d, N)

    barrier = pltpu.get_barrier_semaphore()
    peers = [to_core, to_y, {"seq": s_diag}] + [{"fsdp": other(d)} for d in range(1, N)]
    for dev in peers:
        pl.semaphore_signal(barrier, inc=1, device_id=dev, device_id_type=MESH)

    def bring(k, src, dst):
        pltpu.make_async_copy(src, dst, loc_sem.at[k]).start()

    bring(0, tok_in, tok)
    for k in range(8):
        bring(1, vecs_in[k], vecs.at[k])
    bring(2, ub_in, ub4)
    for hp in range(HP):
        for part in range(3):
            cols = pl.ds(pl.multiple_of(part * D + s * DH + hp * 128, 128), 128)
            lo = hp * 384 + part * 128
            bring(3, qkv_in.at[:, cols], wqkv.at[rows_of(f, w), lo : lo + 128])
    bring(4, out_in.at[:, quarter], wout.at[rows_of(f, w), quarter])
    bring(5, cot_in, cot)
    bring(6, len_in, lens)
    if z["up_whole"]:
        for k in range(N):
            cols = pl.ds(pl.multiple_of((k * 4 + s) * wf, wf), wf)
            bring(7, up_in.at[:, cols], wup.at[rows_of(f, w), k * wf : (k + 1) * wf])
    else:
        bring(7, up_in, wup.at[rows_of(f, w)])
    bring(8, dn_in.at[rows_of(s, wf)], wdn.at[rows_of(f, wf)])

    def put(src, dst, k):
        pltpu.make_async_copy(src, dst, put_sem.at[k]).start()

    def padded(ref):
        return jnp.concatenate([ref[...].astype(F32), jnp.zeros((TP - T, D), F32)], axis=0)

    gvec[...] = jnp.zeros_like(gvec)
    own_rows = [tok, vecs, ub4, wqkv.at[rows_of(f, w)], wout.at[rows_of(f, w), quarter], cot, lens, wup.at[rows_of(f, w)], wdn.at[rows_of(f, wf)]]
    for k, dst in enumerate(own_rows):
        pltpu.make_async_copy(dst, dst, loc_sem.at[k]).wait()
    quarters = ub4[...].astype(F32)
    ub = sum(quarters[k : k + 1] * (s == k).astype(F32) for k in range(4))
    vector_rows = [vecs[k].astype(F32) for k in range(8)] + [ub, jnp.zeros((7, 128), F32)]
    smg[f] = jnp.concatenate(vector_rows, axis=0).astype(BF)
    xg[s] = padded(tok).astype(BF)
    cg[s] = padded(cot).astype(BF)
    column = lax.broadcasted_iota(jnp.int32, (1, R), 1)
    slot = sum((column >= TP * k).astype(jnp.int32) for k in range(1, 4))
    inside = column - slot * TP
    valid = (inside < T) & (slot * T + inside < lens[0])
    mask[...] = jnp.where(valid, 0.0, -1e30).astype(F32)
    pl.semaphore_wait(barrier, len(peers))

    for d in range(1, N):
        send(smg.at[f], smg.at[f], sa_s.at[0], sa_r.at[0], {"fsdp": other(d)})
    sq_send(KX, x_slot)
    for m in (0, 1, OUT):
        ag_own(m)
    sq_send(KC, c_slot)
    arrive(smg.at[: N - 1], sa_r.at[0], to_ring[0])
    for j in range(LB):
        piece = smg[j * g].astype(F32)
        for i in range(1, g):
            piece = piece + smg[j * g + i].astype(F32)
        vec[:, j * 128 : (j + 1) * 128] = piece

    def row(k):
        return vec[k : k + 1, :]

    def first_norm(k, into=nrm):
        unit, _ = unit_rows(xg[k].astype(F32))
        into[k] = (unit * row(0) + row(1)).astype(BF)

    def project(hp):
        cols = pl.ds(pl.multiple_of(s * DH + hp * 128, 128), 128)
        bias = jnp.concatenate([vec[2:3, cols], jnp.zeros((1, 128), F32), vec[3:4, cols]], axis=1)
        lanes = lax.broadcasted_iota(jnp.int32, (1, 384), 1)
        scale = jnp.where(lanes < 128, HEAD_DIM ** (-0.5), 1.0).astype(F32)
        here = slice(hp * 384, hp * 384 + 384)

        @pl.loop(0, 4)
        def _(k):
            pq[k, :, here] = ((dot_nn(nrm[k], wqkv[:, here]) + bias) * scale).astype(BF)

    first_norm(s)
    ag_fwd(0, 0)
    sq_core(KX, x_slot)
    first_norm(s_core)
    ag_fwd(1, 0)
    ag_fwd(OUT, 0)
    ag_fwd(0, 1)
    ag_fwd(1, 1)
    ag_fwd(OUT, 1)
    sq_relay(KX, x_slot)
    first_norm(s_y)
    ag_fwd(0, 2)
    ag_fwd(1, 2)
    ag_fwd(OUT, 2)
    ag_own(UP)
    ag_own(DN)
    sq_diag(KX, x_slot)
    first_norm(s_diag)
    ag_last(0)
    project(0)

    flat = pq.reshape(R, HP * 384)
    lane = lax.broadcasted_iota(jnp.int32, (1, 128), 1)
    first = (lane < HEAD_DIM).astype(F32)
    picks = (first.astype(BF), (1.0 - first).astype(BF))

    def lanes_at(off):
        return pl.ds(pl.multiple_of(off, 128), 128)

    def slot_rows(k):
        return pl.ds(pl.multiple_of(k * TP, 16), TP)

    @pl.loop(0, 8)
    def _(t):
        hp, k = lax.div(t, 4), lax.rem(t, 4)
        query = pq[k, :, lanes_at(hp * 384)]
        keys = flat[:, lanes_at(hp * 384 + 128)]
        vals = flat[:, lanes_at(hp * 384 + 256)]
        both, logs = [], []
        for h in range(2):
            scores = dot_nt(query * picks[h], keys) + mask[...]
            top = jnp.max(scores, axis=-1, keepdims=True)
            grown = jnp.exp(scores - top)
            total = jnp.sum(grown, axis=-1, keepdims=True)
            logs.append(top + jnp.log(total))
            both.append(dot_nn((grown * (1.0 / total)).astype(BF), vals))
        rows = slot_rows(k)
        ctx[s, rows, lanes_at(hp * 128)] = jnp.where(lane < HEAD_DIM, both[0], both[1]).astype(BF)
        lse[hp, rows, :] = jnp.where(lane < HEAD_DIM, logs[0], logs[1])

        @pl.when(t == 0)
        def _():
            ag_last(OUT)
            sq_send(KO, out_slot)
            ag_last(1)
            project(1)

        @pl.when(t == 2)
        def _():
            ag_fwd(UP, 0)
            sq_relay(KC, c_slot)

        @pl.when(t == 3)
        def _():
            sq_send(KCTX, ctx_slot(0))

        @pl.when(t == 6)
        def _():
            ag_fwd(UP, 1)
            ag_fwd(DN, 0)

        @pl.when(t == 7)
        def _():
            sq_send(KCTX + 1, ctx_slot(1))

    sq_relay(KO, out_slot)
    sq_relay(KCTX, ctx_slot(0))
    sq_core(KO, out_slot)
    sq_diag(KO, out_slot)
    sq_core(KCTX, ctx_slot(0))
    sq_core(KCTX + 1, ctx_slot(1))
    ag_fwd(UP, 2)
    sq_relay(KCTX + 1, ctx_slot(1))
    sq_diag(KCTX, ctx_slot(0))
    sq_diag(KCTX + 1, ctx_slot(1))

    @pl.loop(0, 4)
    def _(i):
        k = order(i)
        joined = jnp.concatenate([ctx[j, slot_rows(k), :] for j in range(4)], axis=1)
        value = xg[k].astype(F32) + dot_nn(joined, wout[...]) + row(4)
        unit, _ = unit_rows(value)
        n2[k] = (unit * row(5) + row(6)).astype(BF)

        @pl.when(i == 3)
        def _():
            mid[...] = value

        @pl.when(i == 1)
        def _():
            ag_fwd(DN, 1)

    sq_core(KC, c_slot)
    sq_diag(KC, c_slot)
    ag_last(UP)

    @pl.loop(0, 4)
    def _(k):
        before = dot_nn(n2[k], wup[...]) + row(8)
        cdf = 0.5 + 0.5 * lax.erf(before * (0.5**0.5))
        slope = cdf + before * (jnp.exp(before * before * -0.5) * (1.0 / math.sqrt(2.0 * math.pi)))
        hid[k] = (before * cdf).astype(BF)
        gbf[k] = slope.astype(BF)

    ag_fwd(DN, 2)

    def weight_grad(left, right, dw, size):
        per = max(512 // size, 1)

        @pl.loop(0, dw.shape[0] // per)
        def _(i):
            lo = pl.ds(pl.multiple_of(i * per * size, per * size), per * size)
            value = dot_tn(left[:, lo], right).astype(BF)
            for j in range(per):
                dw[i * per + j] = value[j * size : (j + 1) * size]

    weight_grad(hid.reshape(R, D), cg.reshape(R, D)[...], dw_dn, wf)
    rg_own(0)
    ag_last(DN)

    def before_grad(theirs, ours, rows):
        count = rows.stop - rows.start
        slope = both_rows(gbf, theirs, ours, rows).astype(F32)
        grad = (dot_nt(both_rows(cg, theirs, ours, rows), wdn[...]) * slope).astype(BF)
        gbf[theirs, rows] = grad[:count]
        gbf[ours, rows] = grad[count:]
        gvec[8:9, :] += jnp.sum(grad.astype(F32), axis=0, keepdims=True)
        return dot_nt(grad, wup[...])

    seq_pass(0, gpart, gown, grecv, before_grad, poll=lambda: rg_fwd(0, 0))
    weight_grad(n2.reshape(R, D), gbf.reshape(R, D)[...], dw_up, w)
    rg_own(1)

    def branch_rows(h):
        rows = halves[h]
        from_core(0, grecv, h)
        from_y(0, grecv, h)
        gn = gown[rows] + grecv[2, rows].astype(F32) + grecv[1, rows].astype(F32)
        unit, rate = unit_rows(mid[rows])
        c_own = cg[s, rows].astype(F32)
        gm = c_own + norm_pull(gn, row(5), unit, rate)
        gmid[rows] = gm
        branch = gm.astype(BF)
        nrm[s, rows] = branch
        sq_send(KG + h, g_slot(h))
        for k, value in ((5, gn * unit), (6, gn), (7, c_own), (4, branch.astype(F32))):
            gvec[k : k + 1, :] += jnp.sum(value, axis=0, keepdims=True)

    @pl.loop(0, 4)
    def _(k):
        first_norm(k, n2)

    branch_rows(0)
    rg_fwd(0, 1)

    seq_pass(1, opart, oown, orecv, lambda theirs, ours, rows: dot_nn(both_rows(hid, theirs, ours, rows), wdn[...]), defer=True, poll=lambda: rg_fwd(1, 0))
    branch_rows(1)
    seq_sent(0, gpart)
    for h in range(2):
        seq_across(1, opart, orecv, h)

    flat_g = gctx.reshape(R, DH)
    dkt[...] = jnp.zeros_like(dkt)
    dvt[...] = jnp.zeros_like(dvt)

    def branch_back(k):
        gctx[k] = dot_nt(nrm[k], wout[pl.ds(pl.multiple_of(s * DH, DH), DH), :]).astype(BF)

    def close_pair(hp):
        lo = hp * 384
        flat[:, lo + 128 : lo + 256] = dkt[hp].T.astype(BF)
        flat[:, lo + 256 : lo + 384] = dvt[hp].T.astype(BF)
        weight_grad(n2.reshape(R, D), flat[:, lo : lo + 384], dw_qkv.at[hp], w)
        rg_own(3 + hp)
        off = lanes_at(s * DH + hp * 128)
        gvec[2:3, off] = jnp.sum(flat[:, lo : lo + 128].astype(F32), axis=0, keepdims=True)
        gvec[3:4, off] = jnp.sum(flat[:, lo + 256 : lo + 384].astype(F32), axis=0, keepdims=True)

    branch_back(s)
    for h in range(2):
        sq_core(KG + h, g_slot(h))
    branch_back(s_core)

    @pl.loop(0, 8)
    def _(t):
        late, u = lax.div(t, 4), lax.rem(t, 4)
        hp = (1 - late) * lax.rem(u, 2) + late * lax.div(u, 2)
        flip = (1 - late) * lax.div(u, 2) + late * lax.rem(u, 2)
        k = lax.rem(y + late, 2) * 2 + lax.rem(c + flip, 2)
        query = pq[k, :, lanes_at(hp * 384)]
        keys = flat[:, lanes_at(hp * 384 + 128)]
        vals = flat[:, lanes_at(hp * 384 + 256)]
        grad = gctx[k, :, lanes_at(hp * 128)]
        logs = lse[hp, slot_rows(k), :]
        both = []
        for h in range(2):
            qh, gh = query * picks[h], grad * picks[h]
            probs = jnp.exp(dot_nt(qh, keys) + mask[...] - logs[:, h * HEAD_DIM : h * HEAD_DIM + 1])
            dp = dot_nt(gh, vals)
            inner = jnp.sum(probs * dp, axis=-1, keepdims=True)
            ds = (probs * (dp - inner)).astype(BF)
            both.append(dot_nn(ds, keys))
            dkt[hp] += dot_tn(qh, ds)
            dvt[hp] += dot_tn(gh, probs.astype(BF))
        dq = jnp.where(lane < HEAD_DIM, both[0], both[1]) * HEAD_DIM ** (-0.5)
        pq[k, :, lanes_at(hp * 384)] = dq.astype(BF)

        @pl.when(t == 0)
        def _():
            rg_fwd(0, 2)

        @pl.when(t == 1)
        def _():
            sq_relay(KG, g_slot(0))

        @pl.when(t == 2)
        def _():
            rg_fwd(1, 1)

        @pl.when(t == 3)
        def _():
            sq_relay(KG + 1, g_slot(1))
            branch_back(s_y)
            for h in range(2):
                sq_diag(KG + h, g_slot(h))
            branch_back(s_diag)
            right = nrm.reshape(R, D)[:, quarter]
            for j in range(4):
                value = dot_tn(ctx[j], right).astype(BF)
                for i in range(DH // w):
                    dw_out[j * (DH // w) + i] = value[i * w : (i + 1) * w]
            rg_own(2)
            rg_fin(0)

        @pl.when(t == 5)
        def _():
            rg_fwd(2, 0)
            rg_fwd(1, 2)
            close_pair(0)

        @pl.when(t == 6)
        def _():
            rg_fwd(2, 1)

    close_pair(1)
    rg_fin(1)
    rg_fwd(3, 0)
    rg_fwd(2, 2)

    seq_pass(2, gpart, gown, grecv, lambda theirs, ours, rows: dot_nt(both_rows(pq, theirs, ours, rows), wqkv[...]), poll=lambda: rg_fwd(4, 0))
    rg_fwd(3, 1)
    for h in range(2):
        from_core(1, orecv, h)
        from_y(1, orecv, h)
    tok[...] = (mid[...] + (oown[...] + orecv[2].astype(F32) + orecv[1].astype(F32)) + row(7))[:T].astype(BF)
    put(tok, h_out, 6)
    rg_fin(2)
    for h in range(2):
        from_core(2, grecv, h)
    here = gown[...] + grecv[2].astype(F32)
    away = gpart[1].astype(F32)
    unit, rate = unit_rows(xg[s].astype(F32))
    unit_y, _ = unit_rows(xg[s_y].astype(F32))
    gvec[0:1, :] = jnp.sum(here * unit + away * unit_y, axis=0, keepdims=True)
    gvec[1:2, :] = jnp.sum(here + away, axis=0, keepdims=True)
    for k in range(N):
        j = k // g
        dw_sm[k] = gvec[:, j * 128 : (j + 1) * 128]
    for d in range(1, N):
        send(dw_sm.at[other(d)], rr_sm.at[d - 1], sg_s.at[0], sg_r.at[0], {"fsdp": other(d)})
    rg_fwd(4, 1)
    rg_fwd(3, 2)
    total = dw_sm[f]
    arrive(rr_sm, sg_r.at[0], to_ring[0])
    for d in range(1, N):
        total = total + rr_sm[d - 1]
    o_sm[s] = total
    for dev in (to_core, to_y, {"seq": s_diag}):
        send(o_sm.at[s], o_sm.at[s], sm_s.at[0], sm_r.at[0], dev)
    rg_fwd(4, 2)

    hbm = [h_dn, h_up, h_ow] + [h_qkv.at[hp] for hp in range(HP)]
    finals = [(KFIN + m, fin_slot(m)) for m in range(MG)]

    def put_slot(m, k):
        put(grads[m][2].at[k], hbm[m].at[k], m)

    def relay_out(m):
        sq_relay(*finals[m])
        put_slot(m, s_y)

    for m in range(3):
        put_slot(m, s)
    relay_out(0)
    rg_fin(3)
    put_slot(3, s)
    relay_out(1)
    for h in range(2):
        from_y(2, grecv, h)
    gn = here + grecv[1].astype(F32)
    cot[...] = (gmid[...] + norm_pull(gn, row(0), unit, rate))[:T].astype(BF)
    put(cot, h_tok, 7)
    rg_fin(4)
    put_slot(4, s)
    for m in range(MG):
        sq_core(*finals[m])
        put_slot(m, s_core)
    for m in range(2, MG):
        relay_out(m)
    arrive(o_sm.at[:3], sm_r.at[0], to_core)
    put(o_sm, h_sm, 5)
    for m in range(MG):
        sq_diag(*finals[m])
        put_slot(m, s_diag)

    for m in range(3 + HP):
        ag_sent(m)
    for m in range(MG):
        rg_sent(m)
    for kind, ref in ((KX, xg), (KC, cg)):
        sq_sent(kind, ref.at[:3])
    for h in range(2):
        sq_sent(KG + h, nrm.at[:3, halves[h]])
    sq_sent(KO, wout.at[:, : 3 * DH])
    for hp in range(HP):
        sq_sent(KCTX + hp, ctx.at[:3, :, hp * 128 : hp * 128 + 128])
    for m in range(MG):
        sq_sent(KFIN + m, grads[m][2].at[:3])
    seq_sent(1, opart)
    seq_sent(2, gpart)
    sent(smg.at[: N - 1], sa_s.at[0], to_ring[0])
    sent(dw_sm.at[: N - 1], sg_s.at[0], to_ring[0])
    sent(o_sm.at[:3], sm_s.at[0], to_core)
    for src, dst, k in [(grads[m][2], hbm[m], m) for m in range(MG)] + [(o_sm, h_sm, 5), (tok, h_out, 6), (cot, h_tok, 7)]:
        pltpu.make_async_copy(src, dst, put_sem.at[k]).wait()


def finish_kernel(z, *refs):
    srcs, dsts = refs[:7], refs[7:22]
    (out, tok, gq, go, gu, gd, gs), bufs = refs[22:29], refs[29:42]
    s_in, s_out = refs[42:]
    D, w, wf, HP, N = z["D"], z["w"], z["wf"], z["HP"], 2 * z["A"]
    DH = D // 4
    loads = [pltpu.make_async_copy(src, dst, s_in.at[k]) for k, (src, dst) in enumerate(zip(srcs, (out, tok, gq, go, gu, gd, gs)))]
    saves = []

    def save(src, k):
        copy = pltpu.make_async_copy(src, dsts[k], s_out.at[k])
        copy.start()
        saves.append(copy)

    for k in (5, 4, 2, 3, 6, 0, 1):
        loads[k].start()
    f_qkv, f_ow, f_up, f_dn = bufs[:4]
    loads[5].wait()
    for s in range(4):
        f_dn[s * wf : (s + 1) * wf] = gd[s].astype(F32)
    save(f_dn, 5)
    loads[4].wait()
    if z["up_whole"]:
        for s in range(4):
            for k in range(N):
                f_up[:, (k * 4 + s) * wf : (k * 4 + s + 1) * wf] = gu[s, :, k * wf : (k + 1) * wf].astype(F32)
    else:
        f_up[...] = gu[...].astype(F32)
    save(f_up, 4)
    loads[2].wait()
    for s in range(4):
        for hp in range(HP):
            for part in range(3):
                lo = part * D + s * DH + hp * 128
                f_qkv[:, lo : lo + 128] = gq[hp, s, :, part * 128 : part * 128 + 128].astype(F32)
    save(f_qkv, 2)
    loads[3].wait()
    for s in range(4):
        f_ow[:, s * DH : (s + 1) * DH] = go[s].astype(F32)
    save(f_ow, 3)
    loads[6].wait()
    total = gs[0] + gs[1] + gs[2] + gs[3]
    for k in range(8):
        bufs[4 + k][...] = total[k : k + 1]
        save(bufs[4 + k], 6 + k)
    bufs[12][...] = jnp.concatenate([gs[s, 8:9] for s in range(4)], axis=1)
    save(bufs[12], 14)
    for k, buf in ((0, out), (1, tok)):
        loads[k].wait()
        save(buf, k)
    for copy in saves:
        copy.wait()


def make_body(mesh):
    N = mesh.shape["fsdp"]
    A = N // 2

    def body(
        tokens, lengths, ln1_gain, ln1_bias, qkv_weight, q_bias, v_bias, out_weight, out_bias,
        ln2_gain, ln2_bias, up_weight, up_bias, down_weight, down_bias, cotangent,
    ):
        _, T, D = tokens.shape
        w, FF = D // N, up_weight.shape[1]
        wf = FF // (4 * N)
        TP = -(-T // 16) * 16
        R = 4 * TP
        DH = D // 4
        HP = DH // 128
        FQ = FF // 4
        assert FQ == D and wf == w and HP == 2
        g = max(128 // w, 1)
        s = lax.axis_index("seq")
        f = lax.axis_index("fsdp")
        up_whole = wf % 128 == 0
        plain = (ln1_gain, ln1_bias, q_bias, v_bias, out_bias, ln2_gain, ln2_bias, down_bias)
        if g == 1:
            vectors_in = [v.reshape(1, w) for v in plain]
            ub_in = up_bias.reshape(4, wf)
        else:
            spot = lax.rem(f, g) * w
            blank = jnp.zeros((1, 128), BF)
            vectors_in = [lax.dynamic_update_slice(blank, v[None], (0, spot)) for v in plain]
            mine = lax.dynamic_slice(up_bias, (s * wf,), (wf,))
            ub_in = lax.dynamic_update_slice(jnp.zeros((4, 128), BF), mine[None], (s, spot))
        if not up_whole:
            up_weight = lax.dynamic_index_in_dim(up_weight.reshape(w, N, 4, wf), s, 2, False).reshape(w, FQ)
        z = dict(D=D, T=T, TP=TP, R=R, A=A, w=w, wf=wf, HP=HP, g=g, up_whole=up_whole)
        vm = pltpu.VMEM
        C = 384
        scratch = [
            vm((T, D), BF), vm((T, D), BF), pltpu.SMEM((1,), jnp.int32), vm((8, 1, 128), BF), vm((4, 128), BF),
            vm((HP, 4, w, C), BF), vm((4, w, DH), BF), vm((4, w, FQ), BF), vm((4, wf, D), BF), vm((4, 16, 128), F32),
            vm((4, TP, D), BF),
            vm((4, TP, D), BF),
            vm((4, TP, D), BF),
            vm((4, R, DH), BF),
            vm((4, TP, D), BF),
            vm((4, TP, D), BF),
            vm((4, TP, D), BF),
            vm((4, TP, HP * C), BF),
            vm((D, HP * C), BF),
            vm((D, D), BF),
            vm((D, FQ), BF),
            vm((FQ, D), BF),
            vm((N, 16, 128), BF),
            vm((16, D), F32),
            vm((16, D), F32),
            vm((HP, R, 128), F32),
            vm((TP, D), F32),
            vm((TP, D), F32),
            vm((4, TP, DH), BF),
            vm((HP, 128, R), F32),
            vm((HP, 128, R), F32),
            vm((3, TP, D), BF), vm((TP, D), F32), vm((3, TP, D), BF),
            vm((3, TP, D), BF), vm((TP, D), F32), vm((3, TP, D), BF),
            vm((1, R), F32),
            vm((HP, N, w, C), BF), vm((N, w, DH), BF), vm((N, w, FQ), BF), vm((N, wf, D), BF), vm((N, 16, 128), F32),
            vm((HP, 2, A, w, C), BF), vm((2, A, w, DH), BF), vm((2, A, w, FQ), BF), vm((2, A, wf, D), BF), vm((N - 1, 16, 128), F32),
        ]
        dma = pltpu.SemaphoreType.DMA
        scratch += [
            dma((9,)), dma((8,)),
            dma((3 + HP,)), dma((3 + HP, A)), dma((3 + HP,)), dma((3 + HP, A)),
            dma((8 + 2 * HP,)), dma((8 + 2 * HP, 3)),
            dma((3,)), dma((3, 3, 2)),
            dma((1,)), dma((1,)), dma((1,)), dma((1,)), dma((1,)), dma((1,)),
        ]
        there = pl.BlockSpec(memory_space=pl.ANY)
        out_shapes = [
            jax.ShapeDtypeStruct((T, D), BF),
            jax.ShapeDtypeStruct((T, D), BF),
            jax.ShapeDtypeStruct((HP, 4, w, C), BF),
            jax.ShapeDtypeStruct((4, w, DH), BF),
            jax.ShapeDtypeStruct((4, w, FQ), BF),
            jax.ShapeDtypeStruct((4, wf, D), BF),
            jax.ShapeDtypeStruct((4, 16, 128), F32),
        ]
        out, gtok, gq, go, gu, gd, gs = pl.pallas_call(
            functools.partial(layer_entry, z),
            out_shape=out_shapes,
            in_specs=[there] * 16,
            out_specs=[there] * 7,
            scratch_shapes=scratch,
            compiler_params=pltpu.CompilerParams(
                collective_id=0, has_side_effects=True, vmem_limit_bytes=67_000_000
            ),
            name="layer",
        )(tokens[0], cotangent[0], lengths, *vectors_in, ub_in, qkv_weight, out_weight, up_weight, down_weight)

        if not up_whole:
            gu = gu.reshape(4, w, N, wf).transpose(1, 2, 0, 3).reshape(w, FF)
        if g > 1:
            gs = lax.dynamic_slice(gs, (0, 0, lax.rem(f, g) * w), (4, 16, w))
        shapes = [((w, 3 * D), F32), ((w, D), F32), ((w, FF), F32), ((4 * wf, D), F32)]
        shapes += [((1, w), F32)] * 8 + [((1, 4 * wf), F32)]
        sources = (out, gtok, gq, go, gu, gd, gs)
        done = pl.pallas_call(
            functools.partial(finish_kernel, z),
            out_shape=[jax.ShapeDtypeStruct(*v) for v in [((T, D), BF)] * 2 + shapes],
            in_specs=[there] * 7,
            out_specs=[there] * 15,
            scratch_shapes=[vm(v.shape, v.dtype) for v in sources] + [vm(*v) for v in shapes] + [dma((7,)), dma((15,))],
            name="finish",
        )(*sources)
        out, gtok, g_qkv, g_out, g_up, g_down = done[:6]
        sums = [v.reshape(-1) for v in done[6:]]
        return (
            out[None], gtok[None], sums[0], sums[1], g_qkv, sums[2], sums[3], g_out, sums[4],
            sums[5], sums[6], g_up, sums[8], g_down, sums[7],
        )

    return body


def solution(mesh):
    row, mat, act = P("fsdp"), P("fsdp", None), P("fsdp", "seq", None)
    return jax.shard_map(
        make_body(mesh),
        mesh=mesh,
        in_specs=(act, row, row, row, mat, row, row, mat, row, row, row, mat, row, mat, row, act),
        out_specs=(act, act, row, row, mat, row, row, mat, row, row, row, mat, row, mat, row),
        check_vma=False,
    )
```

```python
import functools
import math

import jax
import jax.numpy as jnp
from jax import lax
from jax.experimental import pallas as pl
from jax.experimental.pallas import tpu as pltpu
from jax.sharding import PartitionSpec as P

HEAD_DIM = 64
BF = jnp.bfloat16
F32 = jnp.float32
MESH = pl.DeviceIdType.MESH


def dot_nn(left, right):
    return lax.dot_general(left, right, (((1,), (0,)), ((), ())), preferred_element_type=F32)


def dot_nt(left, right):
    return lax.dot_general(left, right, (((1,), (1,)), ((), ())), preferred_element_type=F32)


def dot_tn(left, right):
    return lax.dot_general(left, right, (((0,), (0,)), ((), ())), preferred_element_type=F32)


def unit_rows(values):
    center = values - jnp.mean(values, axis=-1, keepdims=True)
    rate = lax.rsqrt(jnp.mean(center * center, axis=-1, keepdims=True) + 1e-6)
    return center * rate, rate


def norm_pull(grad, gain, unit, rate):
    scaled = grad * gain
    return rate * (
        scaled
        - jnp.mean(scaled, axis=-1, keepdims=True)
        - unit * jnp.mean(scaled * unit, axis=-1, keepdims=True)
    )


def layer_entry(z, *refs):
    layer_kernel(z, *refs[:3], refs[3:11], *refs[11:])


def layer_kernel(
    z,
    tok_in, cot_in, len_in, vecs_in, ub_in, qkv_in, out_in, up_in, dn_in,
    h_out, h_tok, h_qkv, h_ow, h_up, h_dn, h_sm,
    tok, cot, lens, vecs, ub4, o_qkv, o_ow, o_up, o_dn, o_sm,
    xg, cg, nrm, ctx, n2, hid, gbf, pq, wqkv, wout, wup, wdn, smg, vec, gvec, lse, mid, gmid,
    gctx, dkt, dvt, gpart, gown, grecv, opart, oown, orecv, mask,
    dw_qkv, dw_out, dw_up, dw_dn, dw_sm, rr_qkv, rr_out, rr_up, rr_dn, rr_sm,
    loc_sem, put_sem, ag_s, ag_r, rg_s, rg_r, sq_s, sq_r, rs_s, rs_r, sa_s, sa_r, sg_s, sg_r, sm_s, sm_r,
):
    D, T, TP, R, A, w, wf, HP = z["D"], z["T"], z["TP"], z["R"], z["A"], z["w"], z["wf"], z["HP"]
    N, H, DH, LB, g = 2 * A, A, D // 4, D // 128, z["g"]
    s = lax.axis_index("seq")
    f = lax.axis_index("fsdp")
    y, c = lax.div(s, 2), lax.rem(s, 2)
    s_core, s_y, s_diag = y * 2 + 1 - c, (1 - y) * 2 + c, (1 - y) * 2 + 1 - c
    to_core, to_y = {"seq": s_core}, {"seq": s_y}

    odd = lax.rem(f, 2)
    place = (1 - odd) * lax.div(f, 2) + odd * (N - 1 - lax.div(f, 2))

    def at_place(q):
        late = lax.div(q, A)
        return (1 - late) * 2 * q + late * (2 * (N - 1 - q) + 1)

    def ahead(d):
        return at_place(lax.rem(place + d + N, N))

    to_ring = ({"fsdp": ahead(1)}, {"fsdp": ahead(-1)})

    def send(src, dst, ssem, rsem, dev):
        pltpu.make_async_remote_copy(
            src_ref=src, dst_ref=dst, send_sem=ssem, recv_sem=rsem, device_id=dev, device_id_type=MESH
        ).start()

    def arrive(dst, rsem, dev):
        pltpu.make_async_remote_copy(
            src_ref=dst, dst_ref=dst, send_sem=rsem, recv_sem=rsem, device_id=dev, device_id_type=MESH
        ).wait_recv()

    def sent(src, ssem, dev):
        pltpu.make_async_remote_copy(
            src_ref=src, dst_ref=src, send_sem=ssem, recv_sem=ssem, device_id=dev, device_id_type=MESH
        ).wait_send()

    def thirds(first, last):
        count = max(last - first, 0)
        cut = [first + (count * k) // 3 for k in range(4)]
        return [range(cut[k], cut[k + 1]) for k in range(3)]

    quarter = pl.ds(pl.multiple_of(s * DH, DH), DH)

    def rows_of(k, size, half=None):
        if half is None:
            return pl.ds(pl.multiple_of(k * size, size), size)
        return pl.ds(pl.multiple_of(k * size + half * (size // 2), size // 2), size // 2)

    OUT, UP, DNA, DNB = HP, HP + 1, HP + 2, HP + 3
    MA = HP + 4
    low, high = slice(0, D // 2), slice(D // 2, D)
    blocks = {
        OUT: lambda k, half=None: wout.at[rows_of(k, w, half), quarter],
        UP: lambda k, half=None: wup.at[rows_of(k, w, half)],
        DNA: lambda k, half=None: wdn.at[rows_of(k, wf, half), low],
        DNB: lambda k, half=None: wdn.at[rows_of(k, wf, half), high],
    }
    for hp in range(HP):
        blocks[hp] = lambda k, half=None, hp=hp: wqkv.at[rows_of(k, w, half), hp * 384 : hp * 384 + 384]

    def ag_block(m, way, d, back):
        k = ahead(-back if way == 0 else back)
        return blocks[m](k, way if d == H else None)

    def ag_own(m):
        for way in range(2):
            ref = ag_block(m, way, 1, 0)
            send(ref, ref, ag_s.at[m], ag_r.at[m, 0], to_ring[way])

    def ag_take(m, d):
        arrive(ag_rows(m, 1 if d == H else 2), ag_r.at[m, d - 1], to_ring[0])
        for way in range(2):
            if d < H:
                ref = ag_block(m, way, d + 1, d)
                send(ref, ref, ag_s.at[m], ag_r.at[m, d], to_ring[way])

    def ag_fwd(m, third):
        for d in thirds(1, H)[third]:
            ag_take(m, d)

    def ag_last(m):
        ag_take(m, H)

    def ag_rows(m, shards):
        size = shards * (wf if m in (DNA, DNB) else w)
        every = {OUT: wout.at[:size, quarter], UP: wup.at[:size], DNA: wdn.at[:size, low], DNB: wdn.at[:size, high]}
        return every[m] if m in every else wqkv.at[:size, m * 384 : m * 384 + 384]

    def ag_sent(m):
        sent(ag_rows(m, N - 1), ag_s.at[m], to_ring[0])

    def sq_send(kind, ref):
        send(ref(s), ref(s), sq_s.at[kind], sq_r.at[kind, 0], to_core)
        send(ref(s), ref(s), sq_s.at[kind], sq_r.at[kind, 1], to_y)

    def sq_core(kind, ref):
        arrive(ref(s_core), sq_r.at[kind, 0], to_core)

    def sq_relay(kind, ref):
        arrive(ref(s_y), sq_r.at[kind, 1], to_y)
        send(ref(s_y), ref(s_y), sq_s.at[kind], sq_r.at[kind, 2], to_core)

    def sq_diag(kind, ref):
        arrive(ref(s_diag), sq_r.at[kind, 2], to_core)

    def sq_sent(kind, three):
        sent(three, sq_s.at[kind], to_core)

    def x_slot(k):
        return xg.at[k]

    def c_slot(k):
        return cg.at[k]

    def g_slot(h):
        return lambda k: nrm.at[k, halves[h]]

    def out_slot(k):
        return wout.at[:, pl.ds(pl.multiple_of(k * DH, DH), DH)]

    def ctx_slot(hp):
        return lambda k: ctx.at[k, :, hp * 128 : hp * 128 + 128]

    KX, KC, KG, KO, KCTX, KFIN = 0, 1, 2, 4, 5, 5 + HP

    def order(i):
        hb, lb = lax.div(3 - i, 2), lax.rem(3 - i, 2)
        return lax.rem(y + hb, 2) * 2 + lax.rem(c + lb, 2)

    cut = -(-TP // 32) * 16
    halves = (slice(0, cut), slice(cut, TP))

    def seq_across(kind, part, recv, h):
        send(part.at[1, halves[h]], recv.at[1, halves[h]], rs_s.at[kind], rs_r.at[kind, 1, h], to_y)

    def seq_pass(kind, part, own, recv, compute, defer=False, poll=None):
        def chip_sum(h):
            rows = halves[h]
            arrive(recv.at[0, rows], rs_r.at[kind, 0, h], to_core)
            part[1, rows] = (part[1, rows].astype(F32) + recv[0, rows].astype(F32)).astype(BF)
            if not defer:
                seq_across(kind, part, recv, h)

        @pl.loop(0, 2)
        def _(p):
            chip = lax.rem(y + 1 - p, 2) * 2
            theirs, ours = chip + 1 - c, chip + c
            for h, rows in enumerate(halves):
                count = rows.stop - rows.start
                value = compute(theirs, ours, rows)

                @pl.when(p == 0)
                def _():
                    part[0, rows] = value[:count].astype(BF)
                    part[1, rows] = value[count:].astype(BF)
                    send(part.at[0, rows], recv.at[0, rows], rs_s.at[kind], rs_r.at[kind, 0, h], to_core)
                    if h == 1:
                        chip_sum(0)

                @pl.when(p == 1)
                def _():
                    part[2, rows] = value[:count].astype(BF)
                    own[rows] = value[count:]
                    send(part.at[2, rows], recv.at[2, rows], rs_s.at[kind], rs_r.at[kind, 2, h], to_core)
                    if h == 0:
                        chip_sum(1)
                        if poll:
                            poll()

    def both_rows(ref, theirs, ours, rows):
        return jnp.concatenate([ref[theirs, rows], ref[ours, rows]], axis=0)

    def seq_sent(kind, part):
        sent(part, rs_s.at[kind], to_core)

    def from_core(kind, recv, h):
        arrive(recv.at[2, halves[h]], rs_r.at[kind, 2, h], to_core)

    def from_y(kind, recv, h):
        arrive(recv.at[1, halves[h]], rs_r.at[kind, 1, h], to_y)

    grads = {0: (dw_dn, rr_dn, o_dn), 2: (dw_out, rr_out, o_ow)}
    FQ = dw_up.shape[2]
    sides = (slice(0, FQ // 2), slice(FQ // 2, FQ))
    for m, side in zip((1, 6), sides):
        grads[m] = (dw_up.at[:, :, side], rr_up.at[:, :, :, side], o_up.at[:, :, side])
    grads[3] = (dw_qkv.at[0], rr_qkv.at[0], o_qkv.at[0])
    split = (slice(0, w // 2), slice(w // 2, w))
    for h in range(2):
        grads[4 + h] = (dw_qkv.at[1, :, split[h]], rr_qkv.at[1, :, :, split[h]], o_qkv.at[1, :, split[h]])
    MG = 7

    def rg_rows(m, way, j):
        size = grads[m][0].shape[1]
        return slice(way * (size // 2), (way + 1) * (size // 2)) if j == 0 else slice(0, size)

    def rg_owner(way, j):
        return ahead(H - j if way == 0 else j - H)

    def rg_src(m, way, j):
        return grads[m][0].at[rg_owner(way, j), rg_rows(m, way, j)]

    def rg_send(m, way, j):
        dst = grads[m][1].at[way, j, rg_rows(m, way, j)]
        send(rg_src(m, way, j), dst, rg_s.at[m], rg_r.at[m, j], to_ring[way])

    def rg_arrive(m, j):
        arrive(grads[m][0].at[: 1 if j == 0 else 2], rg_r.at[m, j], to_ring[0])

    def rg_own(m):
        for way in range(2):
            rg_send(m, way, 0)

    def rg_fwd(m, third):
        dw, rr, _ = grads[m]
        for j in thirds(1, H)[third]:
            rg_arrive(m, j - 1)
            for way in range(2):
                rows = rg_rows(m, way, j - 1)
                owner = rg_owner(way, j)
                dw[owner, rows] = (dw[owner, rows].astype(F32) + rr[way, j - 1, rows].astype(F32)).astype(dw.dtype)
                rg_send(m, way, j)

    def fin_slot(m):
        return lambda k: grads[m][2].at[k]

    def rg_fin(m):
        dw, rr, out = grads[m]
        total = dw[f].astype(F32)
        rg_arrive(m, H - 1)
        for way in range(2):
            total = total + rr[way, H - 1].astype(F32)
        out[s] = total.astype(out.dtype)
        sq_send(KFIN + m, fin_slot(m))

    def rg_sent(m):
        sent(grads[m][0].at[: N - 1], rg_s.at[m], to_ring[0])

    def other(d):
        return lax.rem(f + d, N)

    barrier = pltpu.get_barrier_semaphore()
    peers = [to_core, to_y, {"seq": s_diag}] + [{"fsdp": other(d)} for d in range(1, N)]
    for dev in peers:
        pl.semaphore_signal(barrier, inc=1, device_id=dev, device_id_type=MESH)

    def bring(k, src, dst):
        pltpu.make_async_copy(src, dst, loc_sem.at[k]).start()

    bring(0, tok_in, tok)
    for k in range(8):
        bring(1, vecs_in[k], vecs.at[k])
    bring(2, ub_in, ub4)
    for hp in range(HP):
        for part in range(3):
            cols = pl.ds(pl.multiple_of(part * D + s * DH + hp * 128, 128), 128)
            lo = hp * 384 + part * 128
            bring(3, qkv_in.at[:, cols], wqkv.at[rows_of(f, w), lo : lo + 128])
    bring(4, out_in.at[:, quarter], wout.at[rows_of(f, w), quarter])
    bring(5, cot_in, cot)
    bring(6, len_in, lens)
    if z["up_whole"]:
        for k in range(N):
            cols = pl.ds(pl.multiple_of((k * 4 + s) * wf, wf), wf)
            bring(7, up_in.at[:, cols], wup.at[rows_of(f, w), k * wf : (k + 1) * wf])
    else:
        bring(7, up_in, wup.at[rows_of(f, w)])
    bring(8, dn_in.at[rows_of(s, wf)], wdn.at[rows_of(f, wf)])

    def put(src, dst, k):
        pltpu.make_async_copy(src, dst, put_sem.at[k]).start()

    def padded(ref):
        return jnp.concatenate([ref[...].astype(F32), jnp.zeros((TP - T, D), F32)], axis=0)

    gvec[...] = jnp.zeros_like(gvec)
    own_rows = [tok, vecs, ub4, wqkv.at[rows_of(f, w)], wout.at[rows_of(f, w), quarter], cot, lens, wup.at[rows_of(f, w)], wdn.at[rows_of(f, wf)]]
    for k, dst in enumerate(own_rows):
        pltpu.make_async_copy(dst, dst, loc_sem.at[k]).wait()
    quarters = ub4[...].astype(F32)
    ub = sum(quarters[k : k + 1] * (s == k).astype(F32) for k in range(4))
    vector_rows = [vecs[k].astype(F32) for k in range(8)] + [ub, jnp.zeros((7, 128), F32)]
    smg[f] = jnp.concatenate(vector_rows, axis=0).astype(BF)
    xg[s] = padded(tok).astype(BF)
    cg[s] = padded(cot).astype(BF)
    column = lax.broadcasted_iota(jnp.int32, (1, R), 1)
    slot = sum((column >= TP * k).astype(jnp.int32) for k in range(1, 4))
    inside = column - slot * TP
    valid = (inside < T) & (slot * T + inside < lens[0])
    mask[...] = jnp.where(valid, 0.0, -1e30).astype(F32)
    pl.semaphore_wait(barrier, len(peers))

    for d in range(1, N):
        send(smg.at[f], smg.at[f], sa_s.at[0], sa_r.at[0], {"fsdp": other(d)})
    sq_send(KX, x_slot)
    for m in (0, 1, OUT):
        ag_own(m)
    sq_send(KC, c_slot)
    arrive(smg.at[: N - 1], sa_r.at[0], to_ring[0])
    for j in range(LB):
        piece = smg[j * g].astype(F32)
        for i in range(1, g):
            piece = piece + smg[j * g + i].astype(F32)
        vec[:, j * 128 : (j + 1) * 128] = piece

    def row(k):
        return vec[k : k + 1, :]

    def first_norm(k, into=nrm):
        unit, _ = unit_rows(xg[k].astype(F32))
        into[k] = (unit * row(0) + row(1)).astype(BF)

    def project(hp):
        cols = pl.ds(pl.multiple_of(s * DH + hp * 128, 128), 128)
        bias = jnp.concatenate([vec[2:3, cols], jnp.zeros((1, 128), F32), vec[3:4, cols]], axis=1)
        lanes = lax.broadcasted_iota(jnp.int32, (1, 384), 1)
        scale = jnp.where(lanes < 128, HEAD_DIM ** (-0.5), 1.0).astype(F32)
        here = slice(hp * 384, hp * 384 + 384)

        @pl.loop(0, 4)
        def _(k):
            pq[k, :, here] = ((dot_nn(nrm[k], wqkv[:, here]) + bias) * scale).astype(BF)

    first_norm(s)
    ag_fwd(0, 0)
    sq_core(KX, x_slot)
    first_norm(s_core)
    ag_fwd(1, 0)
    ag_fwd(OUT, 0)
    ag_fwd(0, 1)
    ag_fwd(1, 1)
    ag_fwd(OUT, 1)
    sq_relay(KX, x_slot)
    first_norm(s_y)
    ag_fwd(0, 2)
    ag_fwd(1, 2)
    ag_fwd(OUT, 2)
    ag_own(UP)
    ag_own(DNA)
    ag_own(DNB)
    sq_diag(KX, x_slot)
    first_norm(s_diag)
    ag_last(0)
    project(0)

    flat = pq.reshape(R, HP * 384)
    lane = lax.broadcasted_iota(jnp.int32, (1, 128), 1)
    first = (lane < HEAD_DIM).astype(F32)
    picks = (first.astype(BF), (1.0 - first).astype(BF))

    def lanes_at(off):
        return pl.ds(pl.multiple_of(off, 128), 128)

    def slot_rows(k):
        return pl.ds(pl.multiple_of(k * TP, 16), TP)

    @pl.loop(0, 8)
    def _(t):
        hp, k = lax.div(t, 4), lax.rem(t, 4)
        query = pq[k, :, lanes_at(hp * 384)]
        keys = flat[:, lanes_at(hp * 384 + 128)]
        vals = flat[:, lanes_at(hp * 384 + 256)]
        both, logs = [], []
        for h in range(2):
            scores = dot_nt(query * picks[h], keys) + mask[...]
            top = jnp.max(scores, axis=-1, keepdims=True)
            grown = jnp.exp(scores - top)
            total = jnp.sum(grown, axis=-1, keepdims=True)
            logs.append(top + jnp.log(total))
            both.append(dot_nn((grown * (1.0 / total)).astype(BF), vals))
        rows = slot_rows(k)
        ctx[s, rows, lanes_at(hp * 128)] = jnp.where(lane < HEAD_DIM, both[0], both[1]).astype(BF)
        lse[hp, rows, :] = jnp.where(lane < HEAD_DIM, logs[0], logs[1])

        @pl.when(t == 0)
        def _():
            ag_last(OUT)
            sq_send(KO, out_slot)
            ag_last(1)
            project(1)

        @pl.when(t == 2)
        def _():
            ag_fwd(UP, 0)
            sq_relay(KC, c_slot)

        @pl.when(t == 3)
        def _():
            sq_send(KCTX, ctx_slot(0))

        @pl.when(t == 5)
        def _():
            ag_fwd(DNA, 0)

        @pl.when(t == 7)
        def _():
            sq_send(KCTX + 1, ctx_slot(1))

    sq_relay(KO, out_slot)
    ag_fwd(UP, 1)
    ag_fwd(DNB, 0)
    sq_relay(KCTX, ctx_slot(0))
    sq_core(KO, out_slot)
    sq_diag(KO, out_slot)
    sq_core(KCTX, ctx_slot(0))
    sq_core(KCTX + 1, ctx_slot(1))
    sq_relay(KCTX + 1, ctx_slot(1))
    ag_fwd(UP, 2)
    ag_fwd(DNA, 1)
    sq_diag(KCTX, ctx_slot(0))
    sq_diag(KCTX + 1, ctx_slot(1))

    @pl.loop(0, 4)
    def _(i):
        k = order(i)
        joined = jnp.concatenate([ctx[j, slot_rows(k), :] for j in range(4)], axis=1)
        value = xg[k].astype(F32) + dot_nn(joined, wout[...]) + row(4)
        unit, _ = unit_rows(value)
        n2[k] = (unit * row(5) + row(6)).astype(BF)

        @pl.when(i == 3)
        def _():
            mid[...] = value

        @pl.when(i == 1)
        def _():
            ag_fwd(DNB, 1)

    sq_core(KC, c_slot)
    sq_diag(KC, c_slot)
    ag_last(UP)

    @pl.loop(0, 4)
    def _(k):
        before = dot_nn(n2[k], wup[...]) + row(8)
        cdf = 0.5 + 0.5 * lax.erf(before * (0.5**0.5))
        slope = cdf + before * (jnp.exp(before * before * -0.5) * (1.0 / math.sqrt(2.0 * math.pi)))
        hid[k] = (before * cdf).astype(BF)
        gbf[k] = slope.astype(BF)

        @pl.when(k == 1)
        def _():
            ag_fwd(DNA, 2)

    ag_fwd(DNB, 2)

    def weight_grad(left, right, dw, size):
        per = max(512 // size, 1)

        @pl.loop(0, dw.shape[0] // per)
        def _(i):
            lo = pl.ds(pl.multiple_of(i * per * size, per * size), per * size)
            value = dot_tn(left[:, lo], right).astype(BF)
            for j in range(per):
                dw[i * per + j] = value[j * size : (j + 1) * size]

    weight_grad(hid.reshape(R, D), cg.reshape(R, D)[...], dw_dn, wf)
    rg_own(0)
    ag_last(DNA)
    ag_last(DNB)

    def before_grad(theirs, ours, rows):
        count = rows.stop - rows.start
        slope = both_rows(gbf, theirs, ours, rows).astype(F32)
        grad = (dot_nt(both_rows(cg, theirs, ours, rows), wdn[...]) * slope).astype(BF)
        gbf[theirs, rows] = grad[:count]
        gbf[ours, rows] = grad[count:]
        gvec[8:9, :] += jnp.sum(grad.astype(F32), axis=0, keepdims=True)
        return dot_nt(grad, wup[...])

    seq_pass(0, gpart, gown, grecv, before_grad, poll=lambda: rg_fwd(0, 0))
    weight_grad(n2.reshape(R, D), gbf.reshape(R, D)[...], dw_up, w)
    rg_own(1)
    rg_own(6)

    def branch_rows(h):
        rows = halves[h]
        from_core(0, grecv, h)
        from_y(0, grecv, h)
        gn = gown[rows] + grecv[2, rows].astype(F32) + grecv[1, rows].astype(F32)
        unit, rate = unit_rows(mid[rows])
        c_own = cg[s, rows].astype(F32)
        gm = c_own + norm_pull(gn, row(5), unit, rate)
        gmid[rows] = gm
        branch = gm.astype(BF)
        nrm[s, rows] = branch
        sq_send(KG + h, g_slot(h))
        for k, value in ((5, gn * unit), (6, gn), (7, c_own), (4, branch.astype(F32))):
            gvec[k : k + 1, :] += jnp.sum(value, axis=0, keepdims=True)

    @pl.loop(0, 4)
    def _(k):
        first_norm(k, n2)

    branch_rows(0)
    rg_fwd(0, 1)

    def up_poll():
        rg_fwd(1, 0)
        rg_fwd(6, 0)

    seq_pass(1, opart, oown, orecv, lambda theirs, ours, rows: dot_nn(both_rows(hid, theirs, ours, rows), wdn[...]), defer=True, poll=up_poll)
    branch_rows(1)
    seq_sent(0, gpart)
    for h in range(2):
        seq_across(1, opart, orecv, h)

    flat_g = gctx.reshape(R, DH)
    dkt[...] = jnp.zeros_like(dkt)
    dvt[...] = jnp.zeros_like(dvt)

    def branch_back(k):
        gctx[k] = dot_nt(nrm[k], wout[pl.ds(pl.multiple_of(s * DH, DH), DH), :]).astype(BF)

    def close_pair(hp):
        lo = hp * 384
        flat[:, lo + 128 : lo + 256] = dkt[hp].T.astype(BF)
        flat[:, lo + 256 : lo + 384] = dvt[hp].T.astype(BF)
        weight_grad(n2.reshape(R, D), flat[:, lo : lo + 384], dw_qkv.at[hp], w)
        for m in ((3,), (4, 5))[hp]:
            rg_own(m)
        off = lanes_at(s * DH + hp * 128)
        gvec[2:3, off] = jnp.sum(flat[:, lo : lo + 128].astype(F32), axis=0, keepdims=True)
        gvec[3:4, off] = jnp.sum(flat[:, lo + 256 : lo + 384].astype(F32), axis=0, keepdims=True)

    branch_back(s)
    for h in range(2):
        sq_core(KG + h, g_slot(h))
    branch_back(s_core)

    @pl.loop(0, 8)
    def _(t):
        late, u = lax.div(t, 4), lax.rem(t, 4)
        hp = (1 - late) * lax.rem(u, 2) + late * lax.div(u, 2)
        flip = (1 - late) * lax.div(u, 2) + late * lax.rem(u, 2)
        k = lax.rem(y + late, 2) * 2 + lax.rem(c + flip, 2)
        query = pq[k, :, lanes_at(hp * 384)]
        keys = flat[:, lanes_at(hp * 384 + 128)]
        vals = flat[:, lanes_at(hp * 384 + 256)]
        grad = gctx[k, :, lanes_at(hp * 128)]
        logs = lse[hp, slot_rows(k), :]
        both = []
        for h in range(2):
            qh, gh = query * picks[h], grad * picks[h]
            probs = jnp.exp(dot_nt(qh, keys) + mask[...] - logs[:, h * HEAD_DIM : h * HEAD_DIM + 1])
            dp = dot_nt(gh, vals)
            inner = jnp.sum(probs * dp, axis=-1, keepdims=True)
            ds = (probs * (dp - inner)).astype(BF)
            both.append(dot_nn(ds, keys))
            dkt[hp] += dot_tn(qh, ds)
            dvt[hp] += dot_tn(gh, probs.astype(BF))
        dq = jnp.where(lane < HEAD_DIM, both[0], both[1]) * HEAD_DIM ** (-0.5)
        pq[k, :, lanes_at(hp * 384)] = dq.astype(BF)

        @pl.when(t == 0)
        def _():
            rg_fwd(0, 2)

        @pl.when(t == 1)
        def _():
            sq_relay(KG, g_slot(0))

        @pl.when(t == 2)
        def _():
            rg_fwd(1, 1)
            rg_fwd(6, 1)

        @pl.when(t == 3)
        def _():
            sq_relay(KG + 1, g_slot(1))
            branch_back(s_y)
            for h in range(2):
                sq_diag(KG + h, g_slot(h))
            branch_back(s_diag)
            right = nrm.reshape(R, D)[:, quarter]
            for j in range(4):
                value = dot_tn(ctx[j], right).astype(BF)
                for i in range(DH // w):
                    dw_out[j * (DH // w) + i] = value[i * w : (i + 1) * w]
            rg_own(2)
            rg_fin(0)

        @pl.when(t == 4)
        def _():
            rg_fwd(1, 2)

        @pl.when(t == 5)
        def _():
            rg_fwd(2, 0)
            rg_fwd(6, 2)
            close_pair(0)

        @pl.when(t == 6)
        def _():
            rg_fin(1)
            rg_fwd(2, 1)

        @pl.when(t == 7)
        def _():
            rg_fin(6)

    close_pair(1)
    rg_fwd(3, 0)
    rg_fwd(2, 2)

    def last_poll():
        rg_fwd(4, 0)
        rg_fwd(5, 0)

    seq_pass(2, gpart, gown, grecv, lambda theirs, ours, rows: dot_nt(both_rows(pq, theirs, ours, rows), wqkv[...]), poll=last_poll)
    rg_fwd(3, 1)
    for h in range(2):
        from_core(1, orecv, h)
        from_y(1, orecv, h)
    tok[...] = (mid[...] + (oown[...] + orecv[2].astype(F32) + orecv[1].astype(F32)) + row(7))[:T].astype(BF)
    put(tok, h_out, 8)
    rg_fin(2)
    for h in range(2):
        from_core(2, grecv, h)
    here = gown[...] + grecv[2].astype(F32)
    away = gpart[1].astype(F32)
    unit, rate = unit_rows(xg[s].astype(F32))
    unit_y, _ = unit_rows(xg[s_y].astype(F32))
    gvec[0:1, :] = jnp.sum(here * unit + away * unit_y, axis=0, keepdims=True)
    gvec[1:2, :] = jnp.sum(here + away, axis=0, keepdims=True)
    for k in range(N):
        j = k // g
        dw_sm[k] = gvec[:, j * 128 : (j + 1) * 128]
    for d in range(1, N):
        send(dw_sm.at[other(d)], rr_sm.at[d - 1], sg_s.at[0], sg_r.at[0], {"fsdp": other(d)})
    rg_fwd(4, 1)
    rg_fwd(5, 1)
    rg_fwd(3, 2)
    rg_fwd(4, 2)
    rg_fwd(5, 2)
    total = dw_sm[f]
    arrive(rr_sm, sg_r.at[0], to_ring[0])
    for d in range(1, N):
        total = total + rr_sm[d - 1]
    o_sm[s] = total
    for dev in (to_core, to_y, {"seq": s_diag}):
        send(o_sm.at[s], o_sm.at[s], sm_s.at[0], sm_r.at[0], dev)

    hbm = [h_dn, h_up.at[:, :, sides[0]], h_ow, h_qkv.at[0]]
    hbm += [h_qkv.at[1, :, split[h]] for h in range(2)] + [h_up.at[:, :, sides[1]]]
    finals = [(KFIN + m, fin_slot(m)) for m in range(MG)]

    def put_slot(m, k):
        put(grads[m][2].at[k], hbm[m].at[k], m)

    def relay_out(m):
        sq_relay(*finals[m])
        put_slot(m, s_y)

    for m in (0, 1, 6, 2):
        put_slot(m, s)
    relay_out(0)
    relay_out(1)
    rg_fin(3)
    put_slot(3, s)
    for m in (4, 5):
        rg_fin(m)
        put_slot(m, s)
    relay_out(6)
    for h in range(2):
        from_y(2, grecv, h)
    gn = here + grecv[1].astype(F32)
    cot[...] = (gmid[...] + norm_pull(gn, row(0), unit, rate))[:T].astype(BF)
    put(cot, h_tok, 9)
    for m in range(MG):
        sq_core(*finals[m])
        put_slot(m, s_core)
    for m in (2, 3, 4, 5):
        relay_out(m)
    arrive(o_sm.at[:3], sm_r.at[0], to_core)
    put(o_sm, h_sm, 7)
    for m in range(MG):
        sq_diag(*finals[m])
        put_slot(m, s_diag)

    for m in range(MA):
        ag_sent(m)
    for m in range(MG):
        rg_sent(m)
    for kind, ref in ((KX, xg), (KC, cg)):
        sq_sent(kind, ref.at[:3])
    for h in range(2):
        sq_sent(KG + h, nrm.at[:3, halves[h]])
    sq_sent(KO, wout.at[:, : 3 * DH])
    for hp in range(HP):
        sq_sent(KCTX + hp, ctx.at[:3, :, hp * 128 : hp * 128 + 128])
    for m in range(MG):
        sq_sent(KFIN + m, grads[m][2].at[:3])
    seq_sent(1, opart)
    seq_sent(2, gpart)
    sent(smg.at[: N - 1], sa_s.at[0], to_ring[0])
    sent(dw_sm.at[: N - 1], sg_s.at[0], to_ring[0])
    sent(o_sm.at[:3], sm_s.at[0], to_core)
    for src, dst, k in [(grads[m][2], hbm[m], m) for m in range(MG)] + [(o_sm, h_sm, 7), (tok, h_out, 8), (cot, h_tok, 9)]:
        pltpu.make_async_copy(src, dst, put_sem.at[k]).wait()


def finish_kernel(z, *refs):
    srcs, dsts = refs[:7], refs[7:22]
    (out, tok, gq, go, gu, gd, gs), bufs = refs[22:29], refs[29:42]
    s_in, s_out = refs[42:]
    D, w, wf, HP, N = z["D"], z["w"], z["wf"], z["HP"], 2 * z["A"]
    DH = D // 4
    loads = [pltpu.make_async_copy(src, dst, s_in.at[k]) for k, (src, dst) in enumerate(zip(srcs, (out, tok, gq, go, gu, gd, gs)))]
    saves = []

    def save(src, k):
        copy = pltpu.make_async_copy(src, dsts[k], s_out.at[k])
        copy.start()
        saves.append(copy)

    for k in (5, 4, 2, 3, 6, 0, 1):
        loads[k].start()
    f_qkv, f_ow, f_up, f_dn = bufs[:4]
    loads[5].wait()
    for s in range(4):
        f_dn[s * wf : (s + 1) * wf] = gd[s].astype(F32)
    save(f_dn, 5)
    loads[4].wait()
    if z["up_whole"]:
        for s in range(4):
            for k in range(N):
                f_up[:, (k * 4 + s) * wf : (k * 4 + s + 1) * wf] = gu[s, :, k * wf : (k + 1) * wf].astype(F32)
    else:
        f_up[...] = gu[...].astype(F32)
    save(f_up, 4)
    loads[2].wait()
    for s in range(4):
        for hp in range(HP):
            for part in range(3):
                lo = part * D + s * DH + hp * 128
                f_qkv[:, lo : lo + 128] = gq[hp, s, :, part * 128 : part * 128 + 128].astype(F32)
    save(f_qkv, 2)
    loads[3].wait()
    for s in range(4):
        f_ow[:, s * DH : (s + 1) * DH] = go[s].astype(F32)
    save(f_ow, 3)
    loads[6].wait()
    total = gs[0] + gs[1] + gs[2] + gs[3]
    for k in range(8):
        bufs[4 + k][...] = total[k : k + 1]
        save(bufs[4 + k], 6 + k)
    bufs[12][...] = jnp.concatenate([gs[s, 8:9] for s in range(4)], axis=1)
    save(bufs[12], 14)
    for k, buf in ((0, out), (1, tok)):
        loads[k].wait()
        save(buf, k)
    for copy in saves:
        copy.wait()


def make_body(mesh):
    N = mesh.shape["fsdp"]
    A = N // 2

    def body(
        tokens, lengths, ln1_gain, ln1_bias, qkv_weight, q_bias, v_bias, out_weight, out_bias,
        ln2_gain, ln2_bias, up_weight, up_bias, down_weight, down_bias, cotangent,
    ):
        _, T, D = tokens.shape
        w, FF = D // N, up_weight.shape[1]
        wf = FF // (4 * N)
        TP = -(-T // 16) * 16
        R = 4 * TP
        DH = D // 4
        HP = DH // 128
        FQ = FF // 4
        assert FQ == D and wf == w and HP == 2
        g = max(128 // w, 1)
        s = lax.axis_index("seq")
        f = lax.axis_index("fsdp")
        up_whole = wf % 128 == 0
        plain = (ln1_gain, ln1_bias, q_bias, v_bias, out_bias, ln2_gain, ln2_bias, down_bias)
        if g == 1:
            vectors_in = [v.reshape(1, w) for v in plain]
            ub_in = up_bias.reshape(4, wf)
        else:
            spot = lax.rem(f, g) * w
            blank = jnp.zeros((1, 128), BF)
            vectors_in = [lax.dynamic_update_slice(blank, v[None], (0, spot)) for v in plain]
            mine = lax.dynamic_slice(up_bias, (s * wf,), (wf,))
            ub_in = lax.dynamic_update_slice(jnp.zeros((4, 128), BF), mine[None], (s, spot))
        if not up_whole:
            up_weight = lax.dynamic_index_in_dim(up_weight.reshape(w, N, 4, wf), s, 2, False).reshape(w, FQ)
        z = dict(D=D, T=T, TP=TP, R=R, A=A, w=w, wf=wf, HP=HP, g=g, up_whole=up_whole)
        vm = pltpu.VMEM
        C = 384
        scratch = [
            vm((T, D), BF), vm((T, D), BF), pltpu.SMEM((1,), jnp.int32), vm((8, 1, 128), BF), vm((4, 128), BF),
            vm((HP, 4, w, C), BF), vm((4, w, DH), BF), vm((4, w, FQ), BF), vm((4, wf, D), BF), vm((4, 16, 128), F32),
            vm((4, TP, D), BF),
            vm((4, TP, D), BF),
            vm((4, TP, D), BF),
            vm((4, R, DH), BF),
            vm((4, TP, D), BF),
            vm((4, TP, D), BF),
            vm((4, TP, D), BF),
            vm((4, TP, HP * C), BF),
            vm((D, HP * C), BF),
            vm((D, D), BF),
            vm((D, FQ), BF),
            vm((FQ, D), BF),
            vm((N, 16, 128), BF),
            vm((16, D), F32),
            vm((16, D), F32),
            vm((HP, R, 128), F32),
            vm((TP, D), F32),
            vm((TP, D), F32),
            vm((4, TP, DH), BF),
            vm((HP, 128, R), F32),
            vm((HP, 128, R), F32),
            vm((3, TP, D), BF), vm((TP, D), F32), vm((3, TP, D), BF),
            vm((3, TP, D), BF), vm((TP, D), F32), vm((3, TP, D), BF),
            vm((1, R), F32),
            vm((HP, N, w, C), BF), vm((N, w, DH), BF), vm((N, w, FQ), BF), vm((N, wf, D), BF), vm((N, 16, 128), F32),
            vm((HP, 2, A, w, C), BF), vm((2, A, w, DH), BF), vm((2, A, w, FQ), BF), vm((2, A, wf, D), BF), vm((N - 1, 16, 128), F32),
        ]
        dma = pltpu.SemaphoreType.DMA
        scratch += [
            dma((9,)), dma((10,)),
            dma((4 + HP,)), dma((4 + HP, A)), dma((7,)), dma((7, A)),
            dma((12 + HP,)), dma((12 + HP, 3)),
            dma((3,)), dma((3, 3, 2)),
            dma((1,)), dma((1,)), dma((1,)), dma((1,)), dma((1,)), dma((1,)),
        ]
        there = pl.BlockSpec(memory_space=pl.ANY)
        out_shapes = [
            jax.ShapeDtypeStruct((T, D), BF),
            jax.ShapeDtypeStruct((T, D), BF),
            jax.ShapeDtypeStruct((HP, 4, w, C), BF),
            jax.ShapeDtypeStruct((4, w, DH), BF),
            jax.ShapeDtypeStruct((4, w, FQ), BF),
            jax.ShapeDtypeStruct((4, wf, D), BF),
            jax.ShapeDtypeStruct((4, 16, 128), F32),
        ]
        out, gtok, gq, go, gu, gd, gs = pl.pallas_call(
            functools.partial(layer_entry, z),
            out_shape=out_shapes,
            in_specs=[there] * 16,
            out_specs=[there] * 7,
            scratch_shapes=scratch,
            compiler_params=pltpu.CompilerParams(
                collective_id=0, has_side_effects=True, vmem_limit_bytes=67_000_000
            ),
            name="layer",
        )(tokens[0], cotangent[0], lengths, *vectors_in, ub_in, qkv_weight, out_weight, up_weight, down_weight)

        if not up_whole:
            gu = gu.reshape(4, w, N, wf).transpose(1, 2, 0, 3).reshape(w, FF)
        if g > 1:
            gs = lax.dynamic_slice(gs, (0, 0, lax.rem(f, g) * w), (4, 16, w))
        shapes = [((w, 3 * D), F32), ((w, D), F32), ((w, FF), F32), ((4 * wf, D), F32)]
        shapes += [((1, w), F32)] * 8 + [((1, 4 * wf), F32)]
        sources = (out, gtok, gq, go, gu, gd, gs)
        done = pl.pallas_call(
            functools.partial(finish_kernel, z),
            out_shape=[jax.ShapeDtypeStruct(*v) for v in [((T, D), BF)] * 2 + shapes],
            in_specs=[there] * 7,
            out_specs=[there] * 15,
            scratch_shapes=[vm(v.shape, v.dtype) for v in sources] + [vm(*v) for v in shapes] + [dma((7,)), dma((15,))],
            name="finish",
        )(*sources)
        out, gtok, g_qkv, g_out, g_up, g_down = done[:6]
        sums = [v.reshape(-1) for v in done[6:]]
        return (
            out[None], gtok[None], sums[0], sums[1], g_qkv, sums[2], sums[3], g_out, sums[4],
            sums[5], sums[6], g_up, sums[8], g_down, sums[7],
        )

    return body


def solution(mesh):
    row, mat, act = P("fsdp"), P("fsdp", None), P("fsdp", "seq", None)
    return jax.shard_map(
        make_body(mesh),
        mesh=mesh,
        in_specs=(act, row, row, row, mat, row, row, mat, row, row, row, mat, row, mat, row, act),
        out_specs=(act, act, row, row, mat, row, row, mat, row, row, row, mat, row, mat, row),
        check_vma=False,
    )
```

```python
import functools
import math

import jax
import jax.numpy as jnp
from jax import lax
from jax.experimental import pallas as pl
from jax.experimental.pallas import tpu as pltpu
from jax.sharding import PartitionSpec as P

HEAD_DIM = 64
BF = jnp.bfloat16
F32 = jnp.float32
MESH = pl.DeviceIdType.MESH


def dot_nn(left, right):
    return lax.dot_general(left, right, (((1,), (0,)), ((), ())), preferred_element_type=F32)


def dot_nt(left, right):
    return lax.dot_general(left, right, (((1,), (1,)), ((), ())), preferred_element_type=F32)


def dot_tn(left, right):
    return lax.dot_general(left, right, (((0,), (0,)), ((), ())), preferred_element_type=F32)


def unit_rows(values):
    center = values - jnp.mean(values, axis=-1, keepdims=True)
    rate = lax.rsqrt(jnp.mean(center * center, axis=-1, keepdims=True) + 1e-6)
    return center * rate, rate


def norm_pull(grad, gain, unit, rate):
    scaled = grad * gain
    return rate * (
        scaled
        - jnp.mean(scaled, axis=-1, keepdims=True)
        - unit * jnp.mean(scaled * unit, axis=-1, keepdims=True)
    )


def layer_entry(z, *refs):
    layer_kernel(z, *refs[:3], refs[3:11], *refs[11:])


def layer_kernel(
    z,
    tok_in, cot_in, len_in, vecs_in, ub_in, qkv_in, out_in, up_in, dn_in,
    h_out, h_tok, h_qkv, h_ow, h_up, h_dn, h_sm,
    tok, cot, lens, vecs, ub4, o_qkv, o_ow, o_up, o_dn, o_sm,
    xg, cg, nrm, ctx, n2, hid, gbf, pq, wqkv, wout, wup, wdn, smg, vec, gvec, lse, mid, gmid,
    gctx, dkt, dvt, gpart, gown, grecv, opart, oown, orecv, mask,
    dw_qkv, dw_out, dw_up, dw_dn, dw_sm, rr_qkv, rr_out, rr_up, rr_dn, rr_sm,
    loc_sem, put_sem, ag_s, ag_r, rg_s, rg_r, sq_s, sq_r, rs_s, rs_r, sa_s, sa_r, sg_s, sg_r, sm_s, sm_r,
):
    D, T, TP, R, A, w, wf, HP = z["D"], z["T"], z["TP"], z["R"], z["A"], z["w"], z["wf"], z["HP"]
    N, H, DH, LB, g = 2 * A, A, D // 4, D // 128, z["g"]
    s = lax.axis_index("seq")
    f = lax.axis_index("fsdp")
    y, c = lax.div(s, 2), lax.rem(s, 2)
    s_core, s_y, s_diag = y * 2 + 1 - c, (1 - y) * 2 + c, (1 - y) * 2 + 1 - c
    to_core, to_y = {"seq": s_core}, {"seq": s_y}

    odd = lax.rem(f, 2)
    place = (1 - odd) * lax.div(f, 2) + odd * (N - 1 - lax.div(f, 2))

    def at_place(q):
        late = lax.div(q, A)
        return (1 - late) * 2 * q + late * (2 * (N - 1 - q) + 1)

    def ahead(d):
        return at_place(lax.rem(place + d + N, N))

    to_ring = ({"fsdp": ahead(1)}, {"fsdp": ahead(-1)})

    def send(src, dst, ssem, rsem, dev):
        pltpu.make_async_remote_copy(
            src_ref=src, dst_ref=dst, send_sem=ssem, recv_sem=rsem, device_id=dev, device_id_type=MESH
        ).start()

    def arrive(dst, rsem, dev):
        pltpu.make_async_remote_copy(
            src_ref=dst, dst_ref=dst, send_sem=rsem, recv_sem=rsem, device_id=dev, device_id_type=MESH
        ).wait_recv()

    def sent(src, ssem, dev):
        pltpu.make_async_remote_copy(
            src_ref=src, dst_ref=src, send_sem=ssem, recv_sem=ssem, device_id=dev, device_id_type=MESH
        ).wait_send()

    def thirds(first, last):
        count = max(last - first, 0)
        cut = [first + (count * k) // 3 for k in range(4)]
        return [range(cut[k], cut[k + 1]) for k in range(3)]

    quarter = pl.ds(pl.multiple_of(s * DH, DH), DH)

    def rows_of(k, size, half=None):
        if half is None:
            return pl.ds(pl.multiple_of(k * size, size), size)
        return pl.ds(pl.multiple_of(k * size + half * (size // 2), size // 2), size // 2)

    OUT, UP, DNA, DNB = HP, HP + 1, HP + 2, HP + 3
    MA = HP + 4
    low, high = slice(0, D // 2), slice(D // 2, D)
    blocks = {
        OUT: lambda k, half=None: wout.at[rows_of(k, w, half), quarter],
        UP: lambda k, half=None: wup.at[rows_of(k, w, half)],
        DNA: lambda k, half=None: wdn.at[rows_of(k, wf, half), low],
        DNB: lambda k, half=None: wdn.at[rows_of(k, wf, half), high],
    }
    for hp in range(HP):
        blocks[hp] = lambda k, half=None, hp=hp: wqkv.at[rows_of(k, w, half), hp * 384 : hp * 384 + 384]

    def ag_block(m, way, d, back):
        k = ahead(-back if way == 0 else back)
        return blocks[m](k, way if d == H else None)

    def ag_own(m):
        for way in range(2):
            ref = ag_block(m, way, 1, 0)
            send(ref, ref, ag_s.at[m], ag_r.at[m, 0], to_ring[way])

    def ag_take(m, d):
        arrive(ag_rows(m, 1 if d == H else 2), ag_r.at[m, d - 1], to_ring[0])
        for way in range(2):
            if d < H:
                ref = ag_block(m, way, d + 1, d)
                send(ref, ref, ag_s.at[m], ag_r.at[m, d], to_ring[way])

    def ag_fwd(m, third):
        for d in thirds(1, H)[third]:
            ag_take(m, d)

    def ag_last(m):
        ag_take(m, H)

    def ag_rows(m, shards):
        size = shards * (wf if m in (DNA, DNB) else w)
        every = {OUT: wout.at[:size, quarter], UP: wup.at[:size], DNA: wdn.at[:size, low], DNB: wdn.at[:size, high]}
        return every[m] if m in every else wqkv.at[:size, m * 384 : m * 384 + 384]

    def ag_sent(m):
        sent(ag_rows(m, N - 1), ag_s.at[m], to_ring[0])

    def sq_send(kind, ref):
        send(ref(s), ref(s), sq_s.at[kind], sq_r.at[kind, 0], to_core)
        send(ref(s), ref(s), sq_s.at[kind], sq_r.at[kind, 1], to_y)

    def sq_core(kind, ref):
        arrive(ref(s_core), sq_r.at[kind, 0], to_core)

    def sq_relay(kind, ref):
        arrive(ref(s_y), sq_r.at[kind, 1], to_y)
        send(ref(s_y), ref(s_y), sq_s.at[kind], sq_r.at[kind, 2], to_core)

    def sq_diag(kind, ref):
        arrive(ref(s_diag), sq_r.at[kind, 2], to_core)

    def sq_sent(kind, three):
        sent(three, sq_s.at[kind], to_core)

    def x_slot(k):
        return xg.at[k]

    def c_slot(k):
        return cg.at[k]

    def g_slot(h):
        return lambda k: nrm.at[k, halves[h]]

    def out_slot(k):
        return wout.at[:, pl.ds(pl.multiple_of(k * DH, DH), DH)]

    def ctx_slot(hp):
        return lambda k: ctx.at[k, :, hp * 128 : hp * 128 + 128]

    KX, KC, KG, KO, KCTX, KFIN = 0, 1, 2, 4, 5, 5 + HP

    def order(i):
        hb, lb = lax.div(3 - i, 2), lax.rem(3 - i, 2)
        return lax.rem(y + hb, 2) * 2 + lax.rem(c + lb, 2)

    cut = -(-TP // 32) * 16
    halves = (slice(0, cut), slice(cut, TP))

    def seq_across(kind, part, recv, h):
        send(part.at[1, halves[h]], recv.at[1, halves[h]], rs_s.at[kind], rs_r.at[kind, 1, h], to_y)

    def seq_pass(kind, part, own, recv, compute, defer=False, poll=None):
        def chip_sum(h):
            rows = halves[h]
            arrive(recv.at[0, rows], rs_r.at[kind, 0, h], to_core)
            part[1, rows] = (part[1, rows].astype(F32) + recv[0, rows].astype(F32)).astype(BF)
            if not defer:
                seq_across(kind, part, recv, h)

        @pl.loop(0, 2)
        def _(p):
            chip = lax.rem(y + 1 - p, 2) * 2
            theirs, ours = chip + 1 - c, chip + c
            for h, rows in enumerate(halves):
                count = rows.stop - rows.start
                value = compute(theirs, ours, rows)

                @pl.when(p == 0)
                def _():
                    part[0, rows] = value[:count].astype(BF)
                    part[1, rows] = value[count:].astype(BF)
                    send(part.at[0, rows], recv.at[0, rows], rs_s.at[kind], rs_r.at[kind, 0, h], to_core)
                    if h == 1:
                        chip_sum(0)

                @pl.when(p == 1)
                def _():
                    part[2, rows] = value[:count].astype(BF)
                    own[rows] = value[count:]
                    send(part.at[2, rows], recv.at[2, rows], rs_s.at[kind], rs_r.at[kind, 2, h], to_core)
                    if h == 0:
                        chip_sum(1)
                        if poll:
                            poll()

    def both_rows(ref, theirs, ours, rows):
        return jnp.concatenate([ref[theirs, rows], ref[ours, rows]], axis=0)

    def seq_sent(kind, part):
        sent(part, rs_s.at[kind], to_core)

    def from_core(kind, recv, h):
        arrive(recv.at[2, halves[h]], rs_r.at[kind, 2, h], to_core)

    def from_y(kind, recv, h):
        arrive(recv.at[1, halves[h]], rs_r.at[kind, 1, h], to_y)

    grads = {0: (dw_dn, rr_dn, o_dn), 2: (dw_out, rr_out, o_ow)}
    FQ = dw_up.shape[2]
    sides = (slice(0, FQ // 2), slice(FQ // 2, FQ))
    for m, side in zip((1, 6), sides):
        grads[m] = (dw_up.at[:, :, side], rr_up.at[:, :, :, side], o_up.at[:, :, side])
    grads[3] = (dw_qkv.at[0], rr_qkv.at[0], o_qkv.at[0])
    split = (slice(0, w // 2), slice(w // 2, w))
    for h in range(2):
        grads[4 + h] = (dw_qkv.at[1, :, split[h]], rr_qkv.at[1, :, :, split[h]], o_qkv.at[1, :, split[h]])
    MG = 7

    def rg_rows(m, way, j):
        size = grads[m][0].shape[1]
        return slice(way * (size // 2), (way + 1) * (size // 2)) if j == 0 else slice(0, size)

    def rg_owner(way, j):
        return ahead(H - j if way == 0 else j - H)

    def rg_src(m, way, j):
        return grads[m][0].at[rg_owner(way, j), rg_rows(m, way, j)]

    def rg_send(m, way, j):
        dst = grads[m][1].at[way, j, rg_rows(m, way, j)]
        send(rg_src(m, way, j), dst, rg_s.at[m], rg_r.at[m, j], to_ring[way])

    def rg_arrive(m, j):
        arrive(grads[m][0].at[: 1 if j == 0 else 2], rg_r.at[m, j], to_ring[0])

    def rg_own(m):
        for way in range(2):
            rg_send(m, way, 0)

    def rg_fwd(m, third):
        dw, rr, _ = grads[m]
        for j in thirds(1, H)[third]:
            rg_arrive(m, j - 1)
            for way in range(2):
                rows = rg_rows(m, way, j - 1)
                owner = rg_owner(way, j)
                dw[owner, rows] = (dw[owner, rows].astype(F32) + rr[way, j - 1, rows].astype(F32)).astype(dw.dtype)
                rg_send(m, way, j)

    def fin_slot(m):
        return lambda k: grads[m][2].at[k]

    def rg_fin(m):
        dw, rr, out = grads[m]
        total = dw[f].astype(F32)
        rg_arrive(m, H - 1)
        for way in range(2):
            total = total + rr[way, H - 1].astype(F32)
        out[s] = total.astype(out.dtype)
        sq_send(KFIN + m, fin_slot(m))

    def rg_sent(m):
        sent(grads[m][0].at[: N - 1], rg_s.at[m], to_ring[0])

    def other(d):
        return lax.rem(f + d, N)

    barrier = pltpu.get_barrier_semaphore()
    peers = [to_core, to_y, {"seq": s_diag}] + [{"fsdp": other(d)} for d in range(1, N)]
    for dev in peers:
        pl.semaphore_signal(barrier, inc=1, device_id=dev, device_id_type=MESH)

    def bring(k, src, dst):
        pltpu.make_async_copy(src, dst, loc_sem.at[k]).start()

    bring(0, tok_in, tok)
    for k in range(8):
        bring(1, vecs_in[k], vecs.at[k])
    bring(2, ub_in, ub4)
    for hp in range(HP):
        for part in range(3):
            cols = pl.ds(pl.multiple_of(part * D + s * DH + hp * 128, 128), 128)
            lo = hp * 384 + part * 128
            bring(3, qkv_in.at[:, cols], wqkv.at[rows_of(f, w), lo : lo + 128])
    bring(4, out_in.at[:, quarter], wout.at[rows_of(f, w), quarter])
    bring(5, cot_in, cot)
    bring(6, len_in, lens)
    if z["up_whole"]:
        for k in range(N):
            cols = pl.ds(pl.multiple_of((k * 4 + s) * wf, wf), wf)
            bring(7, up_in.at[:, cols], wup.at[rows_of(f, w), k * wf : (k + 1) * wf])
    else:
        bring(7, up_in, wup.at[rows_of(f, w)])
    bring(8, dn_in.at[rows_of(s, wf)], wdn.at[rows_of(f, wf)])

    def put(src, dst, k):
        pltpu.make_async_copy(src, dst, put_sem.at[k]).start()

    def padded(ref):
        return jnp.concatenate([ref[...].astype(F32), jnp.zeros((TP - T, D), F32)], axis=0)

    gvec[...] = jnp.zeros_like(gvec)
    own_rows = [tok, vecs, ub4, wqkv.at[rows_of(f, w)], wout.at[rows_of(f, w), quarter], cot, lens, wup.at[rows_of(f, w)], wdn.at[rows_of(f, wf)]]
    for k, dst in enumerate(own_rows):
        pltpu.make_async_copy(dst, dst, loc_sem.at[k]).wait()
    quarters = ub4[...].astype(F32)
    ub = sum(quarters[k : k + 1] * (s == k).astype(F32) for k in range(4))
    vector_rows = [vecs[k].astype(F32) for k in range(8)] + [ub, jnp.zeros((7, 128), F32)]
    smg[f] = jnp.concatenate(vector_rows, axis=0).astype(BF)
    xg[s] = padded(tok).astype(BF)
    cg[s] = padded(cot).astype(BF)
    column = lax.broadcasted_iota(jnp.int32, (1, R), 1)
    slot = sum((column >= TP * k).astype(jnp.int32) for k in range(1, 4))
    inside = column - slot * TP
    valid = (inside < T) & (slot * T + inside < lens[0])
    mask[...] = jnp.where(valid, 0.0, -1e30).astype(F32)
    pl.semaphore_wait(barrier, len(peers))

    for d in range(1, N):
        send(smg.at[f], smg.at[f], sa_s.at[0], sa_r.at[0], {"fsdp": other(d)})
    sq_send(KX, x_slot)
    for m in (0, 1, OUT):
        ag_own(m)
    sq_send(KC, c_slot)
    arrive(smg.at[: N - 1], sa_r.at[0], to_ring[0])
    for j in range(LB):
        piece = smg[j * g].astype(F32)
        for i in range(1, g):
            piece = piece + smg[j * g + i].astype(F32)
        vec[:, j * 128 : (j + 1) * 128] = piece

    def row(k):
        return vec[k : k + 1, :]

    def first_norm(k, into=nrm):
        unit, _ = unit_rows(xg[k].astype(F32))
        into[k] = (unit * row(0) + row(1)).astype(BF)

    def project(hp):
        cols = pl.ds(pl.multiple_of(s * DH + hp * 128, 128), 128)
        bias = jnp.concatenate([vec[2:3, cols], jnp.zeros((1, 128), F32), vec[3:4, cols]], axis=1)
        lanes = lax.broadcasted_iota(jnp.int32, (1, 384), 1)
        scale = jnp.where(lanes < 128, HEAD_DIM ** (-0.5), 1.0).astype(F32)
        here = slice(hp * 384, hp * 384 + 384)

        @pl.loop(0, 4)
        def _(k):
            pq[k, :, here] = ((dot_nn(nrm[k], wqkv[:, here]) + bias) * scale).astype(BF)

    first_norm(s)
    ag_fwd(0, 0)
    sq_core(KX, x_slot)
    first_norm(s_core)
    ag_fwd(1, 0)
    ag_fwd(OUT, 0)
    ag_fwd(0, 1)
    ag_fwd(1, 1)
    ag_fwd(OUT, 1)
    sq_relay(KX, x_slot)
    first_norm(s_y)
    ag_fwd(0, 2)
    ag_fwd(1, 2)
    ag_fwd(OUT, 2)
    ag_own(UP)
    ag_own(DNA)
    ag_own(DNB)
    sq_diag(KX, x_slot)
    first_norm(s_diag)
    ag_last(0)
    project(0)

    flat = pq.reshape(R, HP * 384)
    lane = lax.broadcasted_iota(jnp.int32, (1, 128), 1)
    first = (lane < HEAD_DIM).astype(F32)
    picks = (first.astype(BF), (1.0 - first).astype(BF))

    def lanes_at(off):
        return pl.ds(pl.multiple_of(off, 128), 128)

    def slot_rows(k):
        return pl.ds(pl.multiple_of(k * TP, 16), TP)

    @pl.loop(0, 8)
    def _(t):
        hp, k = lax.div(t, 4), lax.rem(t, 4)
        query = pq[k, :, lanes_at(hp * 384)]
        keys = flat[:, lanes_at(hp * 384 + 128)]
        vals = flat[:, lanes_at(hp * 384 + 256)]
        both, logs = [], []
        for h in range(2):
            scores = dot_nt(query * picks[h], keys) + mask[...]
            top = jnp.max(scores, axis=-1, keepdims=True)
            grown = jnp.exp(scores - top)
            total = jnp.sum(grown, axis=-1, keepdims=True)
            logs.append(top + jnp.log(total))
            both.append(dot_nn((grown * (1.0 / total)).astype(BF), vals))
        rows = slot_rows(k)
        ctx[s, rows, lanes_at(hp * 128)] = jnp.where(lane < HEAD_DIM, both[0], both[1]).astype(BF)
        lse[hp, rows, :] = jnp.where(lane < HEAD_DIM, logs[0], logs[1])

        @pl.when(t == 0)
        def _():
            ag_last(OUT)
            sq_send(KO, out_slot)
            ag_last(1)
            project(1)

        @pl.when(t == 2)
        def _():
            ag_fwd(UP, 0)
            sq_relay(KC, c_slot)

        @pl.when(t == 3)
        def _():
            sq_send(KCTX, ctx_slot(0))

        @pl.when(t == 5)
        def _():
            ag_fwd(DNA, 0)

        @pl.when(t == 7)
        def _():
            sq_send(KCTX + 1, ctx_slot(1))

    sq_relay(KO, out_slot)
    ag_fwd(UP, 1)
    ag_fwd(DNB, 0)
    sq_relay(KCTX, ctx_slot(0))
    sq_core(KO, out_slot)
    sq_diag(KO, out_slot)
    sq_core(KCTX, ctx_slot(0))
    sq_core(KCTX + 1, ctx_slot(1))
    sq_relay(KCTX + 1, ctx_slot(1))
    ag_fwd(UP, 2)
    ag_fwd(DNA, 1)
    sq_diag(KCTX, ctx_slot(0))
    sq_diag(KCTX + 1, ctx_slot(1))

    @pl.loop(0, 4)
    def _(i):
        k = order(i)
        joined = jnp.concatenate([ctx[j, slot_rows(k), :] for j in range(4)], axis=1)
        value = xg[k].astype(F32) + dot_nn(joined, wout[...]) + row(4)
        unit, _ = unit_rows(value)
        n2[k] = (unit * row(5) + row(6)).astype(BF)

        @pl.when(i == 3)
        def _():
            mid[...] = value

        @pl.when(i == 1)
        def _():
            ag_fwd(DNB, 1)

    sq_core(KC, c_slot)
    sq_diag(KC, c_slot)
    ag_last(UP)

    @pl.loop(0, 4)
    def _(k):
        before = dot_nn(n2[k], wup[...]) + row(8)
        cdf = 0.5 + 0.5 * lax.erf(before * (0.5**0.5))
        slope = cdf + before * (jnp.exp(before * before * -0.5) * (1.0 / math.sqrt(2.0 * math.pi)))
        hid[k] = (before * cdf).astype(BF)
        gbf[k] = slope.astype(BF)

        @pl.when(k == 1)
        def _():
            ag_fwd(DNA, 2)

    ag_fwd(DNB, 2)

    def weight_grad(left, right, dw, size):
        per = max(512 // size, 1)

        @pl.loop(0, dw.shape[0] // per)
        def _(i):
            lo = pl.ds(pl.multiple_of(i * per * size, per * size), per * size)
            value = dot_tn(left[:, lo], right).astype(BF)
            for j in range(per):
                dw[i * per + j] = value[j * size : (j + 1) * size]

    weight_grad(hid.reshape(R, D), cg.reshape(R, D)[...], dw_dn, wf)
    rg_own(0)
    ag_last(DNA)
    ag_last(DNB)

    def before_grad(theirs, ours, rows):
        count = rows.stop - rows.start
        slope = both_rows(gbf, theirs, ours, rows).astype(F32)
        grad = (dot_nt(both_rows(cg, theirs, ours, rows), wdn[...]) * slope).astype(BF)
        gbf[theirs, rows] = grad[:count]
        gbf[ours, rows] = grad[count:]
        gvec[8:9, :] += jnp.sum(grad.astype(F32), axis=0, keepdims=True)
        return dot_nt(grad, wup[...])

    seq_pass(0, gpart, gown, grecv, before_grad, poll=lambda: rg_fwd(0, 0))
    weight_grad(n2.reshape(R, D), gbf.reshape(R, D)[...], dw_up, w)
    rg_own(1)
    rg_own(6)

    def branch_rows(h):
        rows = halves[h]
        from_core(0, grecv, h)
        from_y(0, grecv, h)
        gn = gown[rows] + grecv[2, rows].astype(F32) + grecv[1, rows].astype(F32)
        unit, rate = unit_rows(mid[rows])
        c_own = cg[s, rows].astype(F32)
        gm = c_own + norm_pull(gn, row(5), unit, rate)
        gmid[rows] = gm
        branch = gm.astype(BF)
        nrm[s, rows] = branch
        sq_send(KG + h, g_slot(h))
        for k, value in ((5, gn * unit), (6, gn), (7, c_own), (4, branch.astype(F32))):
            gvec[k : k + 1, :] += jnp.sum(value, axis=0, keepdims=True)

    @pl.loop(0, 4)
    def _(k):
        first_norm(k, n2)

    branch_rows(0)
    rg_fwd(0, 1)

    def up_poll():
        rg_fwd(1, 0)
        rg_fwd(6, 0)

    seq_pass(1, opart, oown, orecv, lambda theirs, ours, rows: dot_nn(both_rows(hid, theirs, ours, rows), wdn[...]), defer=True, poll=up_poll)
    branch_rows(1)
    seq_sent(0, gpart)
    for h in range(2):
        seq_across(1, opart, orecv, h)

    flat_g = gctx.reshape(R, DH)
    dkt[...] = jnp.zeros_like(dkt)
    dvt[...] = jnp.zeros_like(dvt)

    def branch_back(k):
        gctx[k] = dot_nt(nrm[k], wout[pl.ds(pl.multiple_of(s * DH, DH), DH), :]).astype(BF)

    def close_pair(hp):
        lo = hp * 384
        flat[:, lo + 128 : lo + 256] = dkt[hp].T.astype(BF)
        flat[:, lo + 256 : lo + 384] = dvt[hp].T.astype(BF)
        weight_grad(n2.reshape(R, D), flat[:, lo : lo + 384], dw_qkv.at[hp], w)
        for m in ((3,), (4, 5))[hp]:
            rg_own(m)
        off = lanes_at(s * DH + hp * 128)
        gvec[2:3, off] = jnp.sum(flat[:, lo : lo + 128].astype(F32), axis=0, keepdims=True)
        gvec[3:4, off] = jnp.sum(flat[:, lo + 256 : lo + 384].astype(F32), axis=0, keepdims=True)

    branch_back(s)
    for h in range(2):
        sq_core(KG + h, g_slot(h))
    branch_back(s_core)

    @pl.loop(0, 8)
    def _(t):
        late, u = lax.div(t, 4), lax.rem(t, 4)
        hp = (1 - late) * lax.rem(u, 2) + late * lax.div(u, 2)
        flip = (1 - late) * lax.div(u, 2) + late * lax.rem(u, 2)
        k = lax.rem(y + late, 2) * 2 + lax.rem(c + flip, 2)
        query = pq[k, :, lanes_at(hp * 384)]
        keys = flat[:, lanes_at(hp * 384 + 128)]
        vals = flat[:, lanes_at(hp * 384 + 256)]
        grad = gctx[k, :, lanes_at(hp * 128)]
        logs = lse[hp, slot_rows(k), :]
        both = []
        for h in range(2):
            qh, gh = query * picks[h], grad * picks[h]
            probs = jnp.exp(dot_nt(qh, keys) + mask[...] - logs[:, h * HEAD_DIM : h * HEAD_DIM + 1])
            dp = dot_nt(gh, vals)
            inner = jnp.sum(probs * dp, axis=-1, keepdims=True)
            ds = (probs * (dp - inner)).astype(BF)
            both.append(dot_nn(ds, keys))
            dkt[hp] += dot_tn(qh, ds)
            dvt[hp] += dot_tn(gh, probs.astype(BF))
        dq = jnp.where(lane < HEAD_DIM, both[0], both[1]) * HEAD_DIM ** (-0.5)
        pq[k, :, lanes_at(hp * 384)] = dq.astype(BF)

        @pl.when(t == 0)
        def _():
            rg_fwd(0, 2)

        @pl.when(t == 1)
        def _():
            sq_relay(KG, g_slot(0))

        @pl.when(t == 2)
        def _():
            rg_fwd(1, 1)
            rg_fwd(6, 1)

        @pl.when(t == 3)
        def _():
            sq_relay(KG + 1, g_slot(1))
            branch_back(s_y)
            for h in range(2):
                sq_diag(KG + h, g_slot(h))
            branch_back(s_diag)
            right = nrm.reshape(R, D)[:, quarter]
            for j in range(4):
                value = dot_tn(ctx[j], right).astype(BF)
                for i in range(DH // w):
                    dw_out[j * (DH // w) + i] = value[i * w : (i + 1) * w]
            rg_own(2)
            rg_fin(0)

        @pl.when(t == 4)
        def _():
            rg_fwd(1, 2)

        @pl.when(t == 5)
        def _():
            rg_fwd(2, 0)
            rg_fwd(6, 2)
            close_pair(0)

        @pl.when(t == 6)
        def _():
            rg_fin(1)
            rg_fwd(2, 1)

        @pl.when(t == 7)
        def _():
            rg_fin(6)

    close_pair(1)
    rg_fwd(3, 0)
    rg_fwd(2, 2)

    def last_poll():
        rg_fwd(4, 0)
        rg_fwd(5, 0)

    seq_pass(2, gpart, gown, grecv, lambda theirs, ours, rows: dot_nt(both_rows(pq, theirs, ours, rows), wqkv[...]), poll=last_poll)
    rg_fwd(3, 1)
    for h in range(2):
        from_core(1, orecv, h)
        from_y(1, orecv, h)
    tok[...] = (mid[...] + (oown[...] + orecv[2].astype(F32) + orecv[1].astype(F32)) + row(7))[:T].astype(BF)
    put(tok, h_out, 8)
    rg_fwd(4, 1)
    for h in range(2):
        from_core(2, grecv, h)
    here = gown[...] + grecv[2].astype(F32)
    away = gpart[1].astype(F32)
    unit, rate = unit_rows(xg[s].astype(F32))
    unit_y, _ = unit_rows(xg[s_y].astype(F32))
    gvec[0:1, :] = jnp.sum(here * unit + away * unit_y, axis=0, keepdims=True)
    gvec[1:2, :] = jnp.sum(here + away, axis=0, keepdims=True)
    for k in range(N):
        j = k // g
        dw_sm[k] = gvec[:, j * 128 : (j + 1) * 128]
    for d in range(1, N):
        send(dw_sm.at[other(d)], rr_sm.at[d - 1], sg_s.at[0], sg_r.at[0], {"fsdp": other(d)})
    rg_fwd(5, 1)
    rg_fin(2)
    rg_fwd(3, 2)
    rg_fwd(4, 2)
    rg_fwd(5, 2)
    total = dw_sm[f]
    arrive(rr_sm, sg_r.at[0], to_ring[0])
    for d in range(1, N):
        total = total + rr_sm[d - 1]
    o_sm[s] = total
    for dev in (to_core, to_y, {"seq": s_diag}):
        send(o_sm.at[s], o_sm.at[s], sm_s.at[0], sm_r.at[0], dev)

    hbm = [h_dn, h_up.at[:, :, sides[0]], h_ow, h_qkv.at[0]]
    hbm += [h_qkv.at[1, :, split[h]] for h in range(2)] + [h_up.at[:, :, sides[1]]]
    finals = [(KFIN + m, fin_slot(m)) for m in range(MG)]

    def put_slot(m, k):
        put(grads[m][2].at[k], hbm[m].at[k], m)

    def relay_out(m):
        sq_relay(*finals[m])
        put_slot(m, s_y)

    for m in (0, 1, 6, 2):
        put_slot(m, s)
    relay_out(0)
    relay_out(1)
    rg_fin(3)
    put_slot(3, s)
    for m in (4, 5):
        rg_fin(m)
        put_slot(m, s)
    relay_out(6)
    for h in range(2):
        from_y(2, grecv, h)
    gn = here + grecv[1].astype(F32)
    cot[...] = (gmid[...] + norm_pull(gn, row(0), unit, rate))[:T].astype(BF)
    put(cot, h_tok, 9)
    for m in range(MG):
        sq_core(*finals[m])
        put_slot(m, s_core)
    for m in (2, 3, 4, 5):
        relay_out(m)
    arrive(o_sm.at[:3], sm_r.at[0], to_core)
    put(o_sm, h_sm, 7)
    for m in range(MG):
        sq_diag(*finals[m])
        put_slot(m, s_diag)

    for m in range(MA):
        ag_sent(m)
    for m in range(MG):
        rg_sent(m)
    for kind, ref in ((KX, xg), (KC, cg)):
        sq_sent(kind, ref.at[:3])
    for h in range(2):
        sq_sent(KG + h, nrm.at[:3, halves[h]])
    sq_sent(KO, wout.at[:, : 3 * DH])
    for hp in range(HP):
        sq_sent(KCTX + hp, ctx.at[:3, :, hp * 128 : hp * 128 + 128])
    for m in range(MG):
        sq_sent(KFIN + m, grads[m][2].at[:3])
    seq_sent(1, opart)
    seq_sent(2, gpart)
    sent(smg.at[: N - 1], sa_s.at[0], to_ring[0])
    sent(dw_sm.at[: N - 1], sg_s.at[0], to_ring[0])
    sent(o_sm.at[:3], sm_s.at[0], to_core)
    for src, dst, k in [(grads[m][2], hbm[m], m) for m in range(MG)] + [(o_sm, h_sm, 7), (tok, h_out, 8), (cot, h_tok, 9)]:
        pltpu.make_async_copy(src, dst, put_sem.at[k]).wait()


def finish_kernel(z, *refs):
    srcs, dsts = refs[:7], refs[7:22]
    (out, tok, gq, go, gu, gd, gs), bufs = refs[22:29], refs[29:42]
    s_in, s_out = refs[42:]
    D, w, wf, HP, N = z["D"], z["w"], z["wf"], z["HP"], 2 * z["A"]
    DH = D // 4
    loads = [pltpu.make_async_copy(src, dst, s_in.at[k]) for k, (src, dst) in enumerate(zip(srcs, (out, tok, gq, go, gu, gd, gs)))]
    saves = []

    def save(src, k):
        copy = pltpu.make_async_copy(src, dsts[k], s_out.at[k])
        copy.start()
        saves.append(copy)

    for k in (0, 1, 5, 4, 2, 3, 6):
        loads[k].start()
    for k, buf in ((0, out), (1, tok)):
        loads[k].wait()
        save(buf, k)
    f_qkv, f_ow, f_up, f_dn = bufs[:4]
    loads[5].wait()
    for s in range(4):
        f_dn[s * wf : (s + 1) * wf] = gd[s].astype(F32)
    save(f_dn, 5)
    loads[4].wait()
    if z["up_whole"]:
        for s in range(4):
            for k in range(N):
                f_up[:, (k * 4 + s) * wf : (k * 4 + s + 1) * wf] = gu[s, :, k * wf : (k + 1) * wf].astype(F32)
    else:
        f_up[...] = gu[...].astype(F32)
    save(f_up, 4)
    loads[2].wait()
    for s in range(4):
        for hp in range(HP):
            for part in range(3):
                lo = part * D + s * DH + hp * 128
                f_qkv[:, lo : lo + 128] = gq[hp, s, :, part * 128 : part * 128 + 128].astype(F32)
    save(f_qkv, 2)
    loads[3].wait()
    for s in range(4):
        f_ow[:, s * DH : (s + 1) * DH] = go[s].astype(F32)
    save(f_ow, 3)
    loads[6].wait()
    total = gs[0] + gs[1] + gs[2] + gs[3]
    for k in range(8):
        bufs[4 + k][...] = total[k : k + 1]
        save(bufs[4 + k], 6 + k)
    bufs[12][...] = jnp.concatenate([gs[s, 8:9] for s in range(4)], axis=1)
    save(bufs[12], 14)
    for copy in saves:
        copy.wait()


def make_body(mesh):
    N = mesh.shape["fsdp"]
    A = N // 2

    def body(
        tokens, lengths, ln1_gain, ln1_bias, qkv_weight, q_bias, v_bias, out_weight, out_bias,
        ln2_gain, ln2_bias, up_weight, up_bias, down_weight, down_bias, cotangent,
    ):
        _, T, D = tokens.shape
        w, FF = D // N, up_weight.shape[1]
        wf = FF // (4 * N)
        TP = -(-T // 16) * 16
        R = 4 * TP
        DH = D // 4
        HP = DH // 128
        FQ = FF // 4
        assert FQ == D and wf == w and HP == 2
        g = max(128 // w, 1)
        s = lax.axis_index("seq")
        f = lax.axis_index("fsdp")
        up_whole = wf % 128 == 0
        plain = (ln1_gain, ln1_bias, q_bias, v_bias, out_bias, ln2_gain, ln2_bias, down_bias)
        if g == 1:
            vectors_in = [v.reshape(1, w) for v in plain]
            ub_in = up_bias.reshape(4, wf)
        else:
            spot = lax.rem(f, g) * w
            blank = jnp.zeros((1, 128), BF)
            vectors_in = [lax.dynamic_update_slice(blank, v[None], (0, spot)) for v in plain]
            mine = lax.dynamic_slice(up_bias, (s * wf,), (wf,))
            ub_in = lax.dynamic_update_slice(jnp.zeros((4, 128), BF), mine[None], (s, spot))
        if not up_whole:
            up_weight = lax.dynamic_index_in_dim(up_weight.reshape(w, N, 4, wf), s, 2, False).reshape(w, FQ)
        z = dict(D=D, T=T, TP=TP, R=R, A=A, w=w, wf=wf, HP=HP, g=g, up_whole=up_whole)
        vm = pltpu.VMEM
        C = 384
        scratch = [
            vm((T, D), BF), vm((T, D), BF), pltpu.SMEM((1,), jnp.int32), vm((8, 1, 128), BF), vm((4, 128), BF),
            vm((HP, 4, w, C), BF), vm((4, w, DH), BF), vm((4, w, FQ), BF), vm((4, wf, D), BF), vm((4, 16, 128), F32),
            vm((4, TP, D), BF),
            vm((4, TP, D), BF),
            vm((4, TP, D), BF),
            vm((4, R, DH), BF),
            vm((4, TP, D), BF),
            vm((4, TP, D), BF),
            vm((4, TP, D), BF),
            vm((4, TP, HP * C), BF),
            vm((D, HP * C), BF),
            vm((D, D), BF),
            vm((D, FQ), BF),
            vm((FQ, D), BF),
            vm((N, 16, 128), BF),
            vm((16, D), F32),
            vm((16, D), F32),
            vm((HP, R, 128), F32),
            vm((TP, D), F32),
            vm((TP, D), F32),
            vm((4, TP, DH), BF),
            vm((HP, 128, R), F32),
            vm((HP, 128, R), F32),
            vm((3, TP, D), BF), vm((TP, D), F32), vm((3, TP, D), BF),
            vm((3, TP, D), BF), vm((TP, D), F32), vm((3, TP, D), BF),
            vm((1, R), F32),
            vm((HP, N, w, C), BF), vm((N, w, DH), BF), vm((N, w, FQ), BF), vm((N, wf, D), BF), vm((N, 16, 128), F32),
            vm((HP, 2, A, w, C), BF), vm((2, A, w, DH), BF), vm((2, A, w, FQ), BF), vm((2, A, wf, D), BF), vm((N - 1, 16, 128), F32),
        ]
        dma = pltpu.SemaphoreType.DMA
        scratch += [
            dma((9,)), dma((10,)),
            dma((4 + HP,)), dma((4 + HP, A)), dma((7,)), dma((7, A)),
            dma((12 + HP,)), dma((12 + HP, 3)),
            dma((3,)), dma((3, 3, 2)),
            dma((1,)), dma((1,)), dma((1,)), dma((1,)), dma((1,)), dma((1,)),
        ]
        there = pl.BlockSpec(memory_space=pl.ANY)
        out_shapes = [
            jax.ShapeDtypeStruct((T, D), BF),
            jax.ShapeDtypeStruct((T, D), BF),
            jax.ShapeDtypeStruct((HP, 4, w, C), BF),
            jax.ShapeDtypeStruct((4, w, DH), BF),
            jax.ShapeDtypeStruct((4, w, FQ), BF),
            jax.ShapeDtypeStruct((4, wf, D), BF),
            jax.ShapeDtypeStruct((4, 16, 128), F32),
        ]
        out, gtok, gq, go, gu, gd, gs = pl.pallas_call(
            functools.partial(layer_entry, z),
            out_shape=out_shapes,
            in_specs=[there] * 16,
            out_specs=[there] * 7,
            scratch_shapes=scratch,
            compiler_params=pltpu.CompilerParams(
                collective_id=0, has_side_effects=True, vmem_limit_bytes=67_000_000
            ),
            name="layer",
        )(tokens[0], cotangent[0], lengths, *vectors_in, ub_in, qkv_weight, out_weight, up_weight, down_weight)

        if not up_whole:
            gu = gu.reshape(4, w, N, wf).transpose(1, 2, 0, 3).reshape(w, FF)
        if g > 1:
            gs = lax.dynamic_slice(gs, (0, 0, lax.rem(f, g) * w), (4, 16, w))
        shapes = [((w, 3 * D), F32), ((w, D), F32), ((w, FF), F32), ((4 * wf, D), F32)]
        shapes += [((1, w), F32)] * 8 + [((1, 4 * wf), F32)]
        sources = (out, gtok, gq, go, gu, gd, gs)
        done = pl.pallas_call(
            functools.partial(finish_kernel, z),
            out_shape=[jax.ShapeDtypeStruct(*v) for v in [((T, D), BF)] * 2 + shapes],
            in_specs=[there] * 7,
            out_specs=[there] * 15,
            scratch_shapes=[vm(v.shape, v.dtype) for v in sources] + [vm(*v) for v in shapes] + [dma((7,)), dma((15,))],
            name="finish",
        )(*sources)
        out, gtok, g_qkv, g_out, g_up, g_down = done[:6]
        sums = [v.reshape(-1) for v in done[6:]]
        return (
            out[None], gtok[None], sums[0], sums[1], g_qkv, sums[2], sums[3], g_out, sums[4],
            sums[5], sums[6], g_up, sums[8], g_down, sums[7],
        )

    return body


def solution(mesh):
    row, mat, act = P("fsdp"), P("fsdp", None), P("fsdp", "seq", None)
    return jax.shard_map(
        make_body(mesh),
        mesh=mesh,
        in_specs=(act, row, row, row, mat, row, row, mat, row, row, row, mat, row, mat, row, act),
        out_specs=(act, act, row, row, mat, row, row, mat, row, row, row, mat, row, mat, row),
        check_vma=False,
    )
```
